32 devices in a mesh: fsdp: 4 (over y, x), ctx: 2 (over core), tp: 4 (over z).
Axes of the slice: x: 2, y: 2, z: 4, core: 2. Of those that a mesh axis runs over, the one named last changes fastest.
Arguments:
- tokens: bfloat16 [4, 1024, 2048], P('fsdp', 'ctx'), may hold values from -6 to 6
- cotangent: bfloat16 [4, 1024, 2048], P('fsdp', 'ctx'), may hold values from -6 to 6
- block_ids: int32 [4, 1024], P('fsdp'), may hold values from 0 to 3, never falling along the last dimension, each value on 1 to 384 neighbouring positions
- live_count: int32 [4], P('fsdp'), may hold values from 0 to 1, as said below
- first_gain: bfloat16 [2048], P(('fsdp', 'ctx')), may hold values from 0.25 to 1.75
- first_shift: bfloat16 [2048], P(('fsdp', 'ctx')), may hold values from -1.796875 to 1.796875
- query_weight: bfloat16 [2048, 2048], P(('fsdp', 'ctx'), 'tp'), may hold values from -0.125 to 0.125
- query_bias: bfloat16 [16, 128], P('tp', ('fsdp', 'ctx')), may hold values from -3 to 3
- key_weight: bfloat16 [2048, 2048], P(('fsdp', 'ctx'), 'tp'), may hold values from -0.125 to 0.125
- value_weight: bfloat16 [2048, 2048], P(('fsdp', 'ctx'), 'tp'), may hold values from -0.125 to 0.125
- value_bias: bfloat16 [16, 128], P('tp', ('fsdp', 'ctx')), may hold values from -3 to 3
- output_weight: bfloat16 [2048, 2048], P('tp', ('fsdp', 'ctx')), may hold values from -0.5 to 0.5
- output_bias: bfloat16 [2048], P(('fsdp', 'ctx')), may hold values from -1.796875 to 1.796875
- second_gain: bfloat16 [2048], P(('fsdp', 'ctx')), may hold values from 0.25 to 1.75
- second_shift: bfloat16 [2048], P(('fsdp', 'ctx')), may hold values from -1.796875 to 1.796875
- expand_weight: bfloat16 [2048, 8192], P(('fsdp', 'ctx'), 'tp'), may hold values from -0.125 to 0.125
- expand_bias: bfloat16 [16, 512], P('tp', ('fsdp', 'ctx')), may hold values from -3 to 3
- reduce_weight: bfloat16 [8192, 2048], P('tp', ('fsdp', 'ctx')), may hold values from -0.0625 to 0.0625
- reduce_bias: bfloat16 [2048], P(('fsdp', 'ctx')), may hold values from -1.796875 to 1.796875
Outputs:
- layer_out: bfloat16 [4, 1024, 2048], P('fsdp', 'ctx')
- tokens_grad: bfloat16 [4, 1024, 2048], P('fsdp', 'ctx')
- first_gain_grad: float32 [2048], P(('fsdp', 'ctx'))
- first_shift_grad: float32 [2048], P(('fsdp', 'ctx'))
- query_weight_grad: float32 [2048, 2048], P(('fsdp', 'ctx'), 'tp')
- query_bias_grad: float32 [16, 128], P('tp', ('fsdp', 'ctx'))
- key_weight_grad: float32 [2048, 2048], P(('fsdp', 'ctx'), 'tp')
- value_weight_grad: float32 [2048, 2048], P(('fsdp', 'ctx'), 'tp')
- value_bias_grad: float32 [16, 128], P('tp', ('fsdp', 'ctx'))
- output_weight_grad: float32 [2048, 2048], P('tp', ('fsdp', 'ctx'))
- output_bias_grad: float32 [2048], P(('fsdp', 'ctx'))
- second_gain_grad: float32 [2048], P(('fsdp', 'ctx'))
- second_shift_grad: float32 [2048], P(('fsdp', 'ctx'))
- expand_weight_grad: float32 [2048, 8192], P(('fsdp', 'ctx'), 'tp')
- expand_bias_grad: float32 [16, 512], P('tp', ('fsdp', 'ctx'))
- reduce_weight_grad: float32 [8192, 2048], P('tp', ('fsdp', 'ctx'))
- reduce_bias_grad: float32 [2048], P(('fsdp', 'ctx'))
The draws below stay inside these ranges and needn't reach their ends.
Inputs may be any that keep to these rules, and one draw needn't show every extreme that they name: Index r of fsdp holds one sequence in its single slot if live_count[r] = 1 and none if live_count[r] = 0; at least one index holds a sequence and at least one holds none. `block_ids`: block numbers never fall along a sequence; a block holds 1 to 384 positions.
All inputs are finite; a program needn't handle non-finite values.
Results may differ from the reference program's by a relative error of at most 0.015.
Values may be sent and summed in bfloat16 or wider, within the bound.
A program may use at most 192 MiB of HBM per device.

```python
import math
import jax
import jax.numpy as jnp
import numpy as np
from jax import lax

D = 2048
H = 16
HD = 128
FF = 8192
LEN = 1024
BLK = 256
SLOTS = 1
SEQS = 4
N_FSDP = 4


def draw_live_count(key, part):
    key_coin, key_order = jax.random.split(jax.random.fold_in(key, 7))
    tosses = jax.random.randint(key_coin, (N_FSDP,), 0, 2)
    rank_order = jax.random.permutation(key_order, N_FSDP)
    rank_index = jnp.arange(N_FSDP)
    tosses = jnp.where(rank_index == rank_order[0], 1, tosses)
    tosses = jnp.where(rank_index == rank_order[1], 0, tosses)
    return (SLOTS - 1 + tosses).astype(jnp.int32)


def block_levels(own_key, dims, pieces, low, largest):
    level = 1.0
    for position, shards_of in pieces:
        draws = jax.random.uniform(jax.random.fold_in(jax.random.fold_in(own_key, 6), position), (shards_of,), jnp.float32, low / len(pieces), largest / len(pieces))
        level = level * jnp.repeat(jnp.exp(draws), dims[position] // shards_of).reshape((-1,) + (1,) * (len(dims) - 1 - position))
    return level


def profile(amount, total, bound, skew):
    weights = [(1 << 20) // math.isqrt(grade ** skew) + 1 for grade in range(2, amount + 1)]
    rest, given = total - bound - (amount - 1), [1] * (amount - 1)
    while rest > 0:
        candidates = [i for i in range(amount - 1) if given[i] < bound]
        mass, budget = sum([weights[i] for i in candidates]), rest
        for i in candidates:
            more = min(bound - given[i], max(1, budget * weights[i] // mass), rest)
            given[i] = given[i] + more
            rest = rest - more
    return np.array([bound] + given)


def ragged(rng, amount, total, limit, skew):
    if amount == 2:
        one = jax.random.randint(rng, (), max(1, total - limit), min(limit, total - 1) + 1)
        return jnp.stack([one, total - one])
    tallies = jnp.asarray(profile(amount, total, limit, skew), jnp.int32)
    couples = (amount - 1) // 2
    source_of, receiver = tallies[1:1 + 2 * couples:2], tallies[2:2 + 2 * couples:2]
    room = jnp.minimum(source_of - 1, limit - receiver)
    shifted = jax.random.randint(jax.random.fold_in(rng, 1), (couples,), 0, 1 << 20) % (room + 1)
    tallies = tallies.at[1:1 + 2 * couples:2].set(source_of - shifted).at[2:2 + 2 * couples:2].set(receiver + shifted)
    return tallies[jax.random.permutation(jax.random.fold_in(rng, 2), amount)]


def noise(key, extent, scale, bound, pieces=(), held_as=jnp.bfloat16):
    factor_of = block_levels(key, extent, pieces, -0.22, 0.18) if pieces else 1.0
    values = jax.random.normal(key, extent, jnp.float32) * scale * factor_of
    return jnp.minimum(jnp.maximum(values, -bound), bound).astype(held_as)


def setup_inputs(seed: int = 0) -> dict:
    streams_of = jax.random.split(jax.random.key(seed), 20)
    tokens = noise(streams_of[0], (SEQS, LEN, D), 1.0, 6.0, ((0, 4), (1, 2)))
    cotangent = noise(streams_of[1], (SEQS, LEN, D), 1.0, 6.0, ((0, 4), (1, 2)))
    block_ids = jax.vmap(lambda own: jnp.searchsorted(jnp.cumsum(ragged(own, LEN // BLK, LEN, BLK + BLK // 2, 1)), jnp.arange(LEN), side="right"))(jax.random.split(streams_of[2], SEQS)).reshape((SEQS, LEN)).astype(jnp.int32)
    live_count = draw_live_count(jax.random.fold_in(streams_of[19], 71), 0)
    first_gain = jnp.clip(1.0 + 0.15 * jax.random.normal(streams_of[4], (D,), jnp.float32), 0.25, 1.75).astype(jnp.bfloat16)
    first_shift = noise(streams_of[5], (D,), 0.3, 1.796875, ((0, 8),))
    query_weight = noise(streams_of[6], (D, D), D ** -0.5, 0.125, ((0, 8), (1, 4)))
    query_bias = noise(streams_of[7], (H, HD), 0.5, 3.0, ((0, 4), (1, 8)))
    key_weight = noise(streams_of[8], (D, D), D ** -0.5, 0.125, ((0, 8), (1, 4)))
    value_weight = noise(streams_of[9], (D, D), D ** -0.5, 0.125, ((0, 8), (1, 4)))
    value_bias = noise(streams_of[10], (H, HD), 0.5, 3.0, ((0, 4), (1, 8)))
    output_weight = noise(streams_of[11], (D, D), (D // 16) ** -0.5, 0.5, ((0, 4), (1, 8)))
    output_bias = noise(streams_of[12], (D,), 0.3, 1.796875, ((0, 8),))
    second_gain = jnp.clip(1.0 + 0.15 * jax.random.normal(streams_of[13], (D,), jnp.float32), 0.25, 1.75).astype(jnp.bfloat16)
    second_shift = noise(streams_of[14], (D,), 0.3, 1.796875, ((0, 8),))
    expand_weight = noise(streams_of[15], (D, FF), D ** -0.5, 0.125, ((0, 8), (1, 4)))
    expand_bias = noise(streams_of[16], (H, FF // H), 0.5, 3.0, ((0, 4), (1, 8)))
    reduce_weight = noise(streams_of[17], (FF, D), FF ** -0.5, 0.0625, ((0, 4), (1, 8)))
    reduce_bias = noise(streams_of[18], (D,), 0.3, 1.796875, ((0, 8),))
    return dict(tokens=tokens, cotangent=cotangent, block_ids=block_ids, live_count=live_count, first_gain=first_gain, first_shift=first_shift, query_weight=query_weight, query_bias=query_bias, key_weight=key_weight, value_weight=value_weight, value_bias=value_bias, output_weight=output_weight, output_bias=output_bias, second_gain=second_gain, second_shift=second_shift, expand_weight=expand_weight, expand_bias=expand_bias, reduce_weight=reduce_weight, reduce_bias=reduce_bias)


@jax.custom_vjp
def low(v):
    return lax.optimization_barrier(v.astype(jnp.bfloat16)).astype(jnp.float32)

@jax.custom_vjp
def low_back(v):
    return v

def low_keep(v):
    return (low(v), None)

def low_pass(kept, grad):
    return (grad,)

def back_keep(v):
    return (v, None)

def back_low(kept, grad):
    return (low(grad),)
low.defvjp(low_keep, low_pass)
low_back.defvjp(back_keep, back_low)

def matmul(left, right):
    return jnp.dot(left, right, precision=lax.Precision.HIGHEST, preferred_element_type=jnp.float32)

def layer_norm(values, gain, shift):
    center = values - lax.optimization_barrier(jnp.mean(values, axis=-1, keepdims=True))
    spread = lax.rsqrt(lax.optimization_barrier(jnp.mean(center * center, axis=-1, keepdims=True)) + 1e-05)
    return center * spread * gain + shift

def gelu_exact(values):
    return 0.5 * values * (1.0 + lax.erf(values * (1.0 / math.sqrt(2.0))))

def attend_block(queries, keys, values, query_ids, key_ids):
    scores = jnp.einsum('qhd,khd->hqk', queries, keys, precision=lax.Precision.HIGHEST) * (1.0 / math.sqrt(HD))
    scores = low_back(scores)
    allowed = key_ids[None, None, :] <= query_ids[None, :, None]
    scores = jnp.where(allowed, scores, -1e+30)
    top = lax.optimization_barrier(jnp.max(scores, axis=-1, keepdims=True))
    weights = jnp.exp(scores - top)
    probs = low(weights / lax.optimization_barrier(jnp.sum(weights, axis=-1, keepdims=True)))
    return jnp.einsum('hqk,khd->qhd', probs, values, precision=lax.Precision.HIGHEST)

def attention(queries, keys, values, seq_ids):
    block_len = math.gcd(512, LEN)
    block_count = LEN // block_len
    query_blocks = queries.reshape(block_count, block_len, H, HD)
    id_blocks = seq_ids.reshape(block_count, block_len)
    checked = jax.checkpoint(lambda query_part, id_part: attend_block(query_part, keys, values, id_part, seq_ids))
    result = lax.map(lambda block_pair: checked(block_pair[0], block_pair[1]), (query_blocks, id_blocks))
    return result.reshape(LEN, D)

def layer(params, inputs, seq_ids, live_flag):
    first_gain, first_shift, query_weight, query_bias, key_weight, value_weight, value_bias, output_weight, output_bias, second_gain, second_shift, expand_weight, expand_bias, reduce_weight, reduce_bias = params
    normed_one = low(layer_norm(inputs, first_gain, first_shift))
    queries = low(low_back(matmul(normed_one, query_weight) + query_bias.reshape(-1)))
    keys = low(low_back(matmul(normed_one, key_weight)))
    values = low(low_back(matmul(normed_one, value_weight) + value_bias.reshape(-1)))
    context = attention(queries.reshape(LEN, H, HD), keys.reshape(LEN, H, HD), values.reshape(LEN, H, HD), seq_ids)
    context = low(low_back(context))
    middle = inputs + low_back(matmul(context, output_weight) + output_bias)
    normed_two = low(layer_norm(middle, second_gain, second_shift))
    hidden = low_back(matmul(normed_two, expand_weight) + expand_bias.reshape(-1))
    active = low(gelu_exact(hidden))
    return (middle + matmul(active, reduce_weight) + reduce_bias) * live_flag

def reference(tokens, cotangent, block_ids, live_count, first_gain, first_shift, query_weight, query_bias, key_weight, value_weight, value_bias, output_weight, output_bias, second_gain, second_shift, expand_weight, expand_bias, reduce_weight, reduce_bias):
    params = tuple((member.astype(jnp.float32) for member in (first_gain, first_shift, query_weight, query_bias, key_weight, value_weight, value_bias, output_weight, output_bias, second_gain, second_shift, expand_weight, expand_bias, reduce_weight, reduce_bias)))
    seq_index = jnp.arange(SEQS, dtype=jnp.int32)
    live = (seq_index % SLOTS < live_count[seq_index // SLOTS]).astype(jnp.float32)

    def one_seq(totals, element):
        inputs, grads_in, seq_ids, live_flag = element
        outputs, pullback = jax.vjp(lambda weights, tokens_in: layer(weights, tokens_in, seq_ids, live_flag), params, inputs)
        weight_grads, input_grad = pullback(grads_in)
        totals = jax.tree.map(lambda running, update: running + update, totals, weight_grads)
        return (totals, (outputs.astype(jnp.bfloat16), input_grad.astype(jnp.bfloat16)))
    initial = jax.tree.map(jnp.zeros_like, params)
    totals, outs_pair = lax.scan(one_seq, initial, (tokens.astype(jnp.float32), cotangent.astype(jnp.float32), block_ids, live))
    layer_out, tokens_grad = outs_pair
    g_first_gain, g_first_shift, g_query_weight, g_query_bias, g_key_weight, g_value_weight, g_value_bias, g_output_weight, g_output_bias, g_second_gain, g_second_shift, g_expand_weight, g_expand_bias, g_reduce_weight, g_reduce_bias = totals
    return (layer_out, tokens_grad, g_first_gain, g_first_shift, g_query_weight, g_query_bias, g_key_weight, g_value_weight, g_value_bias, g_output_weight, g_output_bias, g_second_gain, g_second_shift, g_expand_weight, g_expand_bias, g_reduce_weight, g_reduce_bias)
```

```python
import functools
import math

import jax
import jax.numpy as jnp
from jax import lax
from jax.experimental import pallas as pl
from jax.experimental.pallas import tpu as pltpu
from jax.sharding import PartitionSpec as P

HD = 128
NEG = -1e30
MESH = pl.DeviceIdType.MESH
ANY = pl.BlockSpec(memory_space=pl.ANY)
VM = pl.BlockSpec(memory_space=pltpu.VMEM)
BF = jnp.bfloat16
F32 = jnp.float32
epsilon = 1e-05


def dot(left, right):
    return lax.dot_general(left, right, (((1,), (0,)), ((), ())), preferred_element_type=F32)


def dot_nt(left, right):
    return lax.dot_general(left, right, (((1,), (1,)), ((), ())), preferred_element_type=F32)


def dot_tn(left, right):
    return lax.dot_general(left, right, (((0,), (0,)), ((), ())), preferred_element_type=F32)


def al(value, step):
    return pl.multiple_of(value, step)


class Place:
    def __init__(self, n_f, n_t):
        self.n_f, self.n_t, self.m = n_f, n_t, n_f // 2
        self.f = lax.axis_index("fsdp")
        self.c = lax.axis_index("ctx")
        self.t = lax.axis_index("tp")
        self.p = self.spot(self.f)
        self.side = self.t // (n_t - 1)
        self.right = (self.owner(1), self.c, self.t)
        self.left = (self.owner(-1), self.c, self.t)
        self.sib = (self.f, 1 - self.c, self.t)

    def spot(self, g):
        a = g // self.m
        return (1 - a) * g + a * (self.n_f - 1 + self.m - g)

    def owner(self, k):
        return self.spot(lax.rem(self.p + k + self.n_f, self.n_f))

    def shard(self, k, other=False):
        c = 1 - self.c if other else self.c
        return 2 * self.owner(k) + c

    def tp(self, d):
        return (self.f, self.c, lax.rem(self.t + d + self.n_t, self.n_t))

    def plane(self, k):
        return (lax.rem(self.f + k, self.n_f), self.c, self.t)

    def greet(self):
        bar = pltpu.get_barrier_semaphore()
        others = [self.sib] + [self.plane(k) for k in range(1, self.n_f)]
        others += [self.tp(k) for k in range(1, self.n_t)]
        for other in others:
            pl.semaphore_signal(bar, 1, device_id=other, device_id_type=MESH)
        pl.semaphore_wait(bar, len(others))


def remote(src, dst, send, recv, to):
    return pltpu.make_async_remote_copy(
        src_ref=src, dst_ref=dst, send_sem=send, recv_sem=recv, device_id=to, device_id_type=MESH
    )


class Gather:
    def __init__(self, here, own, slot, send, recv):
        self.here, self.own, self.slot, self.send, self.recv = here, own, slot, send, recv
        self.m = here.m

    def half(self, way, s):
        return None if s < self.m else way

    def hop(self, way, s):
        here, sign = self.here, (-1, 1)[way]
        part = self.half(way, s)
        idx = here.shard(sign * (s - 1))
        src = self.own(part) if s == 1 else self.slot(idx, part)
        k = way * self.m + s - 1
        to = (here.right, here.left)[way]
        return remote(src, self.slot(idx, part), self.send.at[k], self.recv.at[k], to)

    def landing(self, way, s):
        here, sign = self.here, (-1, 1)[way]
        part = self.half(way, s)
        ref = self.slot(here.shard(sign * s), part)
        k = way * self.m + s - 1
        to = (here.right, here.left)[way]
        return remote(ref, ref, self.send.at[k], self.recv.at[k], to)

    def cross(self, k, offset, other=False):
        here = self.here
        ref = self.slot(here.shard(offset, other), None)
        src = self.own(None) if (offset == 0 and not other) else ref
        n = 2 * self.m + k
        return remote(src, ref, self.send.at[n], self.recv.at[n], here.sib)

    def crossings(self):
        found = [(0, 0)]
        for s in range(1, self.m):
            found += [(2 * s - 1, -s), (2 * s, s)]
        return found + [(2 * self.m - 1, self.m)]

    def start(self):
        self.hop(0, 1).start()
        self.hop(1, 1).start()
        self.cross(0, 0).start()

    def step(self, s):
        self.landing(0, s).wait_recv()
        self.landing(1, s).wait_recv()
        if s < self.m:
            self.hop(0, s + 1).start()
            self.hop(1, s + 1).start()
            self.cross(2 * s - 1, -s).start()
            self.cross(2 * s, s).start()
        else:
            self.cross(2 * self.m - 1, self.m).start()

    def arrive(self):
        for k, offset in self.crossings():
            self.cross(k, offset, True).wait_recv()

    def finish(self):
        for s in range(1, self.m + 1):
            self.hop(0, s).wait_send()
            self.hop(1, s).wait_send()
        for k, offset in self.crossings():
            self.cross(k, offset).wait_send()

    @staticmethod
    def sems(n_f):
        return 2 * n_f


class Line:
    def __init__(self, here, part, rbuf, norm, sems, chunks, lag):
        self.here, self.part, self.rbuf, self.norm = here, part, rbuf, norm
        self.s_send, self.s_recv, self.g_send, self.g_recv = sems
        self.half = part.shape[0] // 2
        self.nc, self.lag = chunks, lag
        self.cr = self.half // chunks

    def rows(self, d, j):
        return pl.ds(al(d * self.half + j * self.cr, self.cr), self.cr)

    def span(self, j):
        return pl.ds(al(j * self.cr, self.cr), self.cr)

    def s_copy(self, d, j):
        return remote(
            self.part.at[self.rows(d, j)],
            self.rbuf.at[d, self.span(j)],
            self.s_send.at[d, j],
            self.s_recv.at[d, j],
            self.here.tp(2 * d - 1),
        )

    def g_copy(self, d, j):
        ref = self.norm.at[self.rows(d, j)]
        to = self.here.tp(1 - 2 * d)
        return remote(ref, ref, self.g_send.at[d, j], self.g_recv.at[d, j], to)

    def depth(self, d):
        t, n = self.here.t, self.here.n_t
        return t if d == 1 else n - 1 - t

    def sum_step(self, d, tau):
        depth, n = self.depth(d), self.here.n_t
        j = tau - self.lag * depth
        valid = (j >= 0) & (j < self.nc)

        @pl.when(valid & (depth > 0))
        def _():
            self.s_copy(d, j).wait_recv()

        @pl.when(valid & (depth > 0) & (depth < n - 1))
        def _():
            own = self.part[self.rows(d, j), :].astype(F32)
            got = self.rbuf[d, self.span(j), :].astype(F32)
            self.part[self.rows(d, j), :] = (own + got).astype(BF)

        @pl.when(valid & (depth < n - 1))
        def _():
            self.s_copy(d, j).start()

    def owner_step(self, tau, final, back=True):
        here, n = self.here, self.here.n_t
        j = tau - self.lag * (n - 1)
        end = (here.t == 0) | (here.t == n - 1)

        @pl.when(end & (j >= 0) & (j < self.nc))
        def _():
            d = here.side
            rows = self.rows(d, j)
            total = self.part[rows, :].astype(F32) + self.rbuf[d, self.span(j), :].astype(F32)
            final(rows, self.span(j), total)
            if back:
                self.back_copy(j).start()

    def back_copy(self, j):
        here = self.here
        d = here.side
        ref = self.norm.at[self.rows(d, j)]
        return remote(
            ref, ref, self.g_send.at[d, j], self.g_recv.at[d, j], here.tp(1 - 2 * d)
        )

    def gather_step(self, d, tau, base):
        t, n = self.here.t, self.here.n_t
        depth = t if d == 0 else n - 1 - t
        j = tau - base - self.lag * depth
        valid = (j >= 0) & (j < self.nc) & (depth > 0)

        @pl.when(valid)
        def _():
            self.g_copy(d, j).wait_recv()

        @pl.when(valid & (depth < n - 1))
        def _():
            self.g_copy(d, j).start()

    def sum_ticks(self):
        return self.nc + self.lag * (self.here.n_t - 1)

    def ticks(self):
        return self.nc + 2 * self.lag * (self.here.n_t - 1)

    def tick(self, tau, final, back=True):
        self.sum_step(1, tau)
        self.sum_step(0, tau)
        self.owner_step(tau, final, back)
        if back:
            base = self.lag * (self.here.n_t - 1)
            self.gather_step(0, tau, base)
            self.gather_step(1, tau, base)

    def finish_sum(self):
        t, n = self.here.t, self.here.n_t

        def body(j, _):
            @pl.when(t > 0)
            def _():
                self.s_copy(0, j).wait_send()

            @pl.when(t < n - 1)
            def _():
                self.s_copy(1, j).wait_send()

            return 0

        lax.fori_loop(0, self.nc, body, 0)

    def finish_back(self):
        t, n = self.here.t, self.here.n_t

        def body(j, _):
            @pl.when(t < n - 1)
            def _():
                self.g_copy(0, j).wait_send()

            @pl.when(t > 0)
            def _():
                self.g_copy(1, j).wait_send()

            return 0

        lax.fori_loop(0, self.nc, body, 0)

    @staticmethod
    def sems(chunks):
        return [pltpu.SemaphoreType.DMA((2, chunks))] * 4


def norm_rows(values):
    mean = jnp.mean(values, axis=-1, keepdims=True)
    center = values - mean
    spread = lax.rsqrt(jnp.mean(center * center, axis=-1, keepdims=True) + epsilon)
    return center * spread, spread


class Outs:
    def __init__(self, sem):
        self.sem, self.made = sem, []

    def put(self, src, dst):
        copy = pltpu.make_async_copy(src, dst, self.sem.at[len(self.made)])
        copy.start()
        self.made.append(copy)

    def wait(self):
        for copy in self.made:
            copy.wait()


def row_slots(ref, size):
    def slot(idx, part):
        if part is None:
            return ref.at[pl.ds(al(idx * size, size), size)]
        return ref.at[pl.ds(al(idx * size + part * (size // 2), size // 2), size // 2)]

    return slot


def lead_slots(ref):
    size = ref.shape[1]

    def slot(idx, part):
        if part is None:
            return ref.at[idx]
        return ref.at[idx, pl.ds(part * (size // 2), size // 2)]

    return slot


def own_part(ref):
    size = ref.shape[0]

    def own(part):
        if part is None:
            return ref
        return ref.at[pl.ds(part * (size // 2), size // 2)]

    return own


def allowed_scores(q, k, col, row, scale):
    return jnp.where(row <= col, dot_nt(q, k) * scale, NEG)


def forward_kernel(
    n_f, n_t, chunks, lag,
    tok, col, row, small, wa, wo, we, wr,
    n1_o, q_o, kv_o, ctx_o, n2_o, mid_o, par_o, a_o, o_o, e_o, r_o,
    tokv, n1, full_a, full_o, stage_e, stage_r, q, kv, ctx, part, rbuf, norm, mid,
    sib_small, all_small, par,
    ga_s, ga_r, go_s, go_r, ge_s, ge_r, gr_s, gr_r,
    ls_s, ls_r, lg_s, lg_r, sm_s, sm_r, kv_s, kv_r, in_sem, out_sem,
):
    here = Place(n_f, n_t)
    width = wo.shape[0]
    shard = wa.shape[0]
    rows_all, model = n1.shape
    heads = width // HD
    scale = 1.0 / math.sqrt(HD)
    tok_in = pltpu.make_async_copy(tok, tokv, in_sem.at[0])
    tok_in.start()
    me = 2 * here.f + here.c
    a_slot, o_slot = row_slots(full_a, shard), lead_slots(full_o)
    e_slot, r_slot = row_slots(e_o, shard), lead_slots(r_o)
    loads = [
        pltpu.make_async_copy(wo, o_slot(me, None), in_sem.at[1]),
        pltpu.make_async_copy(wa, a_slot(me, None), in_sem.at[2]),
        pltpu.make_async_copy(we, stage_e, in_sem.at[3]),
        pltpu.make_async_copy(wr, stage_r, in_sem.at[4]),
    ]
    for load in loads:
        load.start()
    here.greet()
    ga = Gather(here, own_part(wa), a_slot, ga_s, ga_r)
    go = Gather(here, own_part(wo), o_slot, go_s, go_r)
    ge = Gather(here, own_part(we), e_slot, ge_s, ge_r)
    gr = Gather(here, own_part(wr), r_slot, gr_s, gr_r)
    outs = Outs(out_sem)
    to_sib = remote(small, sib_small, sm_s.at[0], sm_r.at[0], here.sib)
    to_sib.start()
    go.start()
    to_sib.wait_recv()
    all_small[here.f] = small[...] + sib_small[...]

    def small_copy(k):
        spot = all_small.at[here.f]
        return remote(spot, spot, sm_s.at[k], sm_r.at[k], here.plane(k))

    def small_landing(k):
        spot = all_small.at[lax.rem(here.f + n_f - k, n_f)]
        return remote(spot, spot, sm_s.at[k], sm_r.at[k], here.plane(k))

    for k in range(1, n_f):
        small_copy(k).start()
    ga.start()
    for load in loads[2:]:
        load.wait()
    outs.put(stage_e, e_slot(me, None))
    outs.put(stage_r, r_slot(me, None))
    for s in range(1, here.m):
        go.step(s)
    for k in range(1, n_f):
        small_landing(k).wait_recv()
    total = all_small[0]
    for k in range(1, n_f):
        total = total + all_small[k]
    par[...] = total
    outs.put(par, par_o)
    tok_in.wait()

    def norm_one(i, _):
        rows = pl.ds(al(i * 64, 64), 64)
        scaled, _spread = norm_rows(tokv[rows, :].astype(F32))
        n1[rows, :] = (scaled * par[0:1, :] + par[1:2, :]).astype(BF)
        return 0

    lax.fori_loop(0, rows_all // 64, norm_one, 0)
    outs.put(n1, n1_o)
    for s in range(1, here.m):
        ga.step(s)
    gr.start()
    ge.start()
    go.step(here.m)
    ga.step(here.m)
    for load in loads[:2]:
        load.wait()
    ga.arrive()
    q[...] = (dot(n1[...], full_a[:, 0:width]) + par[6:7, 0:width]).astype(BF)
    kv[0, :, 0:width] = dot(n1[...], full_a[:, width : 2 * width]).astype(BF)
    kv[0, :, width : 2 * width] = (
        dot(n1[...], full_a[:, 2 * width : 3 * width]) + par[6:7, width : 2 * width]
    ).astype(BF)
    swap = remote(kv.at[0], kv.at[1], kv_s.at[0], kv_r.at[0], here.sib)
    swap.start()
    outs.put(full_a, a_o)
    outs.put(q, q_o)
    go.arrive()
    outs.put(full_o, o_o)
    swap.wait_recv()
    outs.put(kv, kv_o)
    blk = rows_all // 2

    def head(i, _):
        h = i // 2
        rows = pl.ds(al((i - 2 * h) * blk, blk), blk)
        kc = pl.ds(al(h * HD, HD), HD)
        vc = pl.ds(al(width + h * HD, HD), HD)
        ids = col[rows, :]
        qh = q[rows, kc]
        near = allowed_scores(qh, kv[0, :, kc], ids, row[0:1, :], scale)
        far = allowed_scores(qh, kv[1, :, kc], ids, row[1:2, :], scale)
        top = jnp.maximum(
            jnp.max(near, axis=-1, keepdims=True), jnp.max(far, axis=-1, keepdims=True)
        )
        near = jnp.exp(near - top)
        far = jnp.exp(far - top)
        total = jnp.sum(near, axis=-1, keepdims=True) + jnp.sum(far, axis=-1, keepdims=True)
        inv = 1.0 / total
        out = dot((near * inv).astype(BF), kv[0, :, vc]) + dot((far * inv).astype(BF), kv[1, :, vc])
        ctx[rows, kc] = out.astype(BF)
        return 0

    lax.fori_loop(0, 2 * heads, head, 0)
    outs.put(ctx, ctx_o)

    def project(s, _):
        cols = pl.ds(al(s * shard, shard), shard)
        part[:, cols] = dot(ctx[...], full_o[s]).astype(BF)
        return 0

    lax.fori_loop(0, 2 * n_f, project, 0)
    line = Line(here, part, rbuf, norm, (ls_s, ls_r, lg_s, lg_r), chunks, lag)

    def final(rows, span, total):
        middle = tokv[rows, :].astype(F32) + total + par[2:3, :]
        mid[span, :] = middle
        scaled, _spread = norm_rows(middle)
        norm[rows, :] = (scaled * par[3:4, :] + par[4:5, :]).astype(BF)

    ticks = line.ticks()
    events = []
    for s in range(1, here.m):
        events += [functools.partial(gr.step, s), functools.partial(ge.step, s)]
    when = [1 + (ticks // 2) * i // max(1, len(events) - 1) for i in range(len(events))]
    events.append(functools.partial(gr.step, here.m))
    when.append(ticks - 2)

    def tick(tau, _):
        line.tick(tau, final)
        for at, event in zip(when, events):
            pl.when(tau == at)(event)
        return 0

    lax.fori_loop(0, ticks, tick, 0)
    outs.put(mid, mid_o)
    outs.put(norm, n2_o)
    ge.step(here.m)
    gr.arrive()
    ge.arrive()
    line.finish_sum()
    line.finish_back()
    for gather in (ga, go, gr, ge):
        gather.finish()
    to_sib.wait_send()
    for k in range(1, n_f):
        small_copy(k).wait_send()
    swap.wait_send()
    outs.wait()


def forward(n_f, n_t, tok, col, row, small, wa, wo, we, wr, chunks=16, lag=3):
    rows, model = tok.shape
    shard, width, ff = wa.shape[0], wo.shape[0], we.shape[1]
    n_s = 2 * n_f
    sds = jax.ShapeDtypeStruct
    dma = pltpu.SemaphoreType.DMA
    outs = (
        sds((rows, model), BF),
        sds((rows, width), BF),
        sds((2, rows, 2 * width), BF),
        sds((rows, width), BF),
        sds((rows, model), BF),
        sds((rows // 2, model), F32),
        sds((8, model), F32),
        sds((model, 3 * width), BF),
        sds((n_s, width, shard), BF),
        sds((model, ff), BF),
        sds((n_s, ff, shard), BF),
    )
    v = pltpu.VMEM
    return pl.pallas_call(
        functools.partial(forward_kernel, n_f, n_t, chunks, lag),
        out_shape=outs,
        in_specs=[ANY, VM, VM, VM, ANY, ANY, ANY, ANY],
        out_specs=(ANY,) * len(outs),
        scratch_shapes=[
            v((rows, model), BF), v((rows, model), BF), v((model, 3 * width), BF),
            v((n_s, width, shard), BF), v((shard, ff), BF), v((ff, shard), BF),
            v((rows, width), BF), v((2, rows, 2 * width), BF), v((rows, width), BF),
            v((rows, model), BF), v((2, rows // 2, model), BF), v((rows, model), BF),
            v((rows // 2, model), F32), v((8, model), F32), v((n_f, 8, model), F32),
            v((8, model), F32),
        ]
        + [dma((Gather.sems(n_f),))] * 8
        + Line.sems(chunks)
        + [dma((n_f,)), dma((n_f,)), dma((1,)), dma((1,)), dma((5,)), dma((16,))],
        compiler_params=pltpu.CompilerParams(
            collective_id=0, has_side_effects=True, vmem_limit_bytes=60 << 20
        ),
        cost_estimate=pl.CostEstimate(
            flops=8 * 10**9, bytes_accessed=60 * 10**6, transcendentals=10**6
        ),
        name="attention_forward",
    )(tok, col, row, small, wa, wo, we, wr)


def norm_back(grad_normed, scaled, spread, gain):
    weighted = grad_normed * gain
    inner = (
        weighted
        - jnp.mean(weighted, axis=-1, keepdims=True)
        - scaled * jnp.mean(weighted * scaled, axis=-1, keepdims=True)
    )
    return (inner * spread, jnp.sum(grad_normed * scaled, axis=0), jnp.sum(grad_normed, axis=0))


def gelu_exact(values):
    return 0.5 * values * (1.0 + lax.erf(values * (1.0 / math.sqrt(2.0))))


def masked_scores(queries, keys, query_ids, key_ids, scale):
    scores = jnp.einsum("qhd,khd->hqk", queries, keys, preferred_element_type=jnp.float32) * scale
    allowed = key_ids[None, None, :] <= query_ids[None, :, None]
    return jnp.where(allowed, scores, -1e30)


def attend_backward(queries, keys, values, query_ids, key_ids, grad_context, scale):
    scores = masked_scores(queries, keys, query_ids, key_ids, scale)
    probs = jax.nn.softmax(scores, axis=-1)
    grad_probs = jnp.einsum(
        "qhd,khd->hqk", grad_context, values, preferred_element_type=jnp.float32
    )
    inner = jnp.sum(grad_probs * probs, axis=-1, keepdims=True)
    grad_scores = (probs * (grad_probs - inner)).astype(jnp.bfloat16)
    grad_queries = (
        jnp.einsum("hqk,khd->qhd", grad_scores, keys, preferred_element_type=jnp.float32) * scale
    )
    grad_keys = (
        jnp.einsum("hqk,qhd->khd", grad_scores, queries, preferred_element_type=jnp.float32) * scale
    )
    grad_values = jnp.einsum(
        "hqk,qhd->khd", probs.astype(jnp.bfloat16), grad_context, preferred_element_type=jnp.float32
    )
    return (grad_queries, grad_keys, grad_values)


def shifted(block, axis, distance):
    devices = range(lax.axis_size(axis))
    route = [((i - distance) % len(devices), i) for i in devices]
    return lax.ppermute(block, axis, route)


def spread_out(piece, index, count):
    spots = (jnp.arange(count) == index).astype(F32)
    return (piece[:, None, :] * spots[None, :, None]).reshape(piece.shape[0], -1)


def local(
    tokens, cotangent, block_ids, live_count, first_gain, first_shift, query_weight, query_bias,
    key_weight, value_weight, value_bias, output_weight, output_bias, second_gain, second_shift,
    expand_weight, expand_bias, reduce_weight, reduce_bias,
):
    n_f, n_t = lax.axis_size("fsdp"), lax.axis_size("tp")
    n_s = 2 * n_f
    _, rows, model = tokens.shape
    c = lax.axis_index("ctx")
    index = 2 * lax.axis_index("fsdp") + c
    width, ff = query_weight.shape[1], expand_weight.shape[1]
    shard = query_weight.shape[0]
    heads = width // HD
    scale = 1.0 / math.sqrt(HD)
    vectors = jnp.stack(
        [first_gain, first_shift, output_bias, second_gain, second_shift, reduce_bias]
    ).astype(F32)

    def wide(bias):
        full = spread_out(bias.astype(F32), index, n_s)
        flat = full.reshape(1, -1)
        return jnp.pad(flat, ((0, 0), (0, model - flat.shape[1])))

    heads_bias = jnp.concatenate([query_bias, value_bias], axis=0)
    small = jnp.concatenate([spread_out(vectors, index, n_s), wide(heads_bias), wide(expand_bias)])
    ids = block_ids[0].reshape(2, rows)
    near, far = lax.dynamic_index_in_dim(ids, c, 0), lax.dynamic_index_in_dim(ids, 1 - c, 0)
    row = jnp.concatenate([near, far])
    col = near.reshape(rows, 1)
    wa = jnp.concatenate([query_weight, key_weight, value_weight], axis=1)
    tok = tokens.reshape(rows, model)
    n1, q, kv, context_low, n2, mid, par, full_a, full_o, full_e, full_r = forward(
        n_f, n_t, tok, col, row, small, wa, output_weight, expand_weight, reduce_weight
    )
    mids = lax.all_gather(mid, "tp")
    middle = jnp.concatenate([mids[0], mids[n_t - 1]])
    inputs = tok.astype(F32)
    scaled_one, spread_one = norm_rows(inputs)
    scaled_two, spread_two = norm_rows(middle)
    flat_r = full_r.transpose(1, 0, 2).reshape(ff, model)
    flat_o = full_o.transpose(1, 0, 2).reshape(width, model)
    row_live = live_count[0].astype(F32)
    hidden = dot(n2, full_e) + par[7:8, :ff]
    active, gelu_pull = jax.vjp(gelu_exact, hidden)
    active_low = active.astype(BF)
    mlp_term = dot(active_low, flat_r)
    layer_out = ((middle + lax.psum(mlp_term, "tp") + par[5:6]) * row_live).astype(BF)
    grad_out = cotangent.astype(F32).reshape(rows, model) * row_live
    grad_low = grad_out.astype(BF)
    reduce_bias_grad = jnp.sum(grad_out, axis=0)
    reduce_weight_grad = dot_tn(active_low, grad_low)
    grad_hidden = gelu_pull(dot_nt(grad_low, flat_r))[0].astype(BF)
    expand_bias_grad = jnp.sum(grad_hidden.astype(F32), axis=0)
    expand_weight_grad = dot_tn(n2, grad_hidden)
    grad_normed_two = lax.psum(dot_nt(grad_hidden, full_e), "tp")
    norm_part_two, second_gain_grad, second_shift_grad = norm_back(
        grad_normed_two, scaled_two, spread_two, par[3:4]
    )
    grad_middle = grad_out + norm_part_two
    grad_branch = grad_middle.astype(BF)
    output_bias_grad = jnp.sum(grad_branch.astype(F32), axis=0)
    output_weight_grad = dot_tn(context_low, grad_branch)
    grad_context = dot_nt(grad_branch, flat_o).astype(BF)
    hs = (rows, heads, HD)
    keys = kv[:, :, :width].reshape(2 * rows, heads, HD)
    values = kv[:, :, width:].reshape(2 * rows, heads, HD)
    gq, gk, gv = attend_backward(
        q.reshape(hs), keys, values, near[0], row.reshape(-1), grad_context.reshape(hs), scale
    )
    gk, gv = gk.reshape(2 * rows, width), gv.reshape(2 * rows, width)
    back_k = shifted(gk[rows:].astype(BF), "ctx", 1).astype(F32)
    back_v = shifted(gv[rows:].astype(BF), "ctx", 1).astype(F32)
    grads = jnp.concatenate(
        [gq.reshape(rows, width), gk[:rows] + back_k, gv[:rows] + back_v], axis=1
    ).astype(BF)
    sums = jnp.sum(grads.astype(F32), axis=0)
    query_bias_grad, value_bias_grad = sums[:width], sums[2 * width :]
    wa_grad = dot_tn(n1, grads)
    grad_normed_one = lax.psum(dot_nt(grads, full_a), "tp")
    norm_part_one, first_gain_grad, first_shift_grad = norm_back(
        grad_normed_one, scaled_one, spread_one, par[0:1]
    )
    tokens_grad = (grad_middle + norm_part_one).astype(BF)
    both = ("fsdp", "ctx")

    def scatter(value, dim):
        low = value.astype(BF)
        return lax.psum_scatter(low, both, scatter_dimension=dim, tiled=True).astype(F32)

    wa_mine = scatter(wa_grad, 0)
    return (
        layer_out.reshape(1, rows, model),
        tokens_grad.reshape(1, rows, model),
        scatter(first_gain_grad, 0),
        scatter(first_shift_grad, 0),
        wa_mine[:, :width],
        scatter(query_bias_grad.reshape(heads, HD), 1),
        wa_mine[:, width : 2 * width],
        wa_mine[:, 2 * width :],
        scatter(value_bias_grad.reshape(heads, HD), 1),
        scatter(output_weight_grad, 1),
        scatter(output_bias_grad, 0),
        scatter(second_gain_grad, 0),
        scatter(second_shift_grad, 0),
        scatter(expand_weight_grad, 0),
        scatter(expand_bias_grad.reshape(expand_bias.shape[0], -1), 1),
        scatter(reduce_weight_grad, 1),
        scatter(reduce_bias_grad, 0),
    )


def solution(mesh):
    tokens, vector = P("fsdp", "ctx", None), P(("fsdp", "ctx"))
    down, across = P(("fsdp", "ctx"), "tp"), P("tp", ("fsdp", "ctx"))
    return jax.shard_map(
        local,
        mesh=mesh,
        in_specs=(
            tokens, tokens, P("fsdp", None), P("fsdp"), vector, vector, down, across, down, down,
            across, across, vector, vector, vector, down, across, across, vector,
        ),
        out_specs=(
            tokens, tokens, vector, vector, down, across, down, down, across, across, vector,
            vector, vector, down, across, across, vector,
        ),
        check_vma=False,
    )
```

```python
import functools
import math

import jax
import jax.numpy as jnp
from jax import lax
from jax.experimental import pallas as pl
from jax.experimental.pallas import tpu as pltpu
from jax.sharding import PartitionSpec as P

HD = 128
NEG = -1e30
MESH = pl.DeviceIdType.MESH
ANY = pl.BlockSpec(memory_space=pl.ANY)
VM = pl.BlockSpec(memory_space=pltpu.VMEM)
BF = jnp.bfloat16
F32 = jnp.float32
epsilon = 1e-05


def dot(left, right):
    return lax.dot_general(left, right, (((1,), (0,)), ((), ())), preferred_element_type=F32)


def dot_nt(left, right):
    return lax.dot_general(left, right, (((1,), (1,)), ((), ())), preferred_element_type=F32)


def dot_tn(left, right):
    return lax.dot_general(left, right, (((0,), (0,)), ((), ())), preferred_element_type=F32)


def al(value, step):
    return pl.multiple_of(value, step)


class Place:
    def __init__(self, n_f, n_t):
        self.n_f, self.n_t, self.m = n_f, n_t, n_f // 2
        self.f = lax.axis_index("fsdp")
        self.c = lax.axis_index("ctx")
        self.t = lax.axis_index("tp")
        self.p = self.spot(self.f)
        self.side = self.t // (n_t - 1)
        self.right = (self.owner(1), self.c, self.t)
        self.left = (self.owner(-1), self.c, self.t)
        self.sib = (self.f, 1 - self.c, self.t)

    def spot(self, g):
        a = g // self.m
        return (1 - a) * g + a * (self.n_f - 1 + self.m - g)

    def owner(self, k):
        return self.spot(lax.rem(self.p + k + self.n_f, self.n_f))

    def shard(self, k, other=False):
        c = 1 - self.c if other else self.c
        return 2 * self.owner(k) + c

    def tp(self, d):
        return (self.f, self.c, lax.rem(self.t + d + self.n_t, self.n_t))

    def plane(self, k):
        return (lax.rem(self.f + k, self.n_f), self.c, self.t)

    def greet_signal(self):
        bar = pltpu.get_barrier_semaphore()
        others = [self.sib] + [self.plane(k) for k in range(1, self.n_f)]
        others += [self.tp(k) for k in range(1, self.n_t)]
        for other in others:
            pl.semaphore_signal(bar, 1, device_id=other, device_id_type=MESH)

    def greet_wait(self):
        pl.semaphore_wait(pltpu.get_barrier_semaphore(), self.n_f + self.n_t - 1)

    def greet(self):
        self.greet_signal()
        self.greet_wait()


def remote(src, dst, send, recv, to):
    return pltpu.make_async_remote_copy(
        src_ref=src, dst_ref=dst, send_sem=send, recv_sem=recv, device_id=to, device_id_type=MESH
    )


class Gather:
    def __init__(self, here, own, slot, send, recv):
        self.here, self.own, self.slot, self.send, self.recv = here, own, slot, send, recv
        self.m = here.m

    def half(self, way, s):
        return None if s < self.m else way

    def hop(self, way, s):
        here, sign = self.here, (-1, 1)[way]
        part = self.half(way, s)
        idx = here.shard(sign * (s - 1))
        src = self.own(part) if s == 1 else self.slot(idx, part)
        k = way * self.m + s - 1
        to = (here.right, here.left)[way]
        return remote(src, self.slot(idx, part), self.send.at[k], self.recv.at[k], to)

    def landing(self, way, s):
        here, sign = self.here, (-1, 1)[way]
        part = self.half(way, s)
        ref = self.slot(here.shard(sign * s), part)
        k = way * self.m + s - 1
        to = (here.right, here.left)[way]
        return remote(ref, ref, self.send.at[k], self.recv.at[k], to)

    def cross(self, k, offset, other=False):
        here = self.here
        ref = self.slot(here.shard(offset, other), None)
        src = self.own(None) if (offset == 0 and not other) else ref
        n = 2 * self.m + k
        return remote(src, ref, self.send.at[n], self.recv.at[n], here.sib)

    def crossings(self):
        found = [(0, 0)]
        for s in range(1, self.m):
            found += [(2 * s - 1, -s), (2 * s, s)]
        return found + [(2 * self.m - 1, self.m)]

    def start(self):
        self.hop(0, 1).start()
        self.hop(1, 1).start()
        self.cross(0, 0).start()

    def step(self, s):
        self.landing(0, s).wait_recv()
        self.landing(1, s).wait_recv()
        if s < self.m:
            self.hop(0, s + 1).start()
            self.hop(1, s + 1).start()
            self.cross(2 * s - 1, -s).start()
            self.cross(2 * s, s).start()
        else:
            self.cross(2 * self.m - 1, self.m).start()

    def arrive(self):
        for k, offset in self.crossings():
            self.cross(k, offset, True).wait_recv()

    def finish(self):
        for s in range(1, self.m + 1):
            self.hop(0, s).wait_send()
            self.hop(1, s).wait_send()
        for k, offset in self.crossings():
            self.cross(k, offset).wait_send()

    @staticmethod
    def sems(n_f):
        return 2 * n_f


class Line:
    def __init__(self, here, part, rbuf, norm, sems, chunks, lag):
        self.here, self.part, self.rbuf, self.norm = here, part, rbuf, norm
        self.s_send, self.s_recv, self.g_send, self.g_recv = sems
        self.half = part.shape[0] // 2
        self.nc, self.lag = chunks, lag
        self.cr = self.half // chunks

    def rows(self, d, j):
        return pl.ds(al(d * self.half + j * self.cr, self.cr), self.cr)

    def span(self, j):
        return pl.ds(al(j * self.cr, self.cr), self.cr)

    def s_copy(self, d, j):
        return remote(
            self.part.at[self.rows(d, j)],
            self.rbuf.at[d, self.span(j)],
            self.s_send.at[d, j],
            self.s_recv.at[d, j],
            self.here.tp(2 * d - 1),
        )

    def g_copy(self, d, j):
        ref = self.norm.at[self.rows(d, j)]
        to = self.here.tp(1 - 2 * d)
        return remote(ref, ref, self.g_send.at[d, j], self.g_recv.at[d, j], to)

    def depth(self, d):
        t, n = self.here.t, self.here.n_t
        return t if d == 1 else n - 1 - t

    def sum_step(self, d, tau):
        depth, n = self.depth(d), self.here.n_t
        j = tau - self.lag * depth
        valid = (j >= 0) & (j < self.nc)

        @pl.when(valid & (depth > 0))
        def _():
            self.s_copy(d, j).wait_recv()

        @pl.when(valid & (depth > 0) & (depth < n - 1))
        def _():
            own = self.part[self.rows(d, j), :].astype(F32)
            got = self.rbuf[d, self.span(j), :].astype(F32)
            self.part[self.rows(d, j), :] = (own + got).astype(BF)

        @pl.when(valid & (depth < n - 1))
        def _():
            self.s_copy(d, j).start()

    def owner_step(self, tau, final, back=True):
        here, n = self.here, self.here.n_t
        j = tau - self.lag * (n - 1)
        end = (here.t == 0) | (here.t == n - 1)

        @pl.when(end & (j >= 0) & (j < self.nc))
        def _():
            d = here.side
            rows = self.rows(d, j)
            total = self.part[rows, :].astype(F32) + self.rbuf[d, self.span(j), :].astype(F32)
            final(rows, self.span(j), total)
            if back:
                self.back_copy(j).start()

    def back_copy(self, j):
        here = self.here
        d = here.side
        ref = self.norm.at[self.rows(d, j)]
        return remote(
            ref, ref, self.g_send.at[d, j], self.g_recv.at[d, j], here.tp(1 - 2 * d)
        )

    def gather_step(self, d, tau, base):
        t, n = self.here.t, self.here.n_t
        depth = t if d == 0 else n - 1 - t
        j = tau - base - self.lag * depth
        valid = (j >= 0) & (j < self.nc) & (depth > 0)

        @pl.when(valid)
        def _():
            self.g_copy(d, j).wait_recv()

        @pl.when(valid & (depth < n - 1))
        def _():
            self.g_copy(d, j).start()

    def sum_ticks(self):
        return self.nc + self.lag * (self.here.n_t - 1)

    def ticks(self):
        return self.nc + 2 * self.lag * (self.here.n_t - 1)

    def tick(self, tau, final, back=True):
        self.sum_step(1, tau)
        self.sum_step(0, tau)
        self.owner_step(tau, final, back)
        if back:
            base = self.lag * (self.here.n_t - 1)
            self.gather_step(0, tau, base)
            self.gather_step(1, tau, base)

    def finish_sum(self):
        t, n = self.here.t, self.here.n_t

        def body(j, _):
            @pl.when(t > 0)
            def _():
                self.s_copy(0, j).wait_send()

            @pl.when(t < n - 1)
            def _():
                self.s_copy(1, j).wait_send()

            return 0

        lax.fori_loop(0, self.nc, body, 0)

    def finish_back(self):
        t, n = self.here.t, self.here.n_t

        def body(j, _):
            @pl.when(t < n - 1)
            def _():
                self.g_copy(0, j).wait_send()

            @pl.when(t > 0)
            def _():
                self.g_copy(1, j).wait_send()

            return 0

        lax.fori_loop(0, self.nc, body, 0)

    @staticmethod
    def sems(chunks):
        return [pltpu.SemaphoreType.DMA((2, chunks))] * 4


def norm_rows(values):
    mean = jnp.mean(values, axis=-1, keepdims=True)
    center = values - mean
    spread = lax.rsqrt(jnp.mean(center * center, axis=-1, keepdims=True) + epsilon)
    return center * spread, spread


class Outs:
    def __init__(self, sem):
        self.sem, self.made = sem, []

    def put(self, src, dst):
        copy = pltpu.make_async_copy(src, dst, self.sem.at[len(self.made)])
        copy.start()
        self.made.append(copy)

    def wait(self):
        for copy in self.made:
            copy.wait()


def row_slots(ref, size):
    def slot(idx, part):
        if part is None:
            return ref.at[pl.ds(al(idx * size, size), size)]
        return ref.at[pl.ds(al(idx * size + part * (size // 2), size // 2), size // 2)]

    return slot


def column_slots(ref, width):
    size = ref.shape[0]

    def slot(idx, part):
        cols = pl.ds(al(idx * width, width), width)
        if part is None:
            return ref.at[:, cols]
        return ref.at[pl.ds(part * (size // 2), size // 2), cols]

    return slot


def own_part(ref):
    size = ref.shape[0]

    def own(part):
        if part is None:
            return ref
        return ref.at[pl.ds(part * (size // 2), size // 2)]

    return own


def allowed_scores(q, k, col, row, scale):
    return jnp.where(row <= col, dot_nt(q, k) * scale, NEG)


def forward_kernel(
    n_f, n_t, chunks, lag,
    tok, col, row, small, wa, wo, we, wr,
    n1_o, q_o, kv_o, ctx_o, n2_o, mid_o, par_o, a_o, o_o, e_o, r_o,
    tokv, n1, full_a, full_o, stage_e, stage_r, q, kv, ctx, part, rbuf, norm, mid,
    sib_small, all_small, par,
    ga_s, ga_r, go_s, go_r, ge_s, ge_r, gr_s, gr_r,
    ls_s, ls_r, lg_s, lg_r, sm_s, sm_r, kv_s, kv_r, in_sem, out_sem,
):
    here = Place(n_f, n_t)
    width = wo.shape[0]
    shard = wa.shape[0]
    rows_all, model = n1.shape
    heads = width // HD
    scale = 1.0 / math.sqrt(HD)
    tok_in = pltpu.make_async_copy(tok, tokv, in_sem.at[0])
    tok_in.start()
    me = 2 * here.f + here.c
    a_slot, o_slot = row_slots(full_a, shard), column_slots(full_o, shard)
    e_slot, r_slot = row_slots(e_o, shard), column_slots(r_o, shard)
    loads = [
        pltpu.make_async_copy(wo, o_slot(me, None), in_sem.at[1]),
        pltpu.make_async_copy(wa, a_slot(me, None), in_sem.at[2]),
        pltpu.make_async_copy(we, stage_e, in_sem.at[3]),
        pltpu.make_async_copy(wr, stage_r, in_sem.at[4]),
    ]
    for load in loads:
        load.start()
    here.greet()
    ga = Gather(here, own_part(wa), a_slot, ga_s, ga_r)
    go = Gather(here, own_part(wo), o_slot, go_s, go_r)
    ge = Gather(here, own_part(we), e_slot, ge_s, ge_r)
    gr = Gather(here, own_part(wr), r_slot, gr_s, gr_r)
    outs = Outs(out_sem)
    to_sib = remote(small, sib_small, sm_s.at[0], sm_r.at[0], here.sib)
    to_sib.start()
    go.start()
    to_sib.wait_recv()
    all_small[here.f] = small[...] + sib_small[...]

    def small_copy(k):
        spot = all_small.at[here.f]
        return remote(spot, spot, sm_s.at[k], sm_r.at[k], here.plane(k))

    def small_landing(k):
        spot = all_small.at[lax.rem(here.f + n_f - k, n_f)]
        return remote(spot, spot, sm_s.at[k], sm_r.at[k], here.plane(k))

    for k in range(1, n_f):
        small_copy(k).start()
    ga.start()
    for load in loads[2:]:
        load.wait()
    outs.put(stage_e, e_slot(me, None))
    outs.put(stage_r, r_slot(me, None))
    for s in range(1, here.m):
        go.step(s)
    for k in range(1, n_f):
        small_landing(k).wait_recv()
    total = all_small[0]
    for k in range(1, n_f):
        total = total + all_small[k]
    par[...] = total
    outs.put(par, par_o)
    tok_in.wait()

    def norm_one(i, _):
        rows = pl.ds(al(i * 64, 64), 64)
        scaled, _spread = norm_rows(tokv[rows, :].astype(F32))
        n1[rows, :] = (scaled * par[0:1, :] + par[1:2, :]).astype(BF)
        return 0

    lax.fori_loop(0, rows_all // 64, norm_one, 0)
    outs.put(n1, n1_o)
    for s in range(1, here.m):
        ga.step(s)
    gr.start()
    ge.start()
    go.step(here.m)
    ga.step(here.m)
    for load in loads[:2]:
        load.wait()
    ga.arrive()
    q[...] = (dot(n1[...], full_a[:, 0:width]) + par[6:7, 0:width]).astype(BF)
    kv[0, :, 0:width] = dot(n1[...], full_a[:, width : 2 * width]).astype(BF)
    kv[0, :, width : 2 * width] = (
        dot(n1[...], full_a[:, 2 * width : 3 * width]) + par[6:7, width : 2 * width]
    ).astype(BF)
    swap = remote(kv.at[0], kv.at[1], kv_s.at[0], kv_r.at[0], here.sib)
    swap.start()
    outs.put(full_a, a_o)
    outs.put(q, q_o)
    go.arrive()
    outs.put(full_o, o_o)
    swap.wait_recv()
    outs.put(kv, kv_o)
    blk = rows_all // 2

    def head(i, _):
        h = i // 2
        rows = pl.ds(al((i - 2 * h) * blk, blk), blk)
        kc = pl.ds(al(h * HD, HD), HD)
        vc = pl.ds(al(width + h * HD, HD), HD)
        ids = col[rows, :]
        qh = q[rows, kc]
        near = allowed_scores(qh, kv[0, :, kc], ids, row[0:1, :], scale)
        far = allowed_scores(qh, kv[1, :, kc], ids, row[1:2, :], scale)
        top = jnp.maximum(
            jnp.max(near, axis=-1, keepdims=True), jnp.max(far, axis=-1, keepdims=True)
        )
        near = jnp.exp(near - top)
        far = jnp.exp(far - top)
        total = jnp.sum(near, axis=-1, keepdims=True) + jnp.sum(far, axis=-1, keepdims=True)
        inv = 1.0 / total
        out = dot((near * inv).astype(BF), kv[0, :, vc]) + dot((far * inv).astype(BF), kv[1, :, vc])
        ctx[rows, kc] = out.astype(BF)
        return 0

    lax.fori_loop(0, 2 * heads, head, 0)
    outs.put(ctx, ctx_o)

    wide = model // 4

    def project(i, _):
        cols = pl.ds(al(i * wide, wide), wide)
        part[:, cols] = dot(ctx[...], full_o[:, cols]).astype(BF)
        return 0

    lax.fori_loop(0, 4, project, 0)
    line = Line(here, part, rbuf, norm, (ls_s, ls_r, lg_s, lg_r), chunks, lag)

    def final(rows, span, total):
        middle = tokv[rows, :].astype(F32) + total + par[2:3, :]
        mid[span, :] = middle
        scaled, _spread = norm_rows(middle)
        norm[rows, :] = (scaled * par[3:4, :] + par[4:5, :]).astype(BF)

    ticks = line.ticks()
    events = []
    for s in range(1, here.m):
        events += [functools.partial(gr.step, s), functools.partial(ge.step, s)]
    when = [1 + (ticks // 2) * i // max(1, len(events) - 1) for i in range(len(events))]
    events.append(functools.partial(gr.step, here.m))
    when.append(ticks - 2)

    def tick(tau, _):
        line.tick(tau, final)
        for at, event in zip(when, events):
            pl.when(tau == at)(event)
        return 0

    lax.fori_loop(0, ticks, tick, 0)
    outs.put(mid, mid_o)
    outs.put(norm, n2_o)
    ge.step(here.m)
    gr.arrive()
    ge.arrive()
    line.finish_sum()
    line.finish_back()
    for gather in (ga, go, gr, ge):
        gather.finish()
    to_sib.wait_send()
    for k in range(1, n_f):
        small_copy(k).wait_send()
    swap.wait_send()
    outs.wait()


def forward(n_f, n_t, tok, col, row, small, wa, wo, we, wr, chunks=16, lag=3):
    rows, model = tok.shape
    shard, width, ff = wa.shape[0], wo.shape[0], we.shape[1]
    sds = jax.ShapeDtypeStruct
    dma = pltpu.SemaphoreType.DMA
    outs = (
        sds((rows, model), BF),
        sds((rows, width), BF),
        sds((2, rows, 2 * width), BF),
        sds((rows, width), BF),
        sds((rows, model), BF),
        sds((rows // 2, model), F32),
        sds((8, model), F32),
        sds((model, 3 * width), BF),
        sds((width, model), BF),
        sds((model, ff), BF),
        sds((ff, model), BF),
    )
    v = pltpu.VMEM
    return pl.pallas_call(
        functools.partial(forward_kernel, n_f, n_t, chunks, lag),
        out_shape=outs,
        in_specs=[ANY, VM, VM, VM, ANY, ANY, ANY, ANY],
        out_specs=(ANY,) * len(outs),
        scratch_shapes=[
            v((rows, model), BF), v((rows, model), BF), v((model, 3 * width), BF),
            v((width, model), BF), v((shard, ff), BF), v((ff, shard), BF),
            v((rows, width), BF), v((2, rows, 2 * width), BF), v((rows, width), BF),
            v((rows, model), BF), v((2, rows // 2, model), BF), v((rows, model), BF),
            v((rows // 2, model), F32), v((8, model), F32), v((n_f, 8, model), F32),
            v((8, model), F32),
        ]
        + [dma((Gather.sems(n_f),))] * 8
        + Line.sems(chunks)
        + [dma((n_f,)), dma((n_f,)), dma((1,)), dma((1,)), dma((5,)), dma((16,))],
        compiler_params=pltpu.CompilerParams(
            collective_id=0, has_side_effects=True, vmem_limit_bytes=60 << 20
        ),
        cost_estimate=pl.CostEstimate(
            flops=8 * 10**9, bytes_accessed=60 * 10**6, transcendentals=10**6
        ),
        name="attention_forward",
    )(tok, col, row, small, wa, wo, we, wr)


class Scatter:
    def __init__(self, here, sums, stage, ring_half, ring_full, send, recv, block):
        self.here, self.sums, self.stage = here, sums, stage
        self.ring_half, self.ring_full = ring_half, ring_full
        self.send, self.recv, self.block = send, recv, block
        self.m, self.size = here.m, sums.shape[1]

    def offset(self, i):
        odd = lax.rem(i, 2)
        return self.m + (1 - 2 * odd) * ((i + 1) // 2)

    def shard(self, i, other):
        return self.here.shard(self.offset(i), other)

    def cross(self, i):
        slot = self.sums.at[self.here.owner(self.offset(i))]
        n = 2 * self.m + i
        return remote(self.stage(i), slot, self.send.at[n], self.recv.at[n], self.here.sib)

    def combine(self, i, own):
        f = self.here.owner(self.offset(i))
        self.sums[f] = (own + self.sums[f].astype(F32)).astype(BF)

    def slot(self, k, half):
        f = self.here.owner(k)
        if half is None:
            return self.sums.at[f]
        return self.sums.at[f, pl.ds(half * (self.size // 2), self.size // 2)]

    def hop(self, way, s):
        here, sign = self.here, (1, -1)[way]
        half = way if s == self.m else None
        dst = self.ring_half.at[way] if s == self.m else self.ring_full.at[way, s - 1]
        n = way * self.m + s - 1
        to = (here.right, here.left)[way]
        return remote(self.slot(sign * s, half), dst, self.send.at[n], self.recv.at[n], to)

    def launch(self, s):
        self.hop(0, s).start()
        self.hop(1, s).start()

    def absorb(self, s):
        for way in (0, 1):
            sign = (1, -1)[way]
            self.hop(way, s).wait_recv()
            f = self.here.owner(sign * (s - 1))
            base = way * (self.size // 2) if s == self.m else 0
            count = (self.size // 2 if s == self.m else self.size) // self.block

            def body(i, _, way=way, f=f, base=base):
                there = pl.ds(al(base + i * self.block, self.block), self.block)
                here_rows = pl.ds(al(i * self.block, self.block), self.block)
                if s == self.m:
                    got = self.ring_half[way, here_rows, :]
                else:
                    got = self.ring_full[way, s - 1, here_rows, :]
                self.sums[f, there, :] = (
                    self.sums[f, there, :].astype(F32) + got.astype(F32)
                ).astype(BF)
                return 0

            lax.fori_loop(0, count, body, 0)

    def finish(self, crossed=True):
        for s in range(1, self.m + 1):
            self.hop(0, s).wait_send()
            self.hop(1, s).wait_send()
        if crossed:
            for i in range(2 * self.m):
                self.cross(i).wait_send()

    @staticmethod
    def buffers(n_f, rows, cols):
        v = pltpu.VMEM
        m = n_f // 2
        return [
            v((n_f, rows, cols), BF),
            v((2, rows // 2, cols), BF),
            v((2, max(1, m - 1), rows, cols), BF),
        ]

    @staticmethod
    def sems(n_f):
        return [pltpu.SemaphoreType.DMA((2 * n_f,))] * 2


def norm_back_rows(total, scaled, spread, gain):
    e = total * gain
    inner = (
        e
        - jnp.mean(e, axis=-1, keepdims=True)
        - scaled * jnp.mean(e * scaled, axis=-1, keepdims=True)
    )
    return inner * spread


def span_when(tau, start, stop, task):
    @pl.when((tau >= start) & (tau < stop))
    def _():
        task(tau - start)


def middle_kernel(
    n_f, n_t, chunks, lag,
    live, n2_i, cot, mid_i, par, full_e, full_r,
    gb_o, lo_o, gm_o, eg_o, pr_o, sums_o,
    ev, rv, n2, g, act, gh, part, part2, rbuf, rbuf2, gb, mid, gm, lo, sums,
    e_sum, e_half, e_full, r_sum,
    e_s, e_r, r_s, r_r,
    ls_s, ls_r, lg_s, lg_r, ms_s, ms_r, in_sem, te_sem, tr_sem, out_sem,
):
    here = Place(n_f, n_t)
    rows_all, model = n2.shape
    ff = act.shape[1]
    shard = e_sum.shape[1]
    tiles = 4
    ft = ff // tiles
    here.greet_signal()

    def e_load(i):
        cols = pl.ds(i * ft, ft)
        return pltpu.make_async_copy(full_e.at[:, cols], ev.at[:, cols], te_sem.at[i])

    def r_load(i):
        rows = pl.ds(i * ft, ft)
        return pltpu.make_async_copy(full_r.at[rows], rv.at[rows], tr_sem.at[i])

    loads = [
        pltpu.make_async_copy(n2_i, n2, in_sem.at[0]),
        pltpu.make_async_copy(cot, g, in_sem.at[1]),
        pltpu.make_async_copy(mid_i, mid, in_sem.at[2]),
    ]
    loads[0].start()
    e_load(0).start()
    loads[1].start()
    r_load(0).start()
    for i in range(1, tiles):
        e_load(i).start()
        r_load(i).start()
    loads[2].start()
    alive = live[0].astype(F32)
    loads[0].wait()
    loads[1].wait()
    sums[...] = jnp.zeros_like(sums)

    def mask(i, total):
        rows = pl.ds(al(i * 64, 64), 64)
        value = g[rows, :].astype(F32) * alive
        g[rows, :] = value.astype(BF)
        return total + jnp.sum(value, axis=0, keepdims=True)

    sums[0:1, :] = lax.fori_loop(0, rows_all // 64, mask, jnp.zeros((1, model), F32))

    def hidden_tile(i):
        cols = pl.ds(i * ft, ft)
        e_load(i).wait()
        h = dot(n2[...], ev[:, cols]) + par[7:8, cols]
        r_load(i).wait()
        ga = dot_nt(g[...], rv[cols, :])
        bell = 0.5 * (1.0 + lax.erf(h * (1.0 / math.sqrt(2.0))))
        act[:, cols] = (h * bell).astype(BF)
        slope = bell + h * jnp.exp(-0.5 * h * h) * (1.0 / math.sqrt(2.0 * math.pi))
        low = (ga * slope).astype(BF)
        gh[:, cols] = low
        sums[1:2, cols] = jnp.sum(low.astype(F32), axis=0, keepdims=True)

    for i in range(tiles):
        hidden_tile(i)
    wide = model // 4

    def back_tile(i, _):
        cols = pl.ds(al(i * wide, wide), wide)
        part[:, cols] = dot_nt(gh[...], ev[cols, :]).astype(BF)
        return 0

    lax.fori_loop(0, 4, back_tile, 0)
    loads[2].wait()
    here.greet_wait()
    line = Line(here, part, rbuf, gb, (ls_s, ls_r, lg_s, lg_r), chunks, lag)
    line2 = Line(here, part2, rbuf2, gb, (ms_s, ms_r, None, None), chunks, lag)
    outs = Outs(out_sem)

    def final(rows, span, total):
        scaled, spread = norm_rows(mid[span, :])
        grad = g[rows, :].astype(F32) + norm_back_rows(total, scaled, spread, par[3:4, :])
        gm[span, :] = grad
        gb[rows, :] = grad.astype(BF)
        sums[4:5, :] += jnp.sum(total * scaled, axis=0, keepdims=True)
        sums[5:6, :] += jnp.sum(total, axis=0, keepdims=True)

    def final2(rows, span, total):
        lo[span, :] = ((mid[span, :] + total + par[5:6, :]) * alive).astype(BF)

    def e_stage(i):
        return ev.at[pl.ds(al(i * shard, shard), shard)]

    def r_stage(i):
        return rv.at[:, pl.ds(al(i * shard, shard), shard)]

    def cols_of(i):
        return pl.ds(al(i * shard, shard), shard)

    es = Scatter(here, e_sum, e_stage, e_half, e_full, e_s, e_r, 64)
    rs = Scatter(here, r_sum, r_stage, None, None, r_s, r_r, 256)

    def e_other(i):
        value = dot_tn(n2[:, cols_of(es.shard(i, True))], gh[...])
        ev[pl.ds(al(i * shard, shard), shard), :] = value.astype(BF)
        es.cross(i).start()

    def e_own(i):
        value = dot_tn(n2[:, cols_of(es.shard(i, False))], gh[...])
        es.cross(i).wait_recv()
        es.combine(i, value)

    def mlp(i):
        part2[:, cols_of(i)] = dot(act[...], rv[:, cols_of(i)]).astype(BF)

    def r_other(i):
        value = dot_tn(act[...], g[:, cols_of(rs.shard(i, True))])
        rv[:, cols_of(i)] = value.astype(BF)
        rs.cross(i).start()

    def r_own(i):
        value = dot_tn(act[...], g[:, cols_of(rs.shard(i, False))])
        rs.cross(i).wait_recv()
        rs.combine(i, value)

    n_s = 2 * n_f
    a, b = n_f, 2 * n_f
    d = b + n_s
    ticks = max(line.ticks(), d + 2 * n_f, d + line2.sum_ticks())
    gap = max(1, (ticks - b) // (n_f // 2 + 1))

    def tick(tau, _):
        line.tick(tau, final)
        line2.tick(tau - d, final2, back=False)
        span_when(tau, 0, a, e_other)
        span_when(tau, a, b, e_own)
        span_when(tau, b, d, mlp)
        span_when(tau, d, d + n_f, r_other)
        span_when(tau, d + n_f, d + 2 * n_f, r_own)

        @pl.when(tau == a)
        def _():
            es.launch(here.m)

        for s in range(here.m, 1, -1):

            @pl.when(tau == b + gap * (here.m - s + 1) - 1)
            def _(s=s):
                es.absorb(s)
                es.launch(s - 1)

        return 0

    lax.fori_loop(0, ticks, tick, 0)
    outs.put(gb, gb_o)
    outs.put(gm, gm_o)
    outs.put(lo, lo_o)
    outs.put(r_sum, pr_o)
    outs.put(sums, sums_o)
    es.absorb(1)
    outs.put(e_sum.at[here.f], eg_o)
    line.finish_sum()
    line.finish_back()
    line2.finish_sum()
    es.finish()
    for i in range(n_f):
        rs.cross(i).wait_send()
    outs.wait()


def middle(n_f, n_t, live, n2, cot, mid, par, full_e, full_r, chunks=16, lag=3):
    rows, model = n2.shape
    ff = full_e.shape[1]
    shard = model // (2 * n_f)
    sds, dma, v = jax.ShapeDtypeStruct, pltpu.SemaphoreType.DMA, pltpu.VMEM
    outs = (
        sds((rows, model), BF),
        sds((rows // 2, model), BF),
        sds((rows // 2, model), F32),
        sds((shard, ff), BF),
        sds((n_f, ff, shard), BF),
        sds((8, model), F32),
    )
    return pl.pallas_call(
        functools.partial(middle_kernel, n_f, n_t, chunks, lag),
        out_shape=outs,
        in_specs=[pl.BlockSpec(memory_space=pltpu.SMEM), ANY, ANY, ANY, VM, ANY, ANY],
        out_specs=(ANY,) * len(outs),
        scratch_shapes=[
            v((model, ff), BF), v((ff, model), BF), v((rows, model), BF), v((rows, model), BF),
            v((rows, ff), BF), v((rows, ff), BF), v((rows, model), BF), v((rows, model), BF),
            v((2, rows // 2, model), BF), v((2, rows // 2, model), BF), v((rows, model), BF),
            v((rows // 2, model), F32), v((rows // 2, model), F32), v((rows // 2, model), BF),
            v((8, model), F32),
        ]
        + Scatter.buffers(n_f, shard, ff)
        + [v((n_f, ff, shard), BF)]
        + Scatter.sems(n_f)
        + Scatter.sems(n_f)
        + Line.sems(chunks)
        + Line.sems(chunks)[:2]
        + [dma((3,)), dma((4,)), dma((4,)), dma((6,))],
        compiler_params=pltpu.CompilerParams(
            collective_id=1, has_side_effects=True, vmem_limit_bytes=63 << 20
        ),
        cost_estimate=pl.CostEstimate(
            flops=26 * 10**9, bytes_accessed=40 * 10**6, transcendentals=4 * 10**6
        ),
        name="feed_forward",
    )(live, n2, cot, mid, par, full_e, full_r)


def backward_kernel(
    n_f, n_t, chunks, lag, chunks2, lag2,
    col, row, par, sums_i, tok, gm_i, lo_i, gb_i, ctx_i, q_i, kv_i, n1_i, full_a, full_o, pr_i,
    lo_o, tg_o, rg_o, og_o, ag_o, small_o,
    av, ov, gb, n1, tokh, gm, ctx, q, kv, gc, grads, near_g, far_g, got_g, lof, norm, part, rbuf,
    sm, tp_small, sib_small, all_small,
    r_sum, r_half, r_full, o_sum, o_half, o_full, a_sum, a_half, a_full,
    r_s, r_r, o_s, o_r, a_s, a_r,
    ls_s, ls_r, lg_s, lg_r, ms_s, ms_r, mg_s, mg_r,
    kv_s, kv_r, tp_s, tp_r, sb_s, sb_r, pl_s, pl_r, in_sem, out_sem,
):
    here = Place(n_f, n_t)
    rows_all, model = gb.shape
    width = q.shape[1]
    shard = a_sum.shape[1]
    heads = width // HD
    half = rows_all // 2
    scale = 1.0 / math.sqrt(HD)
    here.greet_signal()
    mine = pl.ds(al(here.side * half, half), half)
    pairs = [
        (gb_i, gb), (full_o, ov), (pr_i, r_sum), (q_i, q), (kv_i, kv), (ctx_i, ctx),
        (full_a, av), (n1_i, n1), (gm_i, gm), (tok.at[mine], tokh),
    ]
    loads = [pltpu.make_async_copy(s, d, in_sem.at[i]) for i, (s, d) in enumerate(pairs)]
    for load in loads:
        load.start()
    end = (here.t == 0) | (here.t == n_t - 1)
    lo_load = pltpu.make_async_copy(lo_i, lof.at[mine], in_sem.at[len(pairs)])
    pl.when(end)(lo_load.start)
    sm[...] = sums_i[...]
    loads[0].wait()
    loads[1].wait()
    gc[...] = dot_nt(gb[...], ov[...]).astype(BF)
    pl.when(end)(lo_load.wait)
    loads[2].wait()
    here.greet_wait()
    outs = Outs(out_sem)
    line = Line(here, part, rbuf, norm, (ls_s, ls_r, lg_s, lg_r), chunks, lag)
    back = Line(here, lof, rbuf, lof, (ms_s, ms_r, mg_s, mg_r), chunks2, lag2)

    @pl.when(end)
    def _():
        def send(j, _):
            back.back_copy(j).start()
            return 0

        lax.fori_loop(0, chunks2, send, 0)

    back_ticks = chunks2 + lag2 * (n_t - 1)

    def back_tick(tau):
        back.gather_step(0, tau, 0)
        back.gather_step(1, tau, 0)

    def cols_of(i):
        return pl.ds(al(i * shard, shard), shard)

    def rows_of(i):
        return pl.ds(al(i * shard, shard), shard)

    rs = Scatter(here, r_sum, None, r_half, r_full, r_s, r_r, 256)
    os = Scatter(here, o_sum, lambda i: ov.at[:, cols_of(i)], o_half, o_full, o_s, o_r, 128)
    sa = Scatter(here, a_sum, lambda i: av.at[rows_of(i)], a_half, a_full, a_s, a_r, 64)
    rs.launch(here.m)
    for load in loads[3:6]:
        load.wait()

    def head(h, _):
        kc = pl.ds(al(h * HD, HD), HD)
        vc = pl.ds(al(width + h * HD, HD), HD)
        ids = col[...]
        qh, gh = q[:, kc], gc[:, kc]
        near = allowed_scores(qh, kv[0, :, kc], ids, row[0:1, :], scale)
        far = allowed_scores(qh, kv[1, :, kc], ids, row[1:2, :], scale)
        top = jnp.maximum(
            jnp.max(near, axis=-1, keepdims=True), jnp.max(far, axis=-1, keepdims=True)
        )
        near = jnp.exp(near - top)
        far = jnp.exp(far - top)
        inv = 1.0 / (
            jnp.sum(near, axis=-1, keepdims=True) + jnp.sum(far, axis=-1, keepdims=True)
        )
        near = near * inv
        far = far * inv
        near_gv = dot_tn(near.astype(BF), gh)
        far_gv = dot_tn(far.astype(BF), gh)
        gp_near = dot_nt(gh, kv[0, :, vc])
        gp_far = dot_nt(gh, kv[1, :, vc])
        inner = jnp.sum(gp_near * near, axis=-1, keepdims=True) + jnp.sum(
            gp_far * far, axis=-1, keepdims=True
        )
        gs_near = (near * (gp_near - inner)).astype(BF)
        gs_far = (far * (gp_far - inner)).astype(BF)
        gq = (dot(gs_near, kv[0, :, kc]) + dot(gs_far, kv[1, :, kc])) * scale
        grads[:, kc] = gq.astype(BF)
        near_g[:, kc] = dot_tn(gs_near, qh) * scale
        far_g[:, kc] = (dot_tn(gs_far, qh) * scale).astype(BF)
        near_g[:, vc] = near_gv
        far_g[:, vc] = far_gv.astype(BF)
        back_tick(2 * h)
        back_tick(2 * h + 1)

        @pl.when(h == heads // 2)
        def _():
            rs.absorb(here.m)
            rs.launch(here.m - 1)

        return 0

    lax.fori_loop(0, heads, head, 0)
    swap = remote(far_g, got_g, kv_s.at[0], kv_r.at[0], here.sib)
    swap.start()
    for s in range(here.m - 1, 1, -1):
        rs.absorb(s)
        rs.launch(s - 1)

    def out_task(i, _):
        value = dot_tn(ctx[...], gb[:, cols_of(os.shard(i, True))])
        ov[:, cols_of(i)] = value.astype(BF)
        os.cross(i).start()
        back_tick(2 * heads + i)
        return 0

    lax.fori_loop(0, n_f, out_task, 0)

    def out_own(i, _):
        value = dot_tn(ctx[...], gb[:, cols_of(os.shard(i, False))])
        os.cross(i).wait_recv()
        os.combine(i, value)
        back_tick(2 * heads + n_f + i)
        return 0

    lax.fori_loop(0, n_f, out_own, 0)
    os.launch(here.m)
    swap.wait_recv()

    def add_rows(i, total):
        rows = pl.ds(al(i * 128, 128), 128)
        low = (near_g[rows, :] + got_g[rows, :].astype(F32)).astype(BF)
        grads[rows, width:] = low
        both = jnp.concatenate([grads[rows, 0:width], low[:, width:]], axis=1).astype(F32)
        return total + jnp.sum(both, axis=0, keepdims=True)

    sm[3:4, 0 : 2 * width] = lax.fori_loop(
        0, rows_all // 128, add_rows, jnp.zeros((1, 2 * width), F32)
    )
    loads[6].wait()
    wide = model // 4

    def back_part(i, _):
        cols = pl.ds(al(i * wide, wide), wide)
        part[:, cols] = dot_nt(grads[...], av[cols, :]).astype(BF)
        return 0

    lax.fori_loop(0, 4, back_part, 0)
    for load in loads[7:]:
        load.wait()

    def final(rows, span, total):
        scaled, spread = norm_rows(tokh[span, :].astype(F32))
        grad = gm[span, :] + norm_back_rows(total, scaled, spread, par[0:1, :])
        norm[rows, :] = grad.astype(BF)
        sm[6:7, :] += jnp.sum(total * scaled, axis=0, keepdims=True)
        sm[7:8, :] += jnp.sum(total, axis=0, keepdims=True)

    def a_other(i):
        value = dot_tn(n1[:, cols_of(sa.shard(i, True))], grads[...])
        av[rows_of(i), :] = value.astype(BF)
        sa.cross(i).start()

    def a_own(i):
        value = dot_tn(n1[:, cols_of(sa.shard(i, False))], grads[...])
        sa.cross(i).wait_recv()
        sa.combine(i, value)

    def branch_sum(i):
        rows = pl.ds(al(i * 64, 64), 64)
        sm[2:3, :] += jnp.sum(gb[rows, :].astype(F32), axis=0, keepdims=True)

    sm[2:3, :] = jnp.zeros((1, model), F32)
    blocks = rows_all // 64
    d = 2 * n_f
    ticks = max(line.ticks(), d + blocks)
    plan = [(d, lambda: rs.absorb(1))]
    room = ticks - d
    for s in range(here.m, 1, -1):
        k = here.m - s
        spots = here.m - 1
        plan.append((d + 2 + (room * k) // (2 * spots), functools.partial(ring_step, os, s)))
        plan.append((d + room // 4 + (room * k) // (2 * spots), functools.partial(ring_step, sa, s)))

    def tick(tau, _):
        line.tick(tau, final)
        span_when(tau, 0, n_f, a_other)
        span_when(tau, n_f, d, a_own)
        span_when(tau, d, d + blocks, branch_sum)
        pl.when(tau == n_f)(lambda: sa.launch(here.m))
        for at, event in plan:
            pl.when(tau == at)(event)
        return 0

    lax.fori_loop(0, ticks, tick, 0)
    outs.put(norm, tg_o)
    outs.put(r_sum.at[here.f], rg_o)

    def rest(tau, _):
        back_tick(tau)
        return 0

    lax.fori_loop(min(2 * heads + 2 * n_f, back_ticks), back_ticks, rest, 0)
    outs.put(lof, lo_o)

    def tp_copy(k):
        spot = tp_small.at[here.side]
        return remote(sm, spot, tp_s.at[k - 1], tp_r.at[here.side], here.tp(k))

    @pl.when(end)
    def _():
        for k in range(1, n_t):
            tp_copy(k).start()

    def tp_landing(side):
        spot = tp_small.at[side]
        return remote(sm, spot, tp_s.at[0], tp_r.at[side], here.tp(1))

    @pl.when(here.t != 0)
    def _():
        tp_landing(0).wait_recv()

    @pl.when(here.t != n_t - 1)
    def _():
        tp_landing(1).wait_recv()

    @pl.when(end)
    def _():
        tp_small[here.side] = sm[...]

    top_rows = lax.broadcasted_iota(jnp.int32, (8, model), 0) < 4
    all_small[here.f] = jnp.where(top_rows, sm[...], tp_small[0] + tp_small[1])
    to_sib = remote(all_small.at[here.f], sib_small, sb_s.at[0], sb_r.at[0], here.sib)
    to_sib.start()
    to_sib.wait()
    all_small[here.f] += sib_small[...]

    def plane_copy(k):
        spot = all_small.at[here.f]
        return remote(spot, spot, pl_s.at[k], pl_r.at[k], here.plane(k))

    def plane_landing(k):
        spot = all_small.at[lax.rem(here.f + n_f - k, n_f)]
        return remote(spot, spot, pl_s.at[k], pl_r.at[k], here.plane(k))

    for k in range(1, n_f):
        plane_copy(k).start()
    os.absorb(1)
    outs.put(o_sum.at[here.f], og_o)
    sa.absorb(1)
    outs.put(a_sum.at[here.f], ag_o)
    for k in range(1, n_f):
        plane_landing(k).wait_recv()
    total = all_small[0]
    for k in range(1, n_f):
        total = total + all_small[k]
    sib_small[...] = total
    outs.put(sib_small, small_o)
    line.finish_sum()
    line.finish_back()
    back.finish_back()
    rs.finish(False)
    os.finish()
    sa.finish()
    swap.wait_send()

    @pl.when(end)
    def _():
        for k in range(1, n_t):
            tp_copy(k).wait_send()

    for k in range(1, n_f):
        plane_copy(k).wait_send()
    outs.wait()


def ring_step(scatter, s):
    scatter.absorb(s)
    scatter.launch(s - 1)


def backward(
    n_f, n_t, col, row, par, sums, tok, gm, lo, gb, ctx, q, kv, n1, full_a, full_o, pr,
    chunks=16, lag=3, chunks2=8, lag2=2,
):
    rows, model = gb.shape
    width, ff = q.shape[1], pr.shape[1]
    shard = model // (2 * n_f)
    sds, dma, v = jax.ShapeDtypeStruct, pltpu.SemaphoreType.DMA, pltpu.VMEM
    outs = (
        sds((rows, model), BF),
        sds((rows, model), BF),
        sds((ff, shard), BF),
        sds((width, shard), BF),
        sds((shard, 3 * width), BF),
        sds((8, model), F32),
    )
    return pl.pallas_call(
        functools.partial(backward_kernel, n_f, n_t, chunks, lag, chunks2, lag2),
        out_shape=outs,
        in_specs=[VM] * 4 + [ANY] * 11,
        out_specs=(ANY,) * len(outs),
        scratch_shapes=[
            v((model, 3 * width), BF), v((width, model), BF), v((rows, model), BF),
            v((rows, model), BF), v((rows // 2, model), BF), v((rows // 2, model), F32),
            v((rows, width), BF), v((rows, width), BF), v((2, rows, 2 * width), BF),
            v((rows, width), BF), v((rows, 3 * width), BF), v((rows, 2 * width), F32),
            v((rows, 2 * width), BF), v((rows, 2 * width), BF), v((rows, model), BF),
            v((rows, model), BF), v((rows, model), BF), v((2, rows // 2, model), BF),
            v((8, model), F32), v((2, 8, model), F32), v((8, model), F32),
            v((n_f, 8, model), F32),
        ]
        + Scatter.buffers(n_f, ff, shard)
        + Scatter.buffers(n_f, width, shard)
        + Scatter.buffers(n_f, shard, 3 * width)
        + Scatter.sems(n_f) * 3
        + Line.sems(chunks)
        + Line.sems(chunks2)
        + [dma((1,)), dma((1,)), dma((n_t - 1,)), dma((2,)), dma((1,)), dma((1,))]
        + [dma((n_f,)), dma((n_f,)), dma((11,)), dma((6,))],
        compiler_params=pltpu.CompilerParams(
            collective_id=2, has_side_effects=True, vmem_limit_bytes=63 << 20
        ),
        cost_estimate=pl.CostEstimate(
            flops=14 * 10**9, bytes_accessed=40 * 10**6, transcendentals=4 * 10**6
        ),
        name="attention_backward",
    )(col, row, par, sums, tok, gm, lo, gb, ctx, q, kv, n1, full_a, full_o, pr)


def spread_out(piece, index, count):
    spots = (jnp.arange(count) == index).astype(F32)
    return (piece[:, None, :] * spots[None, :, None]).reshape(piece.shape[0], -1)


def local(
    tokens, cotangent, block_ids, live_count, first_gain, first_shift, query_weight, query_bias,
    key_weight, value_weight, value_bias, output_weight, output_bias, second_gain, second_shift,
    expand_weight, expand_bias, reduce_weight, reduce_bias,
):
    n_f, n_t = lax.axis_size("fsdp"), lax.axis_size("tp")
    n_s = 2 * n_f
    _, rows, model = tokens.shape
    c = lax.axis_index("ctx")
    index = 2 * lax.axis_index("fsdp") + c
    width, ff = query_weight.shape[1], expand_weight.shape[1]
    shard = query_weight.shape[0]
    vectors = jnp.stack(
        [first_gain, first_shift, output_bias, second_gain, second_shift, reduce_bias]
    ).astype(F32)

    def wide(bias):
        full = spread_out(bias.astype(F32), index, n_s)
        flat = full.reshape(1, -1)
        return jnp.pad(flat, ((0, 0), (0, model - flat.shape[1])))

    heads_bias = jnp.concatenate([query_bias, value_bias], axis=0)
    small = jnp.concatenate([spread_out(vectors, index, n_s), wide(heads_bias), wide(expand_bias)])
    ids = block_ids[0].reshape(2, rows)
    near, far = lax.dynamic_index_in_dim(ids, c, 0), lax.dynamic_index_in_dim(ids, 1 - c, 0)
    row = jnp.concatenate([near, far])
    col = near.reshape(rows, 1)
    wa = jnp.concatenate([query_weight, key_weight, value_weight], axis=1)
    tok = tokens.reshape(rows, model)
    n1, q, kv, ctx, n2, mid, par, full_a, full_o, full_e, full_r = forward(
        n_f, n_t, tok, col, row, small, wa, output_weight, expand_weight, reduce_weight
    )
    gb, lo, gm, e_grad, r_part, sums = middle(
        n_f, n_t, live_count, n2, cotangent.reshape(rows, model), mid, par, full_e, full_r
    )
    layer_out, tokens_grad, r_grad, o_grad, a_grad, total = backward(
        n_f, n_t, col, row, par, sums, tok, gm, lo, gb, ctx, q, kv, n1, full_a, full_o, r_part
    )

    def vector(k):
        return lax.dynamic_slice_in_dim(total[k], index * shard, shard)

    def across(flat, like):
        whole = flat.reshape(like.shape[0], -1)
        return lax.dynamic_slice_in_dim(whole, index * like.shape[1], like.shape[1], 1)

    a_grad = a_grad.astype(F32)
    return (
        layer_out.reshape(1, rows, model),
        tokens_grad.reshape(1, rows, model),
        vector(6),
        vector(7),
        a_grad[:, :width],
        across(total[3, :width], query_bias),
        a_grad[:, width : 2 * width],
        a_grad[:, 2 * width :],
        across(total[3, width : 2 * width], value_bias),
        o_grad.astype(F32),
        vector(2),
        vector(4),
        vector(5),
        e_grad.astype(F32),
        across(total[1, :ff], expand_bias),
        r_grad.astype(F32),
        vector(0),
    )


def solution(mesh):
    tokens, vector = P("fsdp", "ctx", None), P(("fsdp", "ctx"))
    down, across = P(("fsdp", "ctx"), "tp"), P("tp", ("fsdp", "ctx"))
    return jax.shard_map(
        local,
        mesh=mesh,
        in_specs=(
            tokens, tokens, P("fsdp", None), P("fsdp"), vector, vector, down, across, down, down,
            across, across, vector, vector, vector, down, across, across, vector,
        ),
        out_specs=(
            tokens, tokens, vector, vector, down, across, down, down, across, across, vector,
            vector, vector, down, across, across, vector,
        ),
        check_vma=False,
    )
```

```python
import functools
import math

import jax
import jax.numpy as jnp
from jax import lax
from jax.experimental import pallas as pl
from jax.experimental.pallas import tpu as pltpu
from jax.sharding import PartitionSpec as P

HD = 128
NEG = -1e30
MESH = pl.DeviceIdType.MESH
ANY = pl.BlockSpec(memory_space=pl.ANY)
HBM = pl.BlockSpec(memory_space=pltpu.HBM)
VM = pl.BlockSpec(memory_space=pltpu.VMEM)
BF = jnp.bfloat16
F32 = jnp.float32
epsilon = 1e-05


def dot(left, right):
    return lax.dot_general(left, right, (((1,), (0,)), ((), ())), preferred_element_type=F32)


def dot_nt(left, right):
    return lax.dot_general(left, right, (((1,), (1,)), ((), ())), preferred_element_type=F32)


def dot_tn(left, right):
    return lax.dot_general(left, right, (((0,), (0,)), ((), ())), preferred_element_type=F32)


def al(value, step):
    return pl.multiple_of(value, step)


class Place:
    def __init__(self, n_f, n_t):
        self.n_f, self.n_t, self.m = n_f, n_t, n_f // 2
        self.f = lax.axis_index("fsdp")
        self.c = lax.axis_index("ctx")
        self.t = lax.axis_index("tp")
        self.p = self.spot(self.f)
        self.side = self.t // (n_t - 1)
        self.right = (self.owner(1), self.c, self.t)
        self.left = (self.owner(-1), self.c, self.t)
        self.sib = (self.f, 1 - self.c, self.t)

    def spot(self, g):
        a = g // self.m
        return (1 - a) * g + a * (self.n_f - 1 + self.m - g)

    def owner(self, k):
        return self.spot(lax.rem(self.p + k + self.n_f, self.n_f))

    def shard(self, k, other=False):
        c = 1 - self.c if other else self.c
        return 2 * self.owner(k) + c

    def tp(self, d):
        return (self.f, self.c, lax.rem(self.t + d + self.n_t, self.n_t))

    def plane(self, k):
        return (lax.rem(self.f + k, self.n_f), self.c, self.t)

    def greet_signal(self):
        bar = pltpu.get_barrier_semaphore()
        others = [self.sib] + [self.plane(k) for k in range(1, self.n_f)]
        others += [self.tp(k) for k in range(1, self.n_t)]
        for other in others:
            pl.semaphore_signal(bar, 1, device_id=other, device_id_type=MESH)

    def greet_wait(self):
        pl.semaphore_wait(pltpu.get_barrier_semaphore(), self.n_f + self.n_t - 1)

    def greet(self):
        self.greet_signal()
        self.greet_wait()


def remote(src, dst, send, recv, to):
    return pltpu.make_async_remote_copy(
        src_ref=src, dst_ref=dst, send_sem=send, recv_sem=recv, device_id=to, device_id_type=MESH
    )


class Gather:
    def __init__(self, here, own, slot, send, recv):
        self.here, self.own, self.slot, self.send, self.recv = here, own, slot, send, recv
        self.m = here.m

    def half(self, way, s):
        return None if s < self.m else way

    def hop(self, way, s):
        here, sign = self.here, (-1, 1)[way]
        part = self.half(way, s)
        idx = here.shard(sign * (s - 1))
        src = self.own(part) if s == 1 else self.slot(idx, part)
        k = way * self.m + s - 1
        to = (here.right, here.left)[way]
        return remote(src, self.slot(idx, part), self.send.at[k], self.recv.at[k], to)

    def landing(self, way, s):
        here, sign = self.here, (-1, 1)[way]
        part = self.half(way, s)
        ref = self.slot(here.shard(sign * s), part)
        k = way * self.m + s - 1
        to = (here.right, here.left)[way]
        return remote(ref, ref, self.send.at[k], self.recv.at[k], to)

    def cross(self, k, offset, other=False):
        here = self.here
        ref = self.slot(here.shard(offset, other), None)
        src = self.own(None) if (offset == 0 and not other) else ref
        n = 2 * self.m + k
        return remote(src, ref, self.send.at[n], self.recv.at[n], here.sib)

    def crossings(self):
        found = [(0, 0)]
        for s in range(1, self.m):
            found += [(2 * s - 1, -s), (2 * s, s)]
        return found + [(2 * self.m - 1, self.m)]

    def start(self):
        self.hop(0, 1).start()
        self.hop(1, 1).start()
        self.cross(0, 0).start()

    def step(self, s):
        self.landing(0, s).wait_recv()
        self.landing(1, s).wait_recv()
        if s < self.m:
            self.hop(0, s + 1).start()
            self.hop(1, s + 1).start()
            self.cross(2 * s - 1, -s).start()
            self.cross(2 * s, s).start()
        else:
            self.cross(2 * self.m - 1, self.m).start()

    def arrive(self):
        for k, offset in self.crossings():
            self.cross(k, offset, True).wait_recv()

    def finish(self):
        for s in range(1, self.m + 1):
            self.hop(0, s).wait_send()
            self.hop(1, s).wait_send()
        for k, offset in self.crossings():
            self.cross(k, offset).wait_send()

    @staticmethod
    def sems(n_f):
        return 2 * n_f


class Line:
    def __init__(self, here, part, rbuf, norm, sems, chunks, lag):
        self.here, self.part, self.rbuf, self.norm = here, part, rbuf, norm
        self.s_send, self.s_recv, self.g_send, self.g_recv = sems
        self.half = part.shape[0] // 2
        self.nc, self.lag = chunks, lag
        self.cr = self.half // chunks

    def rows(self, d, j):
        return pl.ds(al(d * self.half + j * self.cr, self.cr), self.cr)

    def span(self, j):
        return pl.ds(al(j * self.cr, self.cr), self.cr)

    def s_copy(self, d, j):
        return remote(
            self.part.at[self.rows(d, j)],
            self.rbuf.at[d, self.span(j)],
            self.s_send.at[d, j],
            self.s_recv.at[d, j],
            self.here.tp(2 * d - 1),
        )

    def g_copy(self, d, j):
        ref = self.norm.at[self.rows(d, j)]
        to = self.here.tp(1 - 2 * d)
        return remote(ref, ref, self.g_send.at[d, j], self.g_recv.at[d, j], to)

    def depth(self, d):
        t, n = self.here.t, self.here.n_t
        return t if d == 1 else n - 1 - t

    def sum_step(self, d, tau):
        depth, n = self.depth(d), self.here.n_t
        j = tau - self.lag * depth
        valid = (j >= 0) & (j < self.nc)

        @pl.when(valid & (depth > 0))
        def _():
            self.s_copy(d, j).wait_recv()

        @pl.when(valid & (depth > 0) & (depth < n - 1))
        def _():
            own = self.part[self.rows(d, j), :].astype(F32)
            got = self.rbuf[d, self.span(j), :].astype(F32)
            self.part[self.rows(d, j), :] = (own + got).astype(BF)

        @pl.when(valid & (depth < n - 1))
        def _():
            self.s_copy(d, j).start()

    def owner_step(self, tau, final, back=True):
        here, n = self.here, self.here.n_t
        j = tau - self.lag * (n - 1)
        end = (here.t == 0) | (here.t == n - 1)

        @pl.when(end & (j >= 0) & (j < self.nc))
        def _():
            d = here.side
            rows = self.rows(d, j)
            total = self.part[rows, :].astype(F32) + self.rbuf[d, self.span(j), :].astype(F32)
            final(rows, self.span(j), total)
            if back:
                self.back_copy(j).start()

    def back_copy(self, j):
        here = self.here
        d = here.side
        ref = self.norm.at[self.rows(d, j)]
        return remote(
            ref, ref, self.g_send.at[d, j], self.g_recv.at[d, j], here.tp(1 - 2 * d)
        )

    def gather_step(self, d, tau, base):
        t, n = self.here.t, self.here.n_t
        depth = t if d == 0 else n - 1 - t
        j = tau - base - self.lag * depth
        valid = (j >= 0) & (j < self.nc) & (depth > 0)

        @pl.when(valid)
        def _():
            self.g_copy(d, j).wait_recv()

        @pl.when(valid & (depth < n - 1))
        def _():
            self.g_copy(d, j).start()

    def sum_ticks(self):
        return self.nc + self.lag * (self.here.n_t - 1)

    def ticks(self):
        return self.nc + 2 * self.lag * (self.here.n_t - 1)

    def tick(self, tau, final, back=True):
        self.sum_step(1, tau)
        self.sum_step(0, tau)
        self.owner_step(tau, final, back)
        if back:
            base = self.lag * (self.here.n_t - 1)
            self.gather_step(0, tau, base)
            self.gather_step(1, tau, base)

    def finish_sum(self):
        t, n = self.here.t, self.here.n_t

        def body(j, _):
            @pl.when(t > 0)
            def _():
                self.s_copy(0, j).wait_send()

            @pl.when(t < n - 1)
            def _():
                self.s_copy(1, j).wait_send()

            return 0

        lax.fori_loop(0, self.nc, body, 0)

    def finish_back(self):
        t, n = self.here.t, self.here.n_t

        def body(j, _):
            @pl.when(t < n - 1)
            def _():
                self.g_copy(0, j).wait_send()

            @pl.when(t > 0)
            def _():
                self.g_copy(1, j).wait_send()

            return 0

        lax.fori_loop(0, self.nc, body, 0)

    @staticmethod
    def sems(chunks):
        return [pltpu.SemaphoreType.DMA((2, chunks))] * 4


def norm_rows(values):
    mean = jnp.mean(values, axis=-1, keepdims=True)
    center = values - mean
    spread = lax.rsqrt(jnp.mean(center * center, axis=-1, keepdims=True) + epsilon)
    return center * spread, spread


class Outs:
    def __init__(self, sem):
        self.sem, self.made = sem, []

    def put(self, src, dst):
        copy = pltpu.make_async_copy(src, dst, self.sem.at[len(self.made)])
        copy.start()
        self.made.append(copy)

    def wait(self):
        for copy in self.made:
            copy.wait()


def row_slots(ref, size):
    def slot(idx, part):
        if part is None:
            return ref.at[pl.ds(al(idx * size, size), size)]
        return ref.at[pl.ds(al(idx * size + part * (size // 2), size // 2), size // 2)]

    return slot


def column_slots(ref, width):
    size = ref.shape[0]

    def slot(idx, part):
        cols = pl.ds(al(idx * width, width), width)
        if part is None:
            return ref.at[:, cols]
        return ref.at[pl.ds(part * (size // 2), size // 2), cols]

    return slot


def own_part(ref):
    size = ref.shape[0]

    def own(part):
        if part is None:
            return ref
        return ref.at[pl.ds(part * (size // 2), size // 2)]

    return own


def place_ids(ids, col, row, here):
    rows = col.shape[0]
    row[0:1, :] = ids[:, pl.ds(al(here.c * rows, rows), rows)].astype(F32)
    row[1:2, :] = ids[:, pl.ds(al((1 - here.c) * rows, rows), rows)].astype(F32)
    step = 128

    def turn(i, _):
        start = al(i * step, step)
        down = lax.broadcasted_iota(jnp.int32, (step, rows), 0) + start
        along = lax.broadcasted_iota(jnp.int32, (step, rows), 1)
        kept = jnp.where(down == along, row[0:1, :], 0.0)
        col[pl.ds(start, step), :] = jnp.sum(kept, axis=1, keepdims=True)
        return 0

    lax.fori_loop(0, rows // step, turn, 0)


def picker(index, piece, count):
    down = lax.broadcasted_iota(jnp.int32, (piece, piece * count), 0) + index * piece
    return jnp.where(down == lax.broadcasted_iota(jnp.int32, (piece, piece * count), 1), 1.0, 0.0)


def allowed_scores(q, k, col, row, scale):
    return jnp.where(row <= col, dot_nt(q, k) * scale, NEG)


def forward_kernel(
    n_f, n_t, chunks, lag,
    tok, ids, g1, s1, b_o, g2, s2, b_r, b_q, b_v, b_e, wq, wk, wv, wo, we, wr,
    n1_o, q_o, kv_o, ctx_o, n2_o, mid_o, par_o, a_o, o_o, e_o, r_o,
    tokv, n1, full_a, full_o, stage_e, stage_r, q, kv, ctx, part, rbuf, norm, mid,
    col, row, small, sib_small, all_small, par,
    ga_s, ga_r, go_s, go_r, ge_s, ge_r, gr_s, gr_r,
    ls_s, ls_r, lg_s, lg_r, sm_s, sm_r, kv_s, kv_r, in_sem, out_sem,
):
    here = Place(n_f, n_t)
    width = wo.shape[0]
    shard = wq.shape[0]
    rows_all, model = n1.shape
    heads = width // HD
    scale = 1.0 / math.sqrt(HD)
    tok_in = pltpu.make_async_copy(tok, tokv, in_sem.at[0])
    tok_in.start()
    me = 2 * here.f + here.c
    a_slot, o_slot = row_slots(full_a, shard), column_slots(full_o, shard)
    e_slot, r_slot = row_slots(e_o, shard), column_slots(r_o, shard)
    loads = [
        pltpu.make_async_copy(wo, o_slot(me, None), in_sem.at[1]),
        pltpu.make_async_copy(we, stage_e, in_sem.at[2]),
        pltpu.make_async_copy(wr, stage_r, in_sem.at[3]),
    ]
    mine = pl.ds(al(me * shard, shard), shard)
    for k, w in enumerate((wq, wk, wv)):
        spot = full_a.at[mine, pl.ds(k * width, width)]
        loads.append(pltpu.make_async_copy(w, spot, in_sem.at[4 + k]))
    for load in loads[3:] + loads[:3]:
        load.start()
    here.greet_signal()
    small[...] = jnp.zeros_like(small)
    for k, vector in enumerate((g1, s1, b_o, g2, s2, b_r)):
        small[k : k + 1, mine] = vector[...].astype(F32).reshape(1, shard)

    def put_bias(bias, line, base):
        count, piece = bias.shape
        wide = dot(bias[...].astype(F32), picker(me, piece, 2 * n_f))
        size = piece * 2 * n_f
        for h in range(count):
            small[line : line + 1, base + h * size : base + (h + 1) * size] = wide[h : h + 1, :]

    put_bias(b_q, 6, 0)
    put_bias(b_v, 6, width)
    put_bias(b_e, 7, 0)
    here.greet_wait()
    ga = Gather(here, lambda part: a_slot(me, part), a_slot, ga_s, ga_r)
    go = Gather(here, own_part(wo), o_slot, go_s, go_r)
    ge = Gather(here, own_part(we), e_slot, ge_s, ge_r)
    gr = Gather(here, own_part(wr), r_slot, gr_s, gr_r)
    outs = Outs(out_sem)
    to_sib = remote(small, sib_small, sm_s.at[0], sm_r.at[0], here.sib)
    to_sib.start()
    go.start()
    to_sib.wait_recv()
    all_small[here.f] = small[...] + sib_small[...]

    def small_copy(k):
        spot = all_small.at[here.f]
        return remote(spot, spot, sm_s.at[k], sm_r.at[k], here.plane(k))

    def small_landing(k):
        spot = all_small.at[lax.rem(here.f + n_f - k, n_f)]
        return remote(spot, spot, sm_s.at[k], sm_r.at[k], here.plane(k))

    for k in range(1, n_f):
        small_copy(k).start()
    for load in loads[3:]:
        load.wait()
    ga.start()
    for load in loads[1:3]:
        load.wait()
    outs.put(stage_e, e_slot(me, None))
    outs.put(stage_r, r_slot(me, None))
    for s in range(1, here.m):
        go.step(s)
    for k in range(1, n_f):
        small_landing(k).wait_recv()
    total = all_small[0]
    for k in range(1, n_f):
        total = total + all_small[k]
    par[...] = total
    outs.put(par, par_o)
    tok_in.wait()

    def norm_one(i, _):
        rows = pl.ds(al(i * 64, 64), 64)
        scaled, _spread = norm_rows(tokv[rows, :].astype(F32))
        n1[rows, :] = (scaled * par[0:1, :] + par[1:2, :]).astype(BF)
        return 0

    lax.fori_loop(0, rows_all // 64, norm_one, 0)
    outs.put(n1, n1_o)
    place_ids(ids, col, row, here)
    for s in range(1, here.m):
        ga.step(s)
    gr.start()
    ge.start()
    go.step(here.m)
    ga.step(here.m)
    loads[0].wait()
    ga.arrive()
    q[...] = (dot(n1[...], full_a[:, 0:width]) + par[6:7, 0:width]).astype(BF)
    kv[0, :, 0:width] = dot(n1[...], full_a[:, width : 2 * width]).astype(BF)
    kv[0, :, width : 2 * width] = (
        dot(n1[...], full_a[:, 2 * width : 3 * width]) + par[6:7, width : 2 * width]
    ).astype(BF)
    swap = remote(kv.at[0], kv.at[1], kv_s.at[0], kv_r.at[0], here.sib)
    swap.start()
    outs.put(full_a, a_o)
    outs.put(q, q_o)
    go.arrive()
    outs.put(full_o, o_o)
    swap.wait_recv()
    outs.put(kv, kv_o)
    blk = rows_all // 2

    def head(i, _):
        h = i // 2
        rows = pl.ds(al((i - 2 * h) * blk, blk), blk)
        kc = pl.ds(al(h * HD, HD), HD)
        vc = pl.ds(al(width + h * HD, HD), HD)
        ids = col[rows, :]
        qh = q[rows, kc]
        near = allowed_scores(qh, kv[0, :, kc], ids, row[0:1, :], scale)
        far = allowed_scores(qh, kv[1, :, kc], ids, row[1:2, :], scale)
        top = jnp.maximum(
            jnp.max(near, axis=-1, keepdims=True), jnp.max(far, axis=-1, keepdims=True)
        )
        near = jnp.exp(near - top)
        far = jnp.exp(far - top)
        total = jnp.sum(near, axis=-1, keepdims=True) + jnp.sum(far, axis=-1, keepdims=True)
        inv = 1.0 / total
        out = dot((near * inv).astype(BF), kv[0, :, vc]) + dot((far * inv).astype(BF), kv[1, :, vc])
        ctx[rows, kc] = out.astype(BF)
        return 0

    lax.fori_loop(0, 2 * heads, head, 0)
    outs.put(ctx, ctx_o)

    wide = model // 4

    def project(i, _):
        cols = pl.ds(al(i * wide, wide), wide)
        part[:, cols] = dot(ctx[...], full_o[:, cols]).astype(BF)
        return 0

    lax.fori_loop(0, 4, project, 0)
    line = Line(here, part, rbuf, norm, (ls_s, ls_r, lg_s, lg_r), chunks, lag)

    def final(rows, span, total):
        middle = tokv[rows, :].astype(F32) + total + par[2:3, :]
        mid[span, :] = middle
        scaled, _spread = norm_rows(middle)
        norm[rows, :] = (scaled * par[3:4, :] + par[4:5, :]).astype(BF)

    ticks = line.ticks()
    events = []
    for s in range(1, here.m):
        events += [functools.partial(gr.step, s), functools.partial(ge.step, s)]
    when = [1 + (ticks // 2) * i // max(1, len(events) - 1) for i in range(len(events))]
    events.append(functools.partial(gr.step, here.m))
    when.append(ticks - 2)

    def tick(tau, _):
        line.tick(tau, final)
        for at, event in zip(when, events):
            pl.when(tau == at)(event)
        return 0

    lax.fori_loop(0, ticks, tick, 0)
    outs.put(mid, mid_o)
    outs.put(norm, n2_o)
    ge.step(here.m)
    gr.arrive()
    ge.arrive()
    line.finish_sum()
    line.finish_back()
    for gather in (ga, go, gr, ge):
        gather.finish()
    to_sib.wait_send()
    for k in range(1, n_f):
        small_copy(k).wait_send()
    swap.wait_send()
    outs.wait()


def forward(n_f, n_t, tok, ids, vectors, biases, wq, wk, wv, wo, we, wr, chunks=16, lag=3):
    rows, model = tok.shape
    shard, width, ff = wq.shape[0], wo.shape[0], we.shape[1]
    sds = jax.ShapeDtypeStruct
    dma = pltpu.SemaphoreType.DMA
    outs = (
        sds((rows, model), BF),
        sds((rows, width), BF),
        sds((2, rows, 2 * width), BF),
        sds((rows, width), BF),
        sds((rows, model), BF),
        sds((rows // 2, model), F32),
        sds((8, model), F32),
        sds((model, 3 * width), BF),
        sds((width, model), BF),
        sds((model, ff), BF),
        sds((ff, model), BF),
    )
    v = pltpu.VMEM
    return pl.pallas_call(
        functools.partial(forward_kernel, n_f, n_t, chunks, lag),
        out_shape=outs,
        in_specs=[ANY] + [VM] * 10 + [ANY] * 6,
        out_specs=(ANY,) * len(outs),
        scratch_shapes=[
            v((rows, model), BF), v((rows, model), BF), v((model, 3 * width), BF),
            v((width, model), BF), v((shard, ff), BF), v((ff, shard), BF),
            v((rows, width), BF), v((2, rows, 2 * width), BF), v((rows, width), BF),
            v((rows, model), BF), v((2, rows // 2, model), BF), v((rows, model), BF),
            v((rows // 2, model), F32), v((rows, 1), F32), v((2, rows), F32), v((8, model), F32),
            v((8, model), F32), v((n_f, 8, model), F32), v((8, model), F32),
        ]
        + [dma((Gather.sems(n_f),))] * 8
        + Line.sems(chunks)
        + [dma((n_f,)), dma((n_f,)), dma((1,)), dma((1,)), dma((7,)), dma((16,))],
        compiler_params=pltpu.CompilerParams(
            collective_id=0, has_side_effects=True, vmem_limit_bytes=60 << 20
        ),
        cost_estimate=pl.CostEstimate(
            flops=8 * 10**9, bytes_accessed=60 * 10**6, transcendentals=10**6
        ),
        name="attention_forward",
    )(tok, ids, *vectors, *biases, wq, wk, wv, wo, we, wr)


class Scatter:
    def __init__(self, here, sums, stage, ring_half, ring_full, send, recv, block):
        self.here, self.sums, self.stage = here, sums, stage
        self.ring_half, self.ring_full = ring_half, ring_full
        self.send, self.recv, self.block = send, recv, block
        self.m, self.size = here.m, sums.shape[1]

    def offset(self, i):
        odd = lax.rem(i, 2)
        return self.m + (1 - 2 * odd) * ((i + 1) // 2)

    def shard(self, i, other):
        return self.here.shard(self.offset(i), other)

    def cross(self, i):
        slot = self.sums.at[self.here.owner(self.offset(i))]
        n = 2 * self.m + i
        return remote(self.stage(i), slot, self.send.at[n], self.recv.at[n], self.here.sib)

    def combine(self, i, own):
        f = self.here.owner(self.offset(i))
        self.sums[f] = (own + self.sums[f].astype(F32)).astype(BF)

    def slot(self, k, half):
        f = self.here.owner(k)
        if half is None:
            return self.sums.at[f]
        return self.sums.at[f, pl.ds(half * (self.size // 2), self.size // 2)]

    def hop(self, way, s):
        here, sign = self.here, (1, -1)[way]
        half = way if s == self.m else None
        dst = self.ring_half.at[way] if s == self.m else self.ring_full.at[way, s - 1]
        n = way * self.m + s - 1
        to = (here.right, here.left)[way]
        return remote(self.slot(sign * s, half), dst, self.send.at[n], self.recv.at[n], to)

    def launch(self, s):
        self.hop(0, s).start()
        self.hop(1, s).start()

    def absorb(self, s):
        for way in (0, 1):
            sign = (1, -1)[way]
            self.hop(way, s).wait_recv()
            f = self.here.owner(sign * (s - 1))
            base = way * (self.size // 2) if s == self.m else 0
            count = (self.size // 2 if s == self.m else self.size) // self.block

            def body(i, _, way=way, f=f, base=base):
                there = pl.ds(al(base + i * self.block, self.block), self.block)
                here_rows = pl.ds(al(i * self.block, self.block), self.block)
                if s == self.m:
                    got = self.ring_half[way, here_rows, :]
                else:
                    got = self.ring_full[way, s - 1, here_rows, :]
                self.sums[f, there, :] = (
                    self.sums[f, there, :].astype(F32) + got.astype(F32)
                ).astype(BF)
                return 0

            lax.fori_loop(0, count, body, 0)

    def last(self):
        self.hop(0, 1).wait_recv()
        self.hop(1, 1).wait_recv()
        f = self.here.owner(0)

        def body(i, _):
            rows = pl.ds(al(i * self.block, self.block), self.block)
            total = self.sums[f, rows, :].astype(F32) + self.ring_full[0, 0, rows, :].astype(F32)
            total = total + self.ring_full[1, 0, rows, :].astype(F32)
            self.sums[f, rows, :] = total.astype(BF)
            return 0

        lax.fori_loop(0, self.size // self.block, body, 0)

    def finish(self, crossed=True):
        for s in range(1, self.m + 1):
            self.hop(0, s).wait_send()
            self.hop(1, s).wait_send()
        if crossed:
            for i in range(2 * self.m):
                self.cross(i).wait_send()

    @staticmethod
    def buffers(n_f, rows, cols):
        v = pltpu.VMEM
        m = n_f // 2
        return [
            v((n_f, rows, cols), BF),
            v((2, rows // 2, cols), BF),
            v((2, max(1, m - 1), rows, cols), BF),
        ]

    @staticmethod
    def sems(n_f):
        return [pltpu.SemaphoreType.DMA((2 * n_f,))] * 2


def norm_back_rows(total, scaled, spread, gain):
    e = total * gain
    inner = (
        e
        - jnp.mean(e, axis=-1, keepdims=True)
        - scaled * jnp.mean(e * scaled, axis=-1, keepdims=True)
    )
    return inner * spread


def span_when(tau, start, stop, task):
    @pl.when((tau >= start) & (tau < stop))
    def _():
        task(tau - start)


def middle_kernel(
    n_f, n_t, chunks, lag,
    live, n2_i, cot, mid_i, par, full_e, full_r,
    gb_o, lo_o, gm_o, eg_o, pr_o, sums_o,
    ev, rv, n2, g, act, gh, part, part2, rbuf, rbuf2, gb, mid, gm, lo, sums,
    e_sum, e_half, e_full, r_sum,
    e_s, e_r, r_s, r_r,
    ls_s, ls_r, lg_s, lg_r, ms_s, ms_r, in_sem, te_sem, tr_sem, out_sem,
):
    here = Place(n_f, n_t)
    rows_all, model = n2.shape
    ff = act.shape[1]
    shard = e_sum.shape[1]
    tiles = 4
    ft = ff // tiles
    here.greet_signal()

    def e_load(i):
        cols = pl.ds(i * ft, ft)
        return pltpu.make_async_copy(full_e.at[:, cols], ev.at[:, cols], te_sem.at[i])

    def r_load(i):
        rows = pl.ds(i * ft, ft)
        return pltpu.make_async_copy(full_r.at[rows], rv.at[rows], tr_sem.at[i])

    loads = [
        pltpu.make_async_copy(n2_i, n2, in_sem.at[0]),
        pltpu.make_async_copy(cot, g, in_sem.at[1]),
        pltpu.make_async_copy(mid_i, mid, in_sem.at[2]),
    ]
    loads[0].start()
    e_load(0).start()
    loads[1].start()
    r_load(0).start()
    for i in range(1, tiles):
        e_load(i).start()
        r_load(i).start()
    loads[2].start()
    alive = live[0].astype(F32)
    loads[0].wait()
    loads[1].wait()
    sums[...] = jnp.zeros_like(sums)

    def mask(i, total):
        rows = pl.ds(al(i * 64, 64), 64)
        value = g[rows, :].astype(F32) * alive
        g[rows, :] = value.astype(BF)
        return total + jnp.sum(value, axis=0, keepdims=True)

    sums[0:1, :] = lax.fori_loop(0, rows_all // 64, mask, jnp.zeros((1, model), F32))

    def hidden_tile(i):
        cols = pl.ds(i * ft, ft)
        e_load(i).wait()
        h = dot(n2[...], ev[:, cols]) + par[7:8, cols]
        r_load(i).wait()
        ga = dot_nt(g[...], rv[cols, :])
        bell = 0.5 * (1.0 + lax.erf(h * (1.0 / math.sqrt(2.0))))
        act[:, cols] = (h * bell).astype(BF)
        slope = bell + h * jnp.exp(-0.5 * h * h) * (1.0 / math.sqrt(2.0 * math.pi))
        low = (ga * slope).astype(BF)
        gh[:, cols] = low
        sums[1:2, cols] = jnp.sum(low.astype(F32), axis=0, keepdims=True)

    for i in range(tiles):
        hidden_tile(i)
    wide = model // 4

    def back_tile(i, _):
        cols = pl.ds(al(i * wide, wide), wide)
        part[:, cols] = dot_nt(gh[...], ev[cols, :]).astype(BF)
        return 0

    lax.fori_loop(0, 4, back_tile, 0)
    loads[2].wait()
    here.greet_wait()
    line = Line(here, part, rbuf, gb, (ls_s, ls_r, lg_s, lg_r), chunks, lag)
    line2 = Line(here, part2, rbuf2, gb, (ms_s, ms_r, None, None), chunks, lag)
    outs = Outs(out_sem)

    def final(rows, span, total):
        scaled, spread = norm_rows(mid[span, :])
        grad = g[rows, :].astype(F32) + norm_back_rows(total, scaled, spread, par[3:4, :])
        gm[span, :] = grad
        gb[rows, :] = grad.astype(BF)
        sums[4:5, :] += jnp.sum(total * scaled, axis=0, keepdims=True)
        sums[5:6, :] += jnp.sum(total, axis=0, keepdims=True)

    def final2(rows, span, total):
        lo[span, :] = ((mid[span, :] + total + par[5:6, :]) * alive).astype(BF)

    def e_stage(i):
        return ev.at[pl.ds(al(i * shard, shard), shard)]

    def r_stage(i):
        return rv.at[:, pl.ds(al(i * shard, shard), shard)]

    def cols_of(i):
        return pl.ds(al(i * shard, shard), shard)

    es = Scatter(here, e_sum, e_stage, e_half, e_full, e_s, e_r, 64)
    rs = Scatter(here, r_sum, r_stage, None, None, r_s, r_r, 256)

    def e_other(i):
        value = dot_tn(n2[:, cols_of(es.shard(i, True))], gh[...])
        ev[pl.ds(al(i * shard, shard), shard), :] = value.astype(BF)
        es.cross(i).start()

    def e_own(i):
        value = dot_tn(n2[:, cols_of(es.shard(i, False))], gh[...])
        es.cross(i).wait_recv()
        es.combine(i, value)

    def mlp(i):
        part2[:, cols_of(i)] = dot(act[...], rv[:, cols_of(i)]).astype(BF)

    def r_other(i):
        value = dot_tn(act[...], g[:, cols_of(rs.shard(i, True))])
        rv[:, cols_of(i)] = value.astype(BF)
        rs.cross(i).start()

    def r_own(i):
        value = dot_tn(act[...], g[:, cols_of(rs.shard(i, False))])
        rs.cross(i).wait_recv()
        rs.combine(i, value)

    n_s = 2 * n_f
    a, b = n_f, 2 * n_f
    d = b + n_s
    ticks = max(line.ticks(), d + 2 * n_f, d + line2.sum_ticks())
    gap = max(1, (ticks - b) // (n_f // 2 + 1))

    def tick(tau, _):
        line.tick(tau, final)
        line2.tick(tau - d, final2, back=False)
        span_when(tau, 0, a, e_other)
        span_when(tau, a, b, e_own)
        span_when(tau, b, d, mlp)
        span_when(tau, d, d + n_f, r_other)
        span_when(tau, d + n_f, d + 2 * n_f, r_own)

        @pl.when(tau == a)
        def _():
            es.launch(here.m)

        for s in range(here.m, 1, -1):

            @pl.when(tau == b + gap * (here.m - s + 1) - 1)
            def _(s=s):
                es.absorb(s)
                es.launch(s - 1)

        return 0

    lax.fori_loop(0, ticks, tick, 0)
    outs.put(gb, gb_o)
    outs.put(gm, gm_o)
    outs.put(lo, lo_o)
    outs.put(r_sum, pr_o)
    outs.put(sums, sums_o)
    es.last()
    outs.put(e_sum.at[here.f], eg_o)
    line.finish_sum()
    line.finish_back()
    line2.finish_sum()
    es.finish()
    for i in range(n_f):
        rs.cross(i).wait_send()
    outs.wait()


def middle(n_f, n_t, live, n2, cot, mid, par, full_e, full_r, chunks=16, lag=3):
    rows, model = n2.shape
    ff = full_e.shape[1]
    shard = model // (2 * n_f)
    sds, dma, v = jax.ShapeDtypeStruct, pltpu.SemaphoreType.DMA, pltpu.VMEM
    outs = (
        sds((rows, model), BF),
        sds((rows // 2, model), BF),
        sds((rows // 2, model), F32),
        sds((shard, ff), BF),
        sds((n_f, ff, shard), BF),
        sds((8, model), F32),
    )
    return pl.pallas_call(
        functools.partial(middle_kernel, n_f, n_t, chunks, lag),
        out_shape=outs,
        in_specs=[pl.BlockSpec(memory_space=pltpu.SMEM), ANY, ANY, ANY, VM, ANY, ANY],
        out_specs=(ANY,) * len(outs),
        scratch_shapes=[
            v((model, ff), BF), v((ff, model), BF), v((rows, model), BF), v((rows, model), BF),
            v((rows, ff), BF), v((rows, ff), BF), v((rows, model), BF), v((rows, model), BF),
            v((2, rows // 2, model), BF), v((2, rows // 2, model), BF), v((rows, model), BF),
            v((rows // 2, model), F32), v((rows // 2, model), F32), v((rows // 2, model), BF),
            v((8, model), F32),
        ]
        + Scatter.buffers(n_f, shard, ff)
        + [v((n_f, ff, shard), BF)]
        + Scatter.sems(n_f)
        + Scatter.sems(n_f)
        + Line.sems(chunks)
        + Line.sems(chunks)[:2]
        + [dma((3,)), dma((4,)), dma((4,)), dma((6,))],
        compiler_params=pltpu.CompilerParams(
            collective_id=1, has_side_effects=True, vmem_limit_bytes=63 << 20
        ),
        cost_estimate=pl.CostEstimate(
            flops=26 * 10**9, bytes_accessed=40 * 10**6, transcendentals=4 * 10**6
        ),
        name="feed_forward",
    )(live, n2, cot, mid, par, full_e, full_r)


def backward_kernel(
    n_f, n_t, chunks, lag, chunks2, lag2,
    ids, par, sums_i, tok, gm_i, lo_i, gb_i, ctx_i, q_i, kv_i, n1_i, full_a, full_o, pr_i,
    lo_o, tg_o, rg_o, og_o, ag_o, small_o,
    av, ov, gb, n1, tokh, gm, ctx, q, kv, gc, grads, near_g, far_g, got_g, lof, norm, part, rbuf,
    col, row, sm, tp_small, sib_small, all_small,
    r_sum, r_half, r_full, o_sum, o_half, o_full, a_sum, a_half, a_full,
    r_s, r_r, o_s, o_r, a_s, a_r,
    ls_s, ls_r, lg_s, lg_r, ms_s, ms_r, mg_s, mg_r,
    kv_s, kv_r, tp_s, tp_r, sb_s, sb_r, pl_s, pl_r, in_sem, out_sem,
):
    here = Place(n_f, n_t)
    rows_all, model = gb.shape
    width = q.shape[1]
    shard = a_sum.shape[1]
    heads = width // HD
    half = rows_all // 2
    scale = 1.0 / math.sqrt(HD)
    here.greet_signal()
    mine = pl.ds(al(here.side * half, half), half)
    pairs = [
        (gb_i, gb), (full_o, ov), (pr_i, r_sum), (q_i, q), (kv_i, kv), (ctx_i, ctx),
        (full_a, av), (n1_i, n1), (gm_i, gm), (tok.at[mine], tokh),
    ]
    loads = [pltpu.make_async_copy(s, d, in_sem.at[i]) for i, (s, d) in enumerate(pairs)]
    for load in loads:
        load.start()
    end = (here.t == 0) | (here.t == n_t - 1)
    lo_load = pltpu.make_async_copy(lo_i, lof.at[mine], in_sem.at[len(pairs)])
    pl.when(end)(lo_load.start)
    sm[...] = sums_i[...]
    place_ids(ids, col, row, here)
    loads[0].wait()
    loads[1].wait()
    gc[...] = dot_nt(gb[...], ov[...]).astype(BF)
    pl.when(end)(lo_load.wait)
    loads[2].wait()
    here.greet_wait()
    outs = Outs(out_sem)
    line = Line(here, part, rbuf, norm, (ls_s, ls_r, lg_s, lg_r), chunks, lag)
    back = Line(here, lof, rbuf, lof, (ms_s, ms_r, mg_s, mg_r), chunks2, lag2)

    @pl.when(end)
    def _():
        def send(j, _):
            back.back_copy(j).start()
            return 0

        lax.fori_loop(0, chunks2, send, 0)

    back_ticks = chunks2 + lag2 * (n_t - 1)

    def back_tick(tau):
        back.gather_step(0, tau, 0)
        back.gather_step(1, tau, 0)

    def cols_of(i):
        return pl.ds(al(i * shard, shard), shard)

    def rows_of(i):
        return pl.ds(al(i * shard, shard), shard)

    rs = Scatter(here, r_sum, None, r_half, r_full, r_s, r_r, 256)
    os = Scatter(here, o_sum, lambda i: ov.at[:, cols_of(i)], o_half, o_full, o_s, o_r, 128)
    sa = Scatter(here, a_sum, lambda i: av.at[rows_of(i)], a_half, a_full, a_s, a_r, 64)
    rs.launch(here.m)
    for load in loads[3:6]:
        load.wait()

    def head(h, _):
        kc = pl.ds(al(h * HD, HD), HD)
        vc = pl.ds(al(width + h * HD, HD), HD)
        ids = col[...]
        qh, gh = q[:, kc], gc[:, kc]
        near = allowed_scores(qh, kv[0, :, kc], ids, row[0:1, :], scale)
        far = allowed_scores(qh, kv[1, :, kc], ids, row[1:2, :], scale)
        top = jnp.maximum(
            jnp.max(near, axis=-1, keepdims=True), jnp.max(far, axis=-1, keepdims=True)
        )
        near = jnp.exp(near - top)
        far = jnp.exp(far - top)
        inv = 1.0 / (
            jnp.sum(near, axis=-1, keepdims=True) + jnp.sum(far, axis=-1, keepdims=True)
        )
        near = near * inv
        far = far * inv
        near_gv = dot_tn(near.astype(BF), gh)
        far_gv = dot_tn(far.astype(BF), gh)
        gp_near = dot_nt(gh, kv[0, :, vc])
        gp_far = dot_nt(gh, kv[1, :, vc])
        inner = jnp.sum(gp_near * near, axis=-1, keepdims=True) + jnp.sum(
            gp_far * far, axis=-1, keepdims=True
        )
        gs_near = (near * (gp_near - inner)).astype(BF)
        gs_far = (far * (gp_far - inner)).astype(BF)
        gq = (dot(gs_near, kv[0, :, kc]) + dot(gs_far, kv[1, :, kc])) * scale
        grads[:, kc] = gq.astype(BF)
        near_g[:, kc] = dot_tn(gs_near, qh) * scale
        far_g[:, kc] = (dot_tn(gs_far, qh) * scale).astype(BF)
        near_g[:, vc] = near_gv
        far_g[:, vc] = far_gv.astype(BF)
        back_tick(2 * h)
        back_tick(2 * h + 1)

        @pl.when(h == heads // 2)
        def _():
            rs.absorb(here.m)
            rs.launch(here.m - 1)

        return 0

    lax.fori_loop(0, heads, head, 0)
    swap = remote(far_g, got_g, kv_s.at[0], kv_r.at[0], here.sib)
    swap.start()
    for s in range(here.m - 1, 1, -1):
        rs.absorb(s)
        rs.launch(s - 1)

    def out_task(i, _):
        value = dot_tn(ctx[...], gb[:, cols_of(os.shard(i, True))])
        ov[:, cols_of(i)] = value.astype(BF)
        os.cross(i).start()
        back_tick(2 * heads + i)
        return 0

    lax.fori_loop(0, n_f, out_task, 0)

    def out_own(i, _):
        value = dot_tn(ctx[...], gb[:, cols_of(os.shard(i, False))])
        os.cross(i).wait_recv()
        os.combine(i, value)
        back_tick(2 * heads + n_f + i)
        return 0

    lax.fori_loop(0, n_f, out_own, 0)
    os.launch(here.m)
    swap.wait_recv()

    def add_rows(i, total):
        rows = pl.ds(al(i * 128, 128), 128)
        low = (near_g[rows, :] + got_g[rows, :].astype(F32)).astype(BF)
        grads[rows, width:] = low
        both = jnp.concatenate([grads[rows, 0:width], low[:, width:]], axis=1).astype(F32)
        return total + jnp.sum(both, axis=0, keepdims=True)

    sm[3:4, 0 : 2 * width] = lax.fori_loop(
        0, rows_all // 128, add_rows, jnp.zeros((1, 2 * width), F32)
    )
    loads[6].wait()
    wide = model // 4

    def back_part(i, _):
        cols = pl.ds(al(i * wide, wide), wide)
        part[:, cols] = dot_nt(grads[...], av[cols, :]).astype(BF)
        return 0

    lax.fori_loop(0, 4, back_part, 0)
    for load in loads[7:]:
        load.wait()

    def final(rows, span, total):
        scaled, spread = norm_rows(tokh[span, :].astype(F32))
        grad = gm[span, :] + norm_back_rows(total, scaled, spread, par[0:1, :])
        norm[rows, :] = grad.astype(BF)
        sm[6:7, :] += jnp.sum(total * scaled, axis=0, keepdims=True)
        sm[7:8, :] += jnp.sum(total, axis=0, keepdims=True)

    def a_other(i):
        value = dot_tn(n1[:, cols_of(sa.shard(i, True))], grads[...])
        av[rows_of(i), :] = value.astype(BF)
        sa.cross(i).start()

    def a_own(i):
        value = dot_tn(n1[:, cols_of(sa.shard(i, False))], grads[...])
        sa.cross(i).wait_recv()
        sa.combine(i, value)

    def branch_sum(i):
        rows = pl.ds(al(i * 64, 64), 64)
        sm[2:3, :] += jnp.sum(gb[rows, :].astype(F32), axis=0, keepdims=True)

    sm[2:3, :] = jnp.zeros((1, model), F32)
    blocks = rows_all // 64
    d = 2 * n_f
    ticks = max(line.ticks(), d + blocks)
    plan = [(d, rs.last)]
    room = ticks - d
    for s in range(here.m, 1, -1):
        k = here.m - s
        spots = here.m - 1
        plan.append((d + 2 + (room * k) // (2 * spots), functools.partial(ring_step, os, s)))
        plan.append((d + room // 4 + (room * k) // (2 * spots), functools.partial(ring_step, sa, s)))

    def tick(tau, _):
        line.tick(tau, final)
        span_when(tau, 0, n_f, a_other)
        span_when(tau, n_f, d, a_own)
        span_when(tau, d, d + blocks, branch_sum)
        pl.when(tau == n_f)(lambda: sa.launch(here.m))
        for at, event in plan:
            pl.when(tau == at)(event)
        return 0

    lax.fori_loop(0, ticks, tick, 0)
    outs.put(norm, tg_o)
    outs.put(r_sum.at[here.f], rg_o)

    def rest(tau, _):
        back_tick(tau)
        return 0

    lax.fori_loop(min(2 * heads + 2 * n_f, back_ticks), back_ticks, rest, 0)
    outs.put(lof, lo_o)

    def tp_copy(k):
        spot = tp_small.at[here.side]
        return remote(sm, spot, tp_s.at[k - 1], tp_r.at[here.side], here.tp(k))

    @pl.when(end)
    def _():
        for k in range(1, n_t):
            tp_copy(k).start()

    def tp_landing(side):
        spot = tp_small.at[side]
        return remote(sm, spot, tp_s.at[0], tp_r.at[side], here.tp(1))

    @pl.when(here.t != 0)
    def _():
        tp_landing(0).wait_recv()

    @pl.when(here.t != n_t - 1)
    def _():
        tp_landing(1).wait_recv()

    @pl.when(end)
    def _():
        tp_small[here.side] = sm[...]

    top_rows = lax.broadcasted_iota(jnp.int32, (8, model), 0) < 4
    all_small[here.f] = jnp.where(top_rows, sm[...], tp_small[0] + tp_small[1])
    to_sib = remote(all_small.at[here.f], sib_small, sb_s.at[0], sb_r.at[0], here.sib)
    to_sib.start()
    to_sib.wait()
    all_small[here.f] += sib_small[...]

    def plane_copy(k):
        spot = all_small.at[here.f]
        return remote(spot, spot, pl_s.at[k], pl_r.at[k], here.plane(k))

    def plane_landing(k):
        spot = all_small.at[lax.rem(here.f + n_f - k, n_f)]
        return remote(spot, spot, pl_s.at[k], pl_r.at[k], here.plane(k))

    for k in range(1, n_f):
        plane_copy(k).start()
    os.last()
    outs.put(o_sum.at[here.f], og_o)
    sa.last()
    outs.put(a_sum.at[here.f], ag_o)
    for k in range(1, n_f):
        plane_landing(k).wait_recv()
    total = all_small[0]
    for k in range(1, n_f):
        total = total + all_small[k]
    sib_small[...] = total
    outs.put(sib_small, small_o)
    line.finish_sum()
    line.finish_back()
    back.finish_back()
    rs.finish(False)
    os.finish()
    sa.finish()
    swap.wait_send()

    @pl.when(end)
    def _():
        for k in range(1, n_t):
            tp_copy(k).wait_send()

    for k in range(1, n_f):
        plane_copy(k).wait_send()
    outs.wait()


def ring_step(scatter, s):
    scatter.absorb(s)
    scatter.launch(s - 1)


def backward(
    n_f, n_t, ids, par, sums, tok, gm, lo, gb, ctx, q, kv, n1, full_a, full_o, pr,
    chunks=16, lag=3, chunks2=8, lag2=2,
):
    rows, model = gb.shape
    width, ff = q.shape[1], pr.shape[1]
    shard = model // (2 * n_f)
    sds, dma, v = jax.ShapeDtypeStruct, pltpu.SemaphoreType.DMA, pltpu.VMEM
    outs = (
        sds((rows, model), BF),
        sds((rows, model), BF),
        sds((ff, shard), BF),
        sds((width, shard), BF),
        sds((shard, 3 * width), BF),
        sds((8, model), F32),
    )
    return pl.pallas_call(
        functools.partial(backward_kernel, n_f, n_t, chunks, lag, chunks2, lag2),
        out_shape=outs,
        in_specs=[VM] * 3 + [ANY] * 11,
        out_specs=(ANY,) * len(outs),
        scratch_shapes=[
            v((model, 3 * width), BF), v((width, model), BF), v((rows, model), BF),
            v((rows, model), BF), v((rows // 2, model), BF), v((rows // 2, model), F32),
            v((rows, width), BF), v((rows, width), BF), v((2, rows, 2 * width), BF),
            v((rows, width), BF), v((rows, 3 * width), BF), v((rows, 2 * width), F32),
            v((rows, 2 * width), BF), v((rows, 2 * width), BF), v((rows, model), BF),
            v((rows, model), BF), v((rows, model), BF), v((2, rows // 2, model), BF),
            v((rows, 1), F32), v((2, rows), F32),
            v((8, model), F32), v((2, 8, model), F32), v((8, model), F32),
            v((n_f, 8, model), F32),
        ]
        + Scatter.buffers(n_f, ff, shard)
        + Scatter.buffers(n_f, width, shard)
        + Scatter.buffers(n_f, shard, 3 * width)
        + Scatter.sems(n_f) * 3
        + Line.sems(chunks)
        + Line.sems(chunks2)
        + [dma((1,)), dma((1,)), dma((n_t - 1,)), dma((2,)), dma((1,)), dma((1,))]
        + [dma((n_f,)), dma((n_f,)), dma((11,)), dma((6,))],
        compiler_params=pltpu.CompilerParams(
            collective_id=2, has_side_effects=True, vmem_limit_bytes=63 << 20
        ),
        cost_estimate=pl.CostEstimate(
            flops=14 * 10**9, bytes_accessed=40 * 10**6, transcendentals=4 * 10**6
        ),
        name="attention_backward",
    )(ids, par, sums, tok, gm, lo, gb, ctx, q, kv, n1, full_a, full_o, pr)


def finish_kernel(
    n_f, total, lo_i, tg_i, e_i, r_i, a_i, o_i,
    lo_o, tg_o, e_o, r_o, q_o, k_o, v_o, o_o, g1_o, s1_o, bo_o, g2_o, s2_o, br_o, bq_o, bv_o, be_o,
    lo, tg, e, r, a, o, e32, r32, a32, o32, in_sem, out_sem,
):
    me = 2 * lax.axis_index("fsdp") + lax.axis_index("ctx")
    shard, width = q_o.shape
    parts = 4

    def slab(ref, i):
        size = ref.shape[0] // parts
        return ref.at[pl.ds(i * size, size)]

    def load(n, src, dst):
        found = [
            pltpu.make_async_copy(slab(src, i), slab(dst, i), in_sem.at[n, i]) for i in range(parts)
        ]
        for copy in found:
            copy.start()
        return found

    outs = Outs(out_sem)
    loads = [load(n, *pair) for n, pair in enumerate(((e_i, e), (r_i, r), (lo_i, lo), (a_i, a), (o_i, o), (tg_i, tg)))]

    def widen(found, src, dst, out):
        size = src.shape[0] // parts
        for i, copy in enumerate(found):
            copy.wait()
            rows = pl.ds(i * size, size)
            dst[rows, :] = src[rows, :].astype(F32)
            outs.put(slab(dst, i), slab(out, i))

    def pass_on(found, src, out):
        for i, copy in enumerate(found):
            copy.wait()
            outs.put(slab(src, i), slab(out, i))

    widen(loads[0], e, e32, e_o)
    widen(loads[1], r, r32, r_o)
    pass_on(loads[2], lo, lo_o.at[0])
    for copy in loads[3]:
        copy.wait()
    for k, out in enumerate((q_o, k_o, v_o)):
        a32[k] = a[:, k * width : (k + 1) * width].astype(F32)
        outs.put(a32.at[k], out)
    widen(loads[4], o, o32, o_o)
    pass_on(loads[5], tg, tg_o.at[0])
    for k, out in ((0, br_o), (2, bo_o), (4, g2_o), (5, s2_o), (6, g1_o), (7, s1_o)):
        out[...] = total[k : k + 1, pl.ds(al(me * shard, shard), shard)]

    def take_bias(out, line, base):
        count, piece = out.shape
        size = piece * 2 * n_f
        wide = jnp.concatenate(
            [total[line : line + 1, base + h * size : base + (h + 1) * size] for h in range(count)]
        )
        out[...] = lax.dot_general(
            wide, picker(me, piece, 2 * n_f), (((1,), (1,)), ((), ())),
            precision=lax.Precision.HIGHEST, preferred_element_type=F32,
        )

    take_bias(bq_o, 3, 0)
    take_bias(bv_o, 3, width)
    take_bias(be_o, 1, 0)
    outs.wait()


def finish(n_f, total, lo, tg, e, r, a, o, bias, wide_bias):
    (rows, model), (shard, ff), width = lo.shape, e.shape, o.shape[0]
    sds, dma, v = jax.ShapeDtypeStruct, pltpu.SemaphoreType.DMA, pltpu.VMEM
    big = [(1, rows, model)] * 2 + [(shard, ff), (ff, shard)] + [(shard, width)] * 3 + [(width, shard)]
    outs = tuple(sds(shape, BF if i < 2 else F32) for i, shape in enumerate(big))
    outs += (sds((1, shard), F32),) * 6
    outs += (sds(bias.shape, F32),) * 2 + (sds(wide_bias.shape, F32),)
    return pl.pallas_call(
        functools.partial(finish_kernel, n_f),
        out_shape=outs,
        in_specs=[VM] + [HBM] * 6,
        out_specs=(HBM,) * 8 + (VM,) * 9,
        scratch_shapes=[v(x.shape, BF) for x in (lo, tg, e, r, a, o)]
        + [v((shard, ff), F32), v((ff, shard), F32), v((3, shard, width), F32), v((width, shard), F32)]
        + [dma((6, 4)), dma((24,))],
        compiler_params=pltpu.CompilerParams(vmem_limit_bytes=60 << 20),
        cost_estimate=pl.CostEstimate(flops=10**6, bytes_accessed=18 * 10**6, transcendentals=0),
        name="finish",
    )(total, lo, tg, e, r, a, o)


def local(
    tokens, cotangent, block_ids, live_count, first_gain, first_shift, query_weight, query_bias,
    key_weight, value_weight, value_bias, output_weight, output_bias, second_gain, second_shift,
    expand_weight, expand_bias, reduce_weight, reduce_bias,
):
    n_f, n_t = lax.axis_size("fsdp"), lax.axis_size("tp")
    _, rows, model = tokens.shape
    tok = tokens.reshape(rows, model)
    vectors = (first_gain, first_shift, output_bias, second_gain, second_shift, reduce_bias)
    n1, q, kv, ctx, n2, mid, par, full_a, full_o, full_e, full_r = forward(
        n_f, n_t, tok, block_ids, vectors, (query_bias, value_bias, expand_bias),
        query_weight, key_weight, value_weight, output_weight, expand_weight, reduce_weight,
    )
    gb, lo, gm, e_grad, r_part, sums = middle(
        n_f, n_t, live_count, n2, cotangent.reshape(rows, model), mid, par, full_e, full_r
    )
    lo, tg, r_grad, o_grad, a_grad, total = backward(
        n_f, n_t, block_ids, par, sums, tok, gm, lo, gb, ctx, q, kv, n1, full_a, full_o, r_part
    )
    (
        layer_out, tokens_grad, e_grad, r_grad, q_grad, k_grad, v_grad, o_grad,
        g1, s1, b_o, g2, s2, b_r, b_q, b_v, b_e,
    ) = finish(n_f, total, lo, tg, e_grad, r_grad, a_grad, o_grad, query_bias, expand_bias)
    flat = lambda vector: vector.reshape(-1)
    return (
        layer_out, tokens_grad, flat(g1), flat(s1), q_grad, b_q, k_grad, v_grad, b_v, o_grad,
        flat(b_o), flat(g2), flat(s2), e_grad, b_e, r_grad, flat(b_r),
    )


def solution(mesh):
    tokens, vector = P("fsdp", "ctx", None), P(("fsdp", "ctx"))
    down, across = P(("fsdp", "ctx"), "tp"), P("tp", ("fsdp", "ctx"))
    return jax.shard_map(
        local,
        mesh=mesh,
        in_specs=(
            tokens, tokens, P("fsdp", None), P("fsdp"), vector, vector, down, across, down, down,
            across, across, vector, vector, vector, down, across, across, vector,
        ),
        out_specs=(
            tokens, tokens, vector, vector, down, across, down, down, across, across, vector,
            vector, vector, down, across, across, vector,
        ),
        check_vma=False,
    )
```

```python
import functools
import math

import jax
import jax.numpy as jnp
from jax import lax
from jax.experimental import pallas as pl
from jax.experimental.pallas import tpu as pltpu
from jax.sharding import PartitionSpec as P

HD = 128
NEG = -1e30
MESH = pl.DeviceIdType.MESH
ANY = pl.BlockSpec(memory_space=pl.ANY)
HBM = pl.BlockSpec(memory_space=pltpu.HBM)
VM = pl.BlockSpec(memory_space=pltpu.VMEM)
BF = jnp.bfloat16
F32 = jnp.float32
epsilon = 1e-05
TILES = 4
LATE = 1


def dot(left, right):
    return lax.dot_general(left, right, (((1,), (0,)), ((), ())), preferred_element_type=F32)


def dot_nt(left, right):
    return lax.dot_general(left, right, (((1,), (1,)), ((), ())), preferred_element_type=F32)


def dot_tn(left, right):
    return lax.dot_general(left, right, (((0,), (0,)), ((), ())), preferred_element_type=F32)


def al(value, step):
    return pl.multiple_of(value, step)


class Place:
    def __init__(self, n_f, n_t):
        self.n_f, self.n_t, self.m = n_f, n_t, n_f // 2
        self.f = lax.axis_index("fsdp")
        self.c = lax.axis_index("ctx")
        self.t = lax.axis_index("tp")
        self.p = self.spot(self.f)
        self.side = self.t // (n_t - 1)
        self.right = (self.owner(1), self.c, self.t)
        self.left = (self.owner(-1), self.c, self.t)
        self.sib = (self.f, 1 - self.c, self.t)

    def spot(self, g):
        a = g // self.m
        return (1 - a) * g + a * (self.n_f - 1 + self.m - g)

    def owner(self, k):
        return self.spot(lax.rem(self.p + k + self.n_f, self.n_f))

    def shard(self, k, other=False):
        c = 1 - self.c if other else self.c
        return 2 * self.owner(k) + c

    def tp(self, d):
        return (self.f, self.c, lax.rem(self.t + d + self.n_t, self.n_t))

    def plane(self, k):
        return (lax.rem(self.f + k, self.n_f), self.c, self.t)

    def greet_signal(self):
        bar = pltpu.get_barrier_semaphore()
        others = [self.sib] + [self.plane(k) for k in range(1, self.n_f)]
        others += [self.tp(k) for k in range(1, self.n_t)]
        for other in others:
            pl.semaphore_signal(bar, 1, device_id=other, device_id_type=MESH)

    def greet_wait(self):
        pl.semaphore_wait(pltpu.get_barrier_semaphore(), self.n_f + self.n_t - 1)

    def greet(self):
        self.greet_signal()
        self.greet_wait()


def remote(src, dst, send, recv, to):
    return pltpu.make_async_remote_copy(
        src_ref=src, dst_ref=dst, send_sem=send, recv_sem=recv, device_id=to, device_id_type=MESH
    )


class Gather:
    def __init__(self, here, own, slot, send, recv):
        self.here, self.own, self.slot, self.send, self.recv = here, own, slot, send, recv
        self.m = here.m

    def half(self, way, s):
        return None if s < self.m else way

    def hop(self, way, s):
        here, sign = self.here, (-1, 1)[way]
        part = self.half(way, s)
        idx = here.shard(sign * (s - 1))
        src = self.own(part) if s == 1 else self.slot(idx, part)
        k = way * self.m + s - 1
        to = (here.right, here.left)[way]
        return remote(src, self.slot(idx, part), self.send.at[k], self.recv.at[k], to)

    def landing(self, way, s):
        here, sign = self.here, (-1, 1)[way]
        part = self.half(way, s)
        ref = self.slot(here.shard(sign * s), part)
        k = way * self.m + s - 1
        to = (here.right, here.left)[way]
        return remote(ref, ref, self.send.at[k], self.recv.at[k], to)

    def cross(self, k, offset, other=False):
        here = self.here
        ref = self.slot(here.shard(offset, other), None)
        src = self.own(None) if (offset == 0 and not other) else ref
        n = 2 * self.m + k
        return remote(src, ref, self.send.at[n], self.recv.at[n], here.sib)

    def crossings(self):
        found = [(0, 0)]
        for s in range(1, self.m):
            found += [(2 * s - 1, -s), (2 * s, s)]
        return found + [(2 * self.m - 1, self.m)]

    def start(self):
        self.hop(0, 1).start()
        self.hop(1, 1).start()
        self.cross(0, 0).start()

    def step(self, s):
        self.landing(0, s).wait_recv()
        self.landing(1, s).wait_recv()
        if s < self.m:
            self.hop(0, s + 1).start()
            self.hop(1, s + 1).start()
            self.cross(2 * s - 1, -s).start()
            self.cross(2 * s, s).start()
        else:
            self.cross(2 * self.m - 1, self.m).start()

    def arrive(self):
        for k, offset in self.crossings():
            self.cross(k, offset, True).wait_recv()

    def finish(self):
        for s in range(1, self.m + 1):
            self.hop(0, s).wait_send()
            self.hop(1, s).wait_send()
        for k, offset in self.crossings():
            self.cross(k, offset).wait_send()

    @staticmethod
    def sems(n_f):
        return 2 * n_f


class Line:
    def __init__(self, here, part, rbuf, norm, sems, chunks, lag):
        self.here, self.part, self.rbuf, self.norm = here, part, rbuf, norm
        self.s_send, self.s_recv, self.g_send, self.g_recv = sems
        self.half = part.shape[0] // 2
        self.nc, self.lag = chunks, lag
        self.cr = self.half // chunks

    def rows(self, d, j):
        return pl.ds(al(d * self.half + j * self.cr, self.cr), self.cr)

    def span(self, j):
        return pl.ds(al(j * self.cr, self.cr), self.cr)

    def s_copy(self, d, j):
        return remote(
            self.part.at[self.rows(d, j)],
            self.rbuf.at[d, self.span(j)],
            self.s_send.at[d, j],
            self.s_recv.at[d, j],
            self.here.tp(2 * d - 1),
        )

    def g_copy(self, d, j):
        ref = self.norm.at[self.rows(d, j)]
        to = self.here.tp(1 - 2 * d)
        return remote(ref, ref, self.g_send.at[d, j], self.g_recv.at[d, j], to)

    def depth(self, d):
        t, n = self.here.t, self.here.n_t
        return t if d == 1 else n - 1 - t

    def sum_step(self, d, tau):
        depth, n = self.depth(d), self.here.n_t
        j = tau - self.lag * depth
        valid = (j >= 0) & (j < self.nc)

        @pl.when(valid & (depth > 0))
        def _():
            self.s_copy(d, j).wait_recv()

        @pl.when(valid & (depth > 0) & (depth < n - 1))
        def _():
            own = self.part[self.rows(d, j), :].astype(F32)
            got = self.rbuf[d, self.span(j), :].astype(F32)
            self.part[self.rows(d, j), :] = (own + got).astype(BF)

        @pl.when(valid & (depth < n - 1))
        def _():
            self.s_copy(d, j).start()

    def owner_step(self, tau, final, back=True):
        here, n = self.here, self.here.n_t
        j = tau - self.lag * (n - 1)
        end = (here.t == 0) | (here.t == n - 1)

        @pl.when(end & (j >= 0) & (j < self.nc))
        def _():
            d = here.side
            rows = self.rows(d, j)
            total = self.part[rows, :].astype(F32) + self.rbuf[d, self.span(j), :].astype(F32)
            final(rows, self.span(j), total)
            if back:
                self.back_copy(j).start()

    def back_copy(self, j):
        here = self.here
        d = here.side
        ref = self.norm.at[self.rows(d, j)]
        return remote(
            ref, ref, self.g_send.at[d, j], self.g_recv.at[d, j], here.tp(1 - 2 * d)
        )

    def gather_step(self, d, tau, base):
        t, n = self.here.t, self.here.n_t
        depth = t if d == 0 else n - 1 - t
        j = tau - base - self.lag * depth
        valid = (j >= 0) & (j < self.nc) & (depth > 0)

        @pl.when(valid)
        def _():
            self.g_copy(d, j).wait_recv()

        @pl.when(valid & (depth < n - 1))
        def _():
            self.g_copy(d, j).start()

    def sum_ticks(self):
        return self.nc + self.lag * (self.here.n_t - 1)

    def ticks(self):
        return self.nc + 2 * self.lag * (self.here.n_t - 1)

    def tick(self, tau, final, back=True):
        self.sum_step(1, tau)
        self.sum_step(0, tau)
        self.owner_step(tau, final, back)
        if back:
            base = self.lag * (self.here.n_t - 1)
            self.gather_step(0, tau, base)
            self.gather_step(1, tau, base)

    def finish_sum(self):
        t, n = self.here.t, self.here.n_t

        def body(j, _):
            @pl.when(t > 0)
            def _():
                self.s_copy(0, j).wait_send()

            @pl.when(t < n - 1)
            def _():
                self.s_copy(1, j).wait_send()

            return 0

        lax.fori_loop(0, self.nc, body, 0)

    def finish_back(self):
        t, n = self.here.t, self.here.n_t

        def body(j, _):
            @pl.when(t < n - 1)
            def _():
                self.g_copy(0, j).wait_send()

            @pl.when(t > 0)
            def _():
                self.g_copy(1, j).wait_send()

            return 0

        lax.fori_loop(0, self.nc, body, 0)

    @staticmethod
    def sems(chunks):
        return [pltpu.SemaphoreType.DMA((2, chunks))] * 4


def norm_rows(values):
    mean = jnp.mean(values, axis=-1, keepdims=True)
    center = values - mean
    spread = lax.rsqrt(jnp.mean(center * center, axis=-1, keepdims=True) + epsilon)
    return center * spread, spread


class Outs:
    def __init__(self, sem):
        self.sem, self.made = sem, []

    def put(self, src, dst):
        copy = pltpu.make_async_copy(src, dst, self.sem.at[len(self.made)])
        copy.start()
        self.made.append(copy)

    def wait(self):
        for copy in self.made:
            copy.wait()


def row_slots(ref, size):
    def slot(idx, part):
        if part is None:
            return ref.at[pl.ds(al(idx * size, size), size)]
        return ref.at[pl.ds(al(idx * size + part * (size // 2), size // 2), size // 2)]

    return slot


def column_slots(ref, width):
    size = ref.shape[0]

    def slot(idx, part):
        cols = pl.ds(al(idx * width, width), width)
        if part is None:
            return ref.at[:, cols]
        return ref.at[pl.ds(part * (size // 2), size // 2), cols]

    return slot


def own_part(ref):
    size = ref.shape[0]

    def own(part):
        if part is None:
            return ref
        return ref.at[pl.ds(part * (size // 2), size // 2)]

    return own


def place_ids(ids, col, row, here):
    rows = col.shape[0]
    row[0:1, :] = ids[:, pl.ds(al(here.c * rows, rows), rows)].astype(F32)
    row[1:2, :] = ids[:, pl.ds(al((1 - here.c) * rows, rows), rows)].astype(F32)
    step = 128

    def turn(i, _):
        start = al(i * step, step)
        down = lax.broadcasted_iota(jnp.int32, (step, rows), 0) + start
        along = lax.broadcasted_iota(jnp.int32, (step, rows), 1)
        kept = jnp.where(down == along, row[0:1, :], 0.0)
        col[pl.ds(start, step), :] = jnp.sum(kept, axis=1, keepdims=True)
        return 0

    lax.fori_loop(0, rows // step, turn, 0)


def picker(index, piece, count):
    down = lax.broadcasted_iota(jnp.int32, (piece, piece * count), 0) + index * piece
    return jnp.where(down == lax.broadcasted_iota(jnp.int32, (piece, piece * count), 1), 1.0, 0.0)


def allowed_scores(q, k, col, row, scale):
    return jnp.where(row <= col, dot_nt(q, k) * scale, NEG)


def forward_kernel(
    n_f, n_t, chunks, lag,
    tok, ids, g1, s1, b_o, g2, s2, b_r, b_q, b_v, b_e, wq, wk, wv, wo, we, wr,
    n1_o, q_o, kv_o, ctx_o, probs_o, n2_o, mid_o, par_o, a_o, o_o, e_o, r_o,
    tokv, n1, full_a, full_o, stage_e, stage_r, q, kv, ctx, part, rbuf, norm, mid,
    probs, col, row, small, sib_small, all_small, par,
    ga_s, ga_r, go_s, go_r, ge_s, ge_r, gr_s, gr_r,
    ls_s, ls_r, lg_s, lg_r, sm_s, sm_r, kv_s, kv_r, in_sem, out_sem,
):
    here = Place(n_f, n_t)
    width = wo.shape[0]
    shard = wq.shape[0]
    rows_all, model = n1.shape
    heads = width // HD
    scale = 1.0 / math.sqrt(HD)
    tok_in = pltpu.make_async_copy(tok, tokv, in_sem.at[0])
    tok_in.start()
    me = 2 * here.f + here.c
    a_slot, o_slot = row_slots(full_a, shard), column_slots(full_o, shard)
    e_slot, r_slot = row_slots(e_o, shard), column_slots(r_o, shard)
    wr = wr.at[pl.ds(0, r_o.shape[0])]
    loads = [
        pltpu.make_async_copy(wo, o_slot(me, None), in_sem.at[1]),
        pltpu.make_async_copy(we, stage_e, in_sem.at[2]),
        pltpu.make_async_copy(wr, stage_r, in_sem.at[3]),
    ]
    mine = pl.ds(al(me * shard, shard), shard)
    for k, w in enumerate((wq, wk, wv)):
        spot = full_a.at[mine, pl.ds(k * width, width)]
        loads.append(pltpu.make_async_copy(w, spot, in_sem.at[4 + k]))
    for load in loads[3:] + loads[:3]:
        load.start()
    here.greet_signal()
    small[...] = jnp.zeros_like(small)
    for k, vector in enumerate((g1, s1, b_o, g2, s2, b_r)):
        small[k : k + 1, mine] = vector[...].astype(F32).reshape(1, shard)

    def put_bias(bias, line, base):
        count, piece = bias.shape
        wide = dot(bias[...].astype(F32), picker(me, piece, 2 * n_f))
        size = piece * 2 * n_f
        for h in range(count):
            small[line : line + 1, base + h * size : base + (h + 1) * size] = wide[h : h + 1, :]

    put_bias(b_q, 6, 0)
    put_bias(b_v, 6, width)
    put_bias(b_e, 7, 0)
    here.greet_wait()
    ga = Gather(here, lambda part: a_slot(me, part), a_slot, ga_s, ga_r)
    go = Gather(here, own_part(wo), o_slot, go_s, go_r)
    ge = Gather(here, own_part(we), e_slot, ge_s, ge_r)
    gr = Gather(here, own_part(wr), r_slot, gr_s, gr_r)
    outs = Outs(out_sem)
    to_sib = remote(small, sib_small, sm_s.at[0], sm_r.at[0], here.sib)
    to_sib.start()
    go.start()
    to_sib.wait_recv()
    all_small[here.f] = small[...] + sib_small[...]

    def small_copy(k):
        spot = all_small.at[here.f]
        return remote(spot, spot, sm_s.at[k], sm_r.at[k], here.plane(k))

    def small_landing(k):
        spot = all_small.at[lax.rem(here.f + n_f - k, n_f)]
        return remote(spot, spot, sm_s.at[k], sm_r.at[k], here.plane(k))

    for k in range(1, n_f):
        small_copy(k).start()
    for load in loads[3:]:
        load.wait()
    ga.start()
    for load in loads[1:3]:
        load.wait()
    outs.put(stage_e, e_slot(me, None))
    outs.put(stage_r, r_slot(me, None))
    for s in range(1, here.m):
        go.step(s)
    for k in range(1, n_f):
        small_landing(k).wait_recv()
    total = all_small[0]
    for k in range(1, n_f):
        total = total + all_small[k]
    par[...] = total
    outs.put(par, par_o)
    tok_in.wait()

    def norm_one(i, _):
        rows = pl.ds(al(i * 64, 64), 64)
        scaled, _spread = norm_rows(tokv[rows, :].astype(F32))
        n1[rows, :] = (scaled * par[0:1, :] + par[1:2, :]).astype(BF)
        return 0

    lax.fori_loop(0, rows_all // 64, norm_one, 0)
    outs.put(n1, n1_o)
    place_ids(ids, col, row, here)
    for s in range(1, here.m):
        ga.step(s)
    gr.start()
    ge.start()
    go.step(here.m)
    ga.step(here.m)
    loads[0].wait()
    ga.arrive()
    q[...] = (dot(n1[...], full_a[:, 0:width]) + par[6:7, 0:width]).astype(BF)
    kv[0, :, 0:width] = dot(n1[...], full_a[:, width : 2 * width]).astype(BF)
    kv[0, :, width : 2 * width] = (
        dot(n1[...], full_a[:, 2 * width : 3 * width]) + par[6:7, width : 2 * width]
    ).astype(BF)
    swap = remote(kv.at[0], kv.at[1], kv_s.at[0], kv_r.at[0], here.sib)
    swap.start()
    outs.put(full_a, a_o)
    outs.put(q, q_o)
    go.arrive()
    outs.put(full_o, o_o)
    swap.wait_recv()
    outs.put(kv, kv_o)
    blk = rows_all // 2

    def head(i, _):
        h = i // 2
        rows = pl.ds(al((i - 2 * h) * blk, blk), blk)
        kc = pl.ds(al(h * HD, HD), HD)
        vc = pl.ds(al(width + h * HD, HD), HD)
        ids = col[rows, :]
        qh = q[rows, kc]
        near = allowed_scores(qh, kv[0, :, kc], ids, row[0:1, :], scale)
        far = allowed_scores(qh, kv[1, :, kc], ids, row[1:2, :], scale)
        top = jnp.maximum(
            jnp.max(near, axis=-1, keepdims=True), jnp.max(far, axis=-1, keepdims=True)
        )
        near = jnp.exp(near - top)
        far = jnp.exp(far - top)
        total = jnp.sum(near, axis=-1, keepdims=True) + jnp.sum(far, axis=-1, keepdims=True)
        inv = 1.0 / total
        near = (near * inv).astype(BF)
        far = (far * inv).astype(BF)
        probs[h, rows, 0:rows_all] = near
        probs[h, rows, rows_all:] = far
        ctx[rows, kc] = (dot(near, kv[0, :, vc]) + dot(far, kv[1, :, vc])).astype(BF)
        return 0

    lax.fori_loop(0, 2 * heads, head, 0)
    outs.put(ctx, ctx_o)
    outs.put(probs, probs_o)

    wide = model // 4

    def project(i, _):
        cols = pl.ds(al(i * wide, wide), wide)
        part[:, cols] = dot(ctx[...], full_o[:, cols]).astype(BF)
        return 0

    lax.fori_loop(0, 4, project, 0)
    line = Line(here, part, rbuf, norm, (ls_s, ls_r, lg_s, lg_r), chunks, lag)

    def final(rows, span, total):
        middle = tokv[rows, :].astype(F32) + total + par[2:3, :]
        mid[span, :] = middle
        scaled, _spread = norm_rows(middle)
        norm[rows, :] = (scaled * par[3:4, :] + par[4:5, :]).astype(BF)

    ticks = line.ticks()
    events = []
    for s in range(1, here.m):
        events += [functools.partial(gr.step, s), functools.partial(ge.step, s)]
    when = [1 + (ticks // 2) * i // max(1, len(events) - 1) for i in range(len(events))]
    events.append(functools.partial(gr.step, here.m))
    when.append(ticks - 2)

    def tick(tau, _):
        line.tick(tau, final)
        for at, event in zip(when, events):
            pl.when(tau == at)(event)
        return 0

    lax.fori_loop(0, ticks, tick, 0)
    outs.put(mid, mid_o)
    outs.put(norm, n2_o)
    ge.step(here.m)
    gr.arrive()
    ge.arrive()
    line.finish_sum()
    line.finish_back()
    for gather in (ga, go, gr, ge):
        gather.finish()
    to_sib.wait_send()
    for k in range(1, n_f):
        small_copy(k).wait_send()
    swap.wait_send()
    outs.wait()


def forward(n_f, n_t, tok, ids, vectors, biases, wq, wk, wv, wo, we, wr, chunks=16, lag=2):
    rows, model = tok.shape
    shard, width, ff = wq.shape[0], wo.shape[0], we.shape[1]
    early = ff - LATE * (ff // TILES)
    sds = jax.ShapeDtypeStruct
    dma = pltpu.SemaphoreType.DMA
    outs = (
        sds((rows, model), BF),
        sds((rows, width), BF),
        sds((2, rows, 2 * width), BF),
        sds((rows, width), BF),
        sds((width // HD, rows, 2 * rows), BF),
        sds((rows, model), BF),
        sds((rows // 2, model), F32),
        sds((8, model), F32),
        sds((model, 3 * width), BF),
        sds((width, model), BF),
        sds((model, ff), BF),
        sds((early, model), BF),
    )
    v = pltpu.VMEM
    return pl.pallas_call(
        functools.partial(forward_kernel, n_f, n_t, chunks, lag),
        out_shape=outs,
        in_specs=[ANY] + [VM] * 10 + [ANY] * 6,
        out_specs=(ANY,) * len(outs),
        scratch_shapes=[
            v((rows, model), BF), v((rows, model), BF), v((model, 3 * width), BF),
            v((width, model), BF), v((shard, ff), BF), v((early, shard), BF),
            v((rows, width), BF), v((2, rows, 2 * width), BF), v((rows, width), BF),
            v((rows, model), BF), v((2, rows // 2, model), BF), v((rows, model), BF),
            v((rows // 2, model), F32), v((width // HD, rows, 2 * rows), BF),
            v((rows, 1), F32), v((2, rows), F32), v((8, model), F32),
            v((8, model), F32), v((n_f, 8, model), F32), v((8, model), F32),
        ]
        + [dma((Gather.sems(n_f),))] * 8
        + Line.sems(chunks)
        + [dma((n_f,)), dma((n_f,)), dma((1,)), dma((1,)), dma((7,)), dma((16,))],
        compiler_params=pltpu.CompilerParams(
            collective_id=0, has_side_effects=True, vmem_limit_bytes=60 << 20
        ),
        cost_estimate=pl.CostEstimate(
            flops=8 * 10**9, bytes_accessed=60 * 10**6, transcendentals=10**6
        ),
        name="attention_forward",
    )(tok, ids, *vectors, *biases, wq, wk, wv, wo, we, wr)


class Scatter:
    def __init__(self, here, sums, stage, ring_half, ring_full, send, recv, block):
        self.here, self.sums, self.stage = here, sums, stage
        self.ring_half, self.ring_full = ring_half, ring_full
        self.send, self.recv, self.block = send, recv, block
        self.m, self.size = here.m, sums.shape[1]

    def offset(self, i):
        odd = lax.rem(i, 2)
        return self.m + (1 - 2 * odd) * ((i + 1) // 2)

    def shard(self, i, other):
        return self.here.shard(self.offset(i), other)

    def cross(self, i):
        slot = self.sums.at[self.here.owner(self.offset(i))]
        n = 2 * self.m + i
        return remote(self.stage(i), slot, self.send.at[n], self.recv.at[n], self.here.sib)

    def combine(self, i, own):
        f = self.here.owner(self.offset(i))
        self.sums[f] = (own + self.sums[f].astype(F32)).astype(BF)

    def slot(self, k, half):
        f = self.here.owner(k)
        if half is None:
            return self.sums.at[f]
        return self.sums.at[f, pl.ds(half * (self.size // 2), self.size // 2)]

    def hop(self, way, s):
        here, sign = self.here, (1, -1)[way]
        half = way if s == self.m else None
        dst = self.ring_half.at[way] if s == self.m else self.ring_full.at[way, s - 1]
        n = way * self.m + s - 1
        to = (here.right, here.left)[way]
        return remote(self.slot(sign * s, half), dst, self.send.at[n], self.recv.at[n], to)

    def launch(self, s):
        self.hop(0, s).start()
        self.hop(1, s).start()

    def absorb(self, s):
        for way in (0, 1):
            sign = (1, -1)[way]
            self.hop(way, s).wait_recv()
            f = self.here.owner(sign * (s - 1))
            base = way * (self.size // 2) if s == self.m else 0
            count = (self.size // 2 if s == self.m else self.size) // self.block

            def body(i, _, way=way, f=f, base=base):
                there = pl.ds(al(base + i * self.block, self.block), self.block)
                here_rows = pl.ds(al(i * self.block, self.block), self.block)
                if s == self.m:
                    got = self.ring_half[way, here_rows, :]
                else:
                    got = self.ring_full[way, s - 1, here_rows, :]
                self.sums[f, there, :] = (
                    self.sums[f, there, :].astype(F32) + got.astype(F32)
                ).astype(BF)
                return 0

            lax.fori_loop(0, count, body, 0)

    def last(self):
        self.hop(0, 1).wait_recv()
        self.hop(1, 1).wait_recv()
        f = self.here.owner(0)

        def body(i, _):
            rows = pl.ds(al(i * self.block, self.block), self.block)
            total = self.sums[f, rows, :].astype(F32) + self.ring_full[0, 0, rows, :].astype(F32)
            total = total + self.ring_full[1, 0, rows, :].astype(F32)
            self.sums[f, rows, :] = total.astype(BF)
            return 0

        lax.fori_loop(0, self.size // self.block, body, 0)

    def finish(self, crossed=True):
        for s in range(1, self.m + 1):
            self.hop(0, s).wait_send()
            self.hop(1, s).wait_send()
        if crossed:
            for i in range(2 * self.m):
                self.cross(i).wait_send()

    @staticmethod
    def buffers(n_f, rows, cols):
        v = pltpu.VMEM
        m = n_f // 2
        return [
            v((n_f, rows, cols), BF),
            v((2, rows // 2, cols), BF),
            v((2, max(1, m - 1), rows, cols), BF),
        ]

    @staticmethod
    def sems(n_f):
        return [pltpu.SemaphoreType.DMA((2 * n_f,))] * 2


def norm_back_rows(total, scaled, spread, gain):
    e = total * gain
    inner = (
        e
        - jnp.mean(e, axis=-1, keepdims=True)
        - scaled * jnp.mean(e * scaled, axis=-1, keepdims=True)
    )
    return inner * spread


def span_when(tau, start, stop, task):
    @pl.when((tau >= start) & (tau < stop))
    def _():
        task(tau - start)


def middle_kernel(
    n_f, n_t, chunks, lag,
    live, n2_i, cot, mid_i, par, full_e, full_r, wr,
    gb_o, lo_o, gm_o, eg_o, pr_o, sums_o,
    ev, rv, n2, g, act, gh, part, part2, rbuf, rbuf2, gb, mid, gm, lo, sums,
    e_sum, e_half, e_full, r_sum,
    e_s, e_r, r_s, r_r, gl_s, gl_r,
    ls_s, ls_r, lg_s, lg_r, ms_s, ms_r, in_sem, te_sem, tr_sem, out_sem,
):
    here = Place(n_f, n_t)
    rows_all, model = n2.shape
    ff = act.shape[1]
    shard = e_sum.shape[1]
    tiles = TILES
    ft = ff // tiles
    early = full_r.shape[0]
    late = ff - early
    here.greet_signal()
    late_own = wr.at[pl.ds(early, late)]
    late_slot = column_slots(rv.at[pl.ds(early, late)], shard)
    gl = Gather(here, own_part(late_own), late_slot, gl_s, gl_r)

    def e_load(i):
        cols = pl.ds(i * ft, ft)
        return pltpu.make_async_copy(full_e.at[:, cols], ev.at[:, cols], te_sem.at[i])

    def r_load(i):
        rows = pl.ds(i * ft, ft)
        return pltpu.make_async_copy(full_r.at[rows], rv.at[rows], tr_sem.at[i])

    loads = [
        pltpu.make_async_copy(n2_i, n2, in_sem.at[0]),
        pltpu.make_async_copy(cot, g, in_sem.at[1]),
        pltpu.make_async_copy(mid_i, mid, in_sem.at[2]),
        pltpu.make_async_copy(late_own, late_slot(2 * here.f + here.c, None), in_sem.at[3]),
    ]
    loads[0].start()
    e_load(0).start()
    loads[1].start()
    for i in range(1, tiles):
        e_load(i).start()
    for i in range(early // ft):
        r_load(i).start()
    loads[3].start()
    loads[2].start()
    here.greet_wait()
    gl.start()
    alive = live[0].astype(F32)
    loads[0].wait()
    loads[1].wait()
    sums[...] = jnp.zeros_like(sums)

    def mask(i, total):
        rows = pl.ds(al(i * 64, 64), 64)
        value = g[rows, :].astype(F32) * alive
        g[rows, :] = value.astype(BF)
        return total + jnp.sum(value, axis=0, keepdims=True)

    sums[0:1, :] = lax.fori_loop(0, rows_all // 64, mask, jnp.zeros((1, model), F32))

    def hidden_tile(i):
        cols = pl.ds(i * ft, ft)
        e_load(i).wait()
        h = dot(n2[...], ev[:, cols]) + par[7:8, cols]
        bell = 0.5 * (1.0 + lax.erf(h * (1.0 / math.sqrt(2.0))))
        act[:, cols] = (h * bell).astype(BF)
        slope = bell + h * jnp.exp(-0.5 * h * h) * (1.0 / math.sqrt(2.0 * math.pi))
        gh[:, cols] = slope.astype(BF)

    def grad_piece(cols):
        low = (dot_nt(g[...], rv[cols, :]) * gh[:, cols].astype(F32)).astype(BF)
        gh[:, cols] = low
        sums[1:2, cols] = jnp.sum(low.astype(F32), axis=0, keepdims=True)

    for i in range(tiles):
        hidden_tile(i)
    for s in range(1, here.m):
        gl.step(s)
    for i in range(early // ft):
        r_load(i).wait()
        grad_piece(pl.ds(i * ft, ft))
    gl.step(here.m)
    loads[3].wait()
    gl.arrive()
    line = Line(here, part, rbuf, gb, (ls_s, ls_r, lg_s, lg_r), chunks, lag)
    line2 = Line(here, part2, rbuf2, gb, (ms_s, ms_r, None, None), chunks, lag)
    outs = Outs(out_sem)

    def final(rows, span, total):
        scaled, spread = norm_rows(mid[span, :])
        grad = g[rows, :].astype(F32) + norm_back_rows(total, scaled, spread, par[3:4, :])
        gm[span, :] = grad
        gb[rows, :] = grad.astype(BF)
        sums[4:5, :] += jnp.sum(total * scaled, axis=0, keepdims=True)
        sums[5:6, :] += jnp.sum(total, axis=0, keepdims=True)

    def final2(rows, span, total):
        lo[span, :] = ((mid[span, :] + total + par[5:6, :]) * alive).astype(BF)

    def mlp(i, _):
        cols = pl.ds(al(i * shard, shard), shard)
        part2[:, cols] = dot(act[...], rv[:, cols]).astype(BF)
        return 0

    lax.fori_loop(0, 2 * n_f, mlp, 0)
    loads[2].wait()
    piece = ft // 2
    pieces, backs = late // piece, 8
    wide = model // backs

    def grad_step(i, _):
        grad_piece(pl.ds(al(early + i * piece, piece), piece))
        line2.tick(i, final2, back=False)
        return 0

    def back_step(i, _):
        cols = pl.ds(al(i * wide, wide), wide)
        part[:, cols] = dot_nt(gh[...], ev[cols, :]).astype(BF)
        line2.tick(pieces + i, final2, back=False)
        return 0

    lax.fori_loop(0, pieces, grad_step, 0)
    lax.fori_loop(0, backs, back_step, 0)
    gl.finish()

    def e_stage(i):
        return ev.at[pl.ds(al(i * shard, shard), shard)]

    def r_stage(i):
        return rv.at[:, pl.ds(al(i * shard, shard), shard)]

    def cols_of(i):
        return pl.ds(al(i * shard, shard), shard)

    es = Scatter(here, e_sum, e_stage, e_half, e_full, e_s, e_r, 64)
    rs = Scatter(here, r_sum, r_stage, None, None, r_s, r_r, 256)

    def e_other(i):
        value = dot_tn(n2[:, cols_of(es.shard(i, True))], gh[...])
        ev[pl.ds(al(i * shard, shard), shard), :] = value.astype(BF)
        es.cross(i).start()

    def e_own(i):
        value = dot_tn(n2[:, cols_of(es.shard(i, False))], gh[...])
        es.cross(i).wait_recv()
        es.combine(i, value)

    def r_other(i):
        value = dot_tn(act[...], g[:, cols_of(rs.shard(i, True))])
        rv[:, cols_of(i)] = value.astype(BF)
        rs.cross(i).start()

    def r_own(i):
        value = dot_tn(act[...], g[:, cols_of(rs.shard(i, False))])
        rs.cross(i).wait_recv()
        rs.combine(i, value)

    a, b = n_f, 2 * n_f
    ahead = pieces + backs
    ticks = max(line.ticks(), b + 2 * n_f, line2.sum_ticks() - ahead)
    gap = max(1, (ticks - b) // (n_f // 2 + 1))

    def tick(tau, _):
        line.tick(tau, final)
        line2.tick(tau + ahead, final2, back=False)
        span_when(tau, 0, a, e_other)
        span_when(tau, a, b, e_own)
        span_when(tau, b, b + n_f, r_other)
        span_when(tau, b + n_f, b + 2 * n_f, r_own)

        @pl.when(tau == a)
        def _():
            es.launch(here.m)

        for s in range(here.m, 1, -1):

            @pl.when(tau == b + gap * (here.m - s + 1) - 1)
            def _(s=s):
                es.absorb(s)
                es.launch(s - 1)

        return 0

    lax.fori_loop(0, ticks, tick, 0)
    outs.put(gb, gb_o)
    outs.put(gm, gm_o)
    outs.put(lo, lo_o)
    outs.put(r_sum, pr_o)
    outs.put(sums, sums_o)
    es.last()
    outs.put(e_sum.at[here.f], eg_o)
    line.finish_sum()
    line.finish_back()
    line2.finish_sum()
    es.finish()
    for i in range(n_f):
        rs.cross(i).wait_send()
    outs.wait()


def middle(n_f, n_t, live, n2, cot, mid, par, full_e, full_r, wr, chunks=16, lag=2):
    rows, model = n2.shape
    ff = full_e.shape[1]
    shard = model // (2 * n_f)
    sds, dma, v = jax.ShapeDtypeStruct, pltpu.SemaphoreType.DMA, pltpu.VMEM
    outs = (
        sds((rows, model), BF),
        sds((rows // 2, model), BF),
        sds((rows // 2, model), F32),
        sds((shard, ff), BF),
        sds((n_f, ff, shard), BF),
        sds((8, model), F32),
    )
    return pl.pallas_call(
        functools.partial(middle_kernel, n_f, n_t, chunks, lag),
        out_shape=outs,
        in_specs=[pl.BlockSpec(memory_space=pltpu.SMEM), ANY, ANY, ANY, VM, ANY, ANY, ANY],
        out_specs=(ANY,) * len(outs),
        scratch_shapes=[
            v((model, ff), BF), v((ff, model), BF), v((rows, model), BF), v((rows, model), BF),
            v((rows, ff), BF), v((rows, ff), BF), v((rows, model), BF), v((rows, model), BF),
            v((2, rows // 2, model), BF), v((2, rows // 2, model), BF), v((rows, model), BF),
            v((rows // 2, model), F32), v((rows // 2, model), F32), v((rows // 2, model), BF),
            v((8, model), F32),
        ]
        + Scatter.buffers(n_f, shard, ff)
        + [v((n_f, ff, shard), BF)]
        + Scatter.sems(n_f)
        + Scatter.sems(n_f)
        + [dma((Gather.sems(n_f),))] * 2
        + Line.sems(chunks)
        + Line.sems(chunks)[:2]
        + [dma((4,)), dma((4,)), dma((4,)), dma((6,))],
        compiler_params=pltpu.CompilerParams(
            collective_id=1, has_side_effects=True, vmem_limit_bytes=63 << 20
        ),
        cost_estimate=pl.CostEstimate(
            flops=26 * 10**9, bytes_accessed=40 * 10**6, transcendentals=4 * 10**6
        ),
        name="feed_forward",
    )(live, n2, cot, mid, par, full_e, full_r, wr)


def backward_kernel(
    n_f, n_t, chunks, lag, chunks2, lag2,
    par, sums_i, tok, gm_i, lo_i, gb_i, ctx_i, q_i, kv_i, probs_i, n1_i, full_a, full_o, pr_i,
    lo_o, tg_o, rg_o, og_o, ag_o, small_o,
    av, ov, gb, n1, tokh, gm, ctx, q, kv, probs, gc, grads, near_g, far_g, got_g, lof, norm, part, rbuf,
    sm, tp_small, sib_small, all_small,
    r_sum, r_half, r_full, o_sum, o_half, o_full, a_sum, a_half, a_full,
    r_s, r_r, o_s, o_r, a_s, a_r,
    ls_s, ls_r, lg_s, lg_r, ms_s, ms_r, mg_s, mg_r,
    kv_s, kv_r, tp_s, tp_r, sb_s, sb_r, pl_s, pl_r, in_sem, out_sem,
):
    here = Place(n_f, n_t)
    rows_all, model = gb.shape
    width = q.shape[1]
    shard = a_sum.shape[1]
    heads = width // HD
    half = rows_all // 2
    scale = 1.0 / math.sqrt(HD)
    here.greet_signal()
    mine = pl.ds(al(here.side * half, half), half)
    pairs = [
        (gb_i, gb), (full_o, ov), (pr_i, r_sum), (q_i, q), (kv_i, kv), (probs_i, probs), (ctx_i, ctx),
        (full_a, av), (n1_i, n1), (gm_i, gm), (tok.at[mine], tokh),
    ]
    loads = [pltpu.make_async_copy(s, d, in_sem.at[i]) for i, (s, d) in enumerate(pairs)]
    for load in loads:
        load.start()
    end = (here.t == 0) | (here.t == n_t - 1)
    lo_load = pltpu.make_async_copy(lo_i, lof.at[mine], in_sem.at[len(pairs)])
    pl.when(end)(lo_load.start)
    sm[...] = sums_i[...]
    loads[0].wait()
    loads[1].wait()
    gc[...] = dot_nt(gb[...], ov[...]).astype(BF)
    pl.when(end)(lo_load.wait)
    loads[2].wait()
    here.greet_wait()
    outs = Outs(out_sem)
    line = Line(here, part, rbuf, norm, (ls_s, ls_r, lg_s, lg_r), chunks, lag)
    back = Line(here, lof, rbuf, lof, (ms_s, ms_r, mg_s, mg_r), chunks2, lag2)

    @pl.when(end)
    def _():
        def send(j, _):
            back.back_copy(j).start()
            return 0

        lax.fori_loop(0, chunks2, send, 0)

    back_ticks = chunks2 + lag2 * (n_t - 1)

    def back_tick(tau):
        back.gather_step(0, tau, 0)
        back.gather_step(1, tau, 0)

    def cols_of(i):
        return pl.ds(al(i * shard, shard), shard)

    def rows_of(i):
        return pl.ds(al(i * shard, shard), shard)

    rs = Scatter(here, r_sum, None, r_half, r_full, r_s, r_r, 256)
    os = Scatter(here, o_sum, lambda i: ov.at[:, cols_of(i)], o_half, o_full, o_s, o_r, 128)
    sa = Scatter(here, a_sum, lambda i: av.at[rows_of(i)], a_half, a_full, a_s, a_r, 64)
    rs.launch(here.m)
    for load in loads[3:7]:
        load.wait()

    def head(h, _):
        kc = pl.ds(al(h * HD, HD), HD)
        vc = pl.ds(al(width + h * HD, HD), HD)
        qh, gh = q[:, kc], gc[:, kc]
        near_low, far_low = probs[h, :, 0:rows_all], probs[h, :, rows_all:]
        near_gv, far_gv = dot_tn(near_low, gh), dot_tn(far_low, gh)
        near, far = near_low.astype(F32), far_low.astype(F32)
        gp_near = dot_nt(gh, kv[0, :, vc])
        gp_far = dot_nt(gh, kv[1, :, vc])
        inner = jnp.sum(gp_near * near, axis=-1, keepdims=True) + jnp.sum(
            gp_far * far, axis=-1, keepdims=True
        )
        gs_near = (near * (gp_near - inner)).astype(BF)
        gs_far = (far * (gp_far - inner)).astype(BF)
        gq = (dot(gs_near, kv[0, :, kc]) + dot(gs_far, kv[1, :, kc])) * scale
        grads[:, kc] = gq.astype(BF)
        near_g[:, kc] = dot_tn(gs_near, qh) * scale
        far_g[:, kc] = (dot_tn(gs_far, qh) * scale).astype(BF)
        near_g[:, vc] = near_gv
        far_g[:, vc] = far_gv.astype(BF)
        for k in range(3):
            back_tick(3 * h + k)

        @pl.when(h == heads // 2)
        def _():
            rs.absorb(here.m)
            rs.launch(here.m - 1)

        return 0

    lax.fori_loop(0, heads, head, 0)
    swap = remote(far_g, got_g, kv_s.at[0], kv_r.at[0], here.sib)
    swap.start()
    for s in range(here.m - 1, 1, -1):
        rs.absorb(s)
        rs.launch(s - 1)

    def out_other(i):
        value = dot_tn(ctx[...], gb[:, cols_of(os.shard(i, True))])
        ov[:, cols_of(i)] = value.astype(BF)
        os.cross(i).start()

    def out_own(i):
        value = dot_tn(ctx[...], gb[:, cols_of(os.shard(i, False))])
        os.cross(i).wait_recv()
        os.combine(i, value)

    swap.wait_recv()

    def add_rows(i, total):
        rows = pl.ds(al(i * 128, 128), 128)
        low = (near_g[rows, :] + got_g[rows, :].astype(F32)).astype(BF)
        grads[rows, width:] = low
        both = jnp.concatenate([grads[rows, 0:width], low[:, width:]], axis=1).astype(F32)
        return total + jnp.sum(both, axis=0, keepdims=True)

    sm[3:4, 0 : 2 * width] = lax.fori_loop(
        0, rows_all // 128, add_rows, jnp.zeros((1, 2 * width), F32)
    )
    loads[7].wait()
    wide = model // 4

    def back_part(i, _):
        cols = pl.ds(al(i * wide, wide), wide)
        part[:, cols] = dot_nt(grads[...], av[cols, :]).astype(BF)
        return 0

    lax.fori_loop(0, 4, back_part, 0)
    for load in loads[8:]:
        load.wait()

    def final(rows, span, total):
        scaled, spread = norm_rows(tokh[span, :].astype(F32))
        grad = gm[span, :] + norm_back_rows(total, scaled, spread, par[0:1, :])
        norm[rows, :] = grad.astype(BF)
        sm[6:7, :] += jnp.sum(total * scaled, axis=0, keepdims=True)
        sm[7:8, :] += jnp.sum(total, axis=0, keepdims=True)

    def a_other(i):
        value = dot_tn(n1[:, cols_of(sa.shard(i, True))], grads[...])
        av[rows_of(i), :] = value.astype(BF)
        sa.cross(i).start()

    def a_own(i):
        value = dot_tn(n1[:, cols_of(sa.shard(i, False))], grads[...])
        sa.cross(i).wait_recv()
        sa.combine(i, value)

    def branch_sum(i):
        rows = pl.ds(al(i * 64, 64), 64)
        sm[2:3, :] += jnp.sum(gb[rows, :].astype(F32), axis=0, keepdims=True)

    sm[2:3, :] = jnp.zeros((1, model), F32)
    blocks = rows_all // 64
    d = 2 * n_f
    full = d + 2 * n_f
    ticks = max(line.ticks(), d + blocks, full + 2 * here.m)
    plan = [(d, rs.last)]
    room, spots = ticks - full, here.m - 1
    for s in range(here.m, 1, -1):
        k = here.m - s
        plan.append((full + 1 + (room * k) // (2 * spots), functools.partial(ring_step, os, s)))
        plan.append((d + 3 + (ticks - d) // 4 + (room * k) // (2 * spots), functools.partial(ring_step, sa, s)))

    def tick(tau, _):
        line.tick(tau, final)
        span_when(tau, 0, n_f, a_other)
        span_when(tau, n_f, d, a_own)
        span_when(tau, d, d + blocks, branch_sum)
        pl.when(tau == n_f)(lambda: sa.launch(here.m))
        span_when(tau, d, d + n_f, out_other)
        span_when(tau, d + n_f, full, out_own)
        pl.when(tau == d + n_f)(lambda: os.launch(here.m))
        back_tick(3 * heads + tau)
        for at, event in plan:
            pl.when(tau == at)(event)
        return 0

    lax.fori_loop(0, ticks, tick, 0)
    outs.put(norm, tg_o)
    outs.put(r_sum.at[here.f], rg_o)

    def rest(tau, _):
        back_tick(tau)
        return 0

    lax.fori_loop(min(3 * heads + ticks, back_ticks), back_ticks, rest, 0)
    outs.put(lof, lo_o)

    def tp_copy(k):
        spot = tp_small.at[here.side]
        return remote(sm, spot, tp_s.at[k - 1], tp_r.at[here.side], here.tp(k))

    @pl.when(end)
    def _():
        for k in range(1, n_t):
            tp_copy(k).start()

    def tp_landing(side):
        spot = tp_small.at[side]
        return remote(sm, spot, tp_s.at[0], tp_r.at[side], here.tp(1))

    @pl.when(here.t != 0)
    def _():
        tp_landing(0).wait_recv()

    @pl.when(here.t != n_t - 1)
    def _():
        tp_landing(1).wait_recv()

    @pl.when(end)
    def _():
        tp_small[here.side] = sm[...]

    top_rows = lax.broadcasted_iota(jnp.int32, (8, model), 0) < 4
    all_small[here.f] = jnp.where(top_rows, sm[...], tp_small[0] + tp_small[1])
    to_sib = remote(all_small.at[here.f], sib_small, sb_s.at[0], sb_r.at[0], here.sib)
    to_sib.start()
    to_sib.wait()
    all_small[here.f] += sib_small[...]

    def plane_copy(k):
        spot = all_small.at[here.f]
        return remote(spot, spot, pl_s.at[k], pl_r.at[k], here.plane(k))

    def plane_landing(k):
        spot = all_small.at[lax.rem(here.f + n_f - k, n_f)]
        return remote(spot, spot, pl_s.at[k], pl_r.at[k], here.plane(k))

    for k in range(1, n_f):
        plane_copy(k).start()
    os.last()
    outs.put(o_sum.at[here.f], og_o)
    sa.last()
    outs.put(a_sum.at[here.f], ag_o)
    for k in range(1, n_f):
        plane_landing(k).wait_recv()
    total = all_small[0]
    for k in range(1, n_f):
        total = total + all_small[k]
    sib_small[...] = total
    outs.put(sib_small, small_o)
    line.finish_sum()
    line.finish_back()
    back.finish_back()
    rs.finish(False)
    os.finish()
    sa.finish()
    swap.wait_send()

    @pl.when(end)
    def _():
        for k in range(1, n_t):
            tp_copy(k).wait_send()

    for k in range(1, n_f):
        plane_copy(k).wait_send()
    outs.wait()


def ring_step(scatter, s):
    scatter.absorb(s)
    scatter.launch(s - 1)


def backward(
    n_f, n_t, par, sums, tok, gm, lo, gb, ctx, q, kv, probs, n1, full_a, full_o, pr,
    chunks=16, lag=2, chunks2=8, lag2=2,
):
    rows, model = gb.shape
    width, ff = q.shape[1], pr.shape[1]
    shard = model // (2 * n_f)
    sds, dma, v = jax.ShapeDtypeStruct, pltpu.SemaphoreType.DMA, pltpu.VMEM
    outs = (
        sds((rows, model), BF),
        sds((rows, model), BF),
        sds((ff, shard), BF),
        sds((width, shard), BF),
        sds((shard, 3 * width), BF),
        sds((8, model), F32),
    )
    return pl.pallas_call(
        functools.partial(backward_kernel, n_f, n_t, chunks, lag, chunks2, lag2),
        out_shape=outs,
        in_specs=[VM] * 2 + [ANY] * 12,
        out_specs=(ANY,) * len(outs),
        scratch_shapes=[
            v((model, 3 * width), BF), v((width, model), BF), v((rows, model), BF),
            v((rows, model), BF), v((rows // 2, model), BF), v((rows // 2, model), F32),
            v((rows, width), BF), v((rows, width), BF), v((2, rows, 2 * width), BF),
            v((width // HD, rows, 2 * rows), BF),
            v((rows, width), BF), v((rows, 3 * width), BF), v((rows, 2 * width), F32),
            v((rows, 2 * width), BF), v((rows, 2 * width), BF), v((rows, model), BF),
            v((rows, model), BF), v((rows, model), BF), v((2, rows // 2, model), BF),
            v((8, model), F32), v((2, 8, model), F32), v((8, model), F32),
            v((n_f, 8, model), F32),
        ]
        + Scatter.buffers(n_f, ff, shard)
        + Scatter.buffers(n_f, width, shard)
        + Scatter.buffers(n_f, shard, 3 * width)
        + Scatter.sems(n_f) * 3
        + Line.sems(chunks)
        + Line.sems(chunks2)
        + [dma((1,)), dma((1,)), dma((n_t - 1,)), dma((2,)), dma((1,)), dma((1,))]
        + [dma((n_f,)), dma((n_f,)), dma((12,)), dma((6,))],
        compiler_params=pltpu.CompilerParams(
            collective_id=2, has_side_effects=True, vmem_limit_bytes=63 << 20
        ),
        cost_estimate=pl.CostEstimate(
            flops=14 * 10**9, bytes_accessed=40 * 10**6, transcendentals=4 * 10**6
        ),
        name="attention_backward",
    )(par, sums, tok, gm, lo, gb, ctx, q, kv, probs, n1, full_a, full_o, pr)


def finish_kernel(
    n_f, total, lo_i, tg_i, e_i, r_i, a_i, o_i,
    lo_o, tg_o, e_o, r_o, q_o, k_o, v_o, o_o, g1_o, s1_o, bo_o, g2_o, s2_o, br_o, bq_o, bv_o, be_o,
    lo, tg, e, r, a, o, e32, r32, a32, o32, in_sem, out_sem,
):
    me = 2 * lax.axis_index("fsdp") + lax.axis_index("ctx")
    shard, width = q_o.shape
    parts = 4

    def slab(ref, i):
        size = ref.shape[0] // parts
        return ref.at[pl.ds(i * size, size)]

    def load(n, src, dst):
        found = [
            pltpu.make_async_copy(slab(src, i), slab(dst, i), in_sem.at[n, i]) for i in range(parts)
        ]
        for copy in found:
            copy.start()
        return found

    outs = Outs(out_sem)
    loads = [load(n, *pair) for n, pair in enumerate(((e_i, e), (r_i, r), (lo_i, lo), (a_i, a), (o_i, o), (tg_i, tg)))]

    def widen(found, src, dst, out):
        size = src.shape[0] // parts
        for i, copy in enumerate(found):
            copy.wait()
            rows = pl.ds(i * size, size)
            dst[rows, :] = src[rows, :].astype(F32)
            outs.put(slab(dst, i), slab(out, i))

    def pass_on(found, src, out):
        for i, copy in enumerate(found):
            copy.wait()
            outs.put(slab(src, i), slab(out, i))

    widen(loads[0], e, e32, e_o)
    widen(loads[1], r, r32, r_o)
    pass_on(loads[2], lo, lo_o.at[0])
    for copy in loads[3]:
        copy.wait()
    for k, out in enumerate((q_o, k_o, v_o)):
        a32[k] = a[:, k * width : (k + 1) * width].astype(F32)
        outs.put(a32.at[k], out)
    widen(loads[4], o, o32, o_o)
    pass_on(loads[5], tg, tg_o.at[0])
    for k, out in ((0, br_o), (2, bo_o), (4, g2_o), (5, s2_o), (6, g1_o), (7, s1_o)):
        out[...] = total[k : k + 1, pl.ds(al(me * shard, shard), shard)]

    def take_bias(out, line, base):
        count, piece = out.shape
        size = piece * 2 * n_f
        wide = jnp.concatenate(
            [total[line : line + 1, base + h * size : base + (h + 1) * size] for h in range(count)]
        )
        out[...] = lax.dot_general(
            wide, picker(me, piece, 2 * n_f), (((1,), (1,)), ((), ())),
            precision=lax.Precision.HIGHEST, preferred_element_type=F32,
        )

    take_bias(bq_o, 3, 0)
    take_bias(bv_o, 3, width)
    take_bias(be_o, 1, 0)
    outs.wait()


def finish(n_f, total, lo, tg, e, r, a, o, bias, wide_bias):
    (rows, model), (shard, ff), width = lo.shape, e.shape, o.shape[0]
    sds, dma, v = jax.ShapeDtypeStruct, pltpu.SemaphoreType.DMA, pltpu.VMEM
    big = [(1, rows, model)] * 2 + [(shard, ff), (ff, shard)] + [(shard, width)] * 3 + [(width, shard)]
    outs = tuple(sds(shape, BF if i < 2 else F32) for i, shape in enumerate(big))
    outs += (sds((1, shard), F32),) * 6
    outs += (sds(bias.shape, F32),) * 2 + (sds(wide_bias.shape, F32),)
    return pl.pallas_call(
        functools.partial(finish_kernel, n_f),
        out_shape=outs,
        in_specs=[VM] + [HBM] * 6,
        out_specs=(HBM,) * 8 + (VM,) * 9,
        scratch_shapes=[v(x.shape, BF) for x in (lo, tg, e, r, a, o)]
        + [v((shard, ff), F32), v((ff, shard), F32), v((3, shard, width), F32), v((width, shard), F32)]
        + [dma((6, 4)), dma((24,))],
        compiler_params=pltpu.CompilerParams(vmem_limit_bytes=60 << 20),
        cost_estimate=pl.CostEstimate(flops=10**6, bytes_accessed=18 * 10**6, transcendentals=0),
        name="finish",
    )(total, lo, tg, e, r, a, o)


def local(
    tokens, cotangent, block_ids, live_count, first_gain, first_shift, query_weight, query_bias,
    key_weight, value_weight, value_bias, output_weight, output_bias, second_gain, second_shift,
    expand_weight, expand_bias, reduce_weight, reduce_bias,
):
    n_f, n_t = lax.axis_size("fsdp"), lax.axis_size("tp")
    _, rows, model = tokens.shape
    tok = tokens.reshape(rows, model)
    vectors = (first_gain, first_shift, output_bias, second_gain, second_shift, reduce_bias)
    n1, q, kv, ctx, probs, n2, mid, par, full_a, full_o, full_e, full_r = forward(
        n_f, n_t, tok, block_ids, vectors, (query_bias, value_bias, expand_bias),
        query_weight, key_weight, value_weight, output_weight, expand_weight, reduce_weight,
    )
    gb, lo, gm, e_grad, r_part, sums = middle(
        n_f, n_t, live_count, n2, cotangent.reshape(rows, model), mid, par, full_e, full_r, reduce_weight
    )
    lo, tg, r_grad, o_grad, a_grad, total = backward(
        n_f, n_t, par, sums, tok, gm, lo, gb, ctx, q, kv, probs, n1, full_a, full_o, r_part
    )
    (
        layer_out, tokens_grad, e_grad, r_grad, q_grad, k_grad, v_grad, o_grad,
        g1, s1, b_o, g2, s2, b_r, b_q, b_v, b_e,
    ) = finish(n_f, total, lo, tg, e_grad, r_grad, a_grad, o_grad, query_bias, expand_bias)
    flat = lambda vector: vector.reshape(-1)
    return (
        layer_out, tokens_grad, flat(g1), flat(s1), q_grad, b_q, k_grad, v_grad, b_v, o_grad,
        flat(b_o), flat(g2), flat(s2), e_grad, b_e, r_grad, flat(b_r),
    )


def solution(mesh):
    tokens, vector = P("fsdp", "ctx", None), P(("fsdp", "ctx"))
    down, across = P(("fsdp", "ctx"), "tp"), P("tp", ("fsdp", "ctx"))
    return jax.shard_map(
        local,
        mesh=mesh,
        in_specs=(
            tokens, tokens, P("fsdp", None), P("fsdp"), vector, vector, down, across, down, down,
            across, across, vector, vector, vector, down, across, across, vector,
        ),
        out_specs=(
            tokens, tokens, vector, vector, down, across, down, down, across, across, vector,
            vector, vector, down, across, across, vector,
        ),
        check_vma=False,
    )
```

```python
import functools
import math

import jax
import jax.numpy as jnp
from jax import lax
from jax.experimental import pallas as pl
from jax.experimental.pallas import tpu as pltpu
from jax.sharding import PartitionSpec as P

HD = 128
NEG = -1e30
MESH = pl.DeviceIdType.MESH
ANY = pl.BlockSpec(memory_space=pl.ANY)
HBM = pl.BlockSpec(memory_space=pltpu.HBM)
VM = pl.BlockSpec(memory_space=pltpu.VMEM)
BF = jnp.bfloat16
F32 = jnp.float32
epsilon = 1e-05
TILES = 4
LATE = 1


def dot(left, right):
    return lax.dot_general(left, right, (((1,), (0,)), ((), ())), preferred_element_type=F32)


def dot_nt(left, right):
    return lax.dot_general(left, right, (((1,), (1,)), ((), ())), preferred_element_type=F32)


def dot_tn(left, right):
    return lax.dot_general(left, right, (((0,), (0,)), ((), ())), preferred_element_type=F32)


def al(value, step):
    return pl.multiple_of(value, step)


class Place:
    def __init__(self, n_f, n_t):
        self.n_f, self.n_t, self.m = n_f, n_t, n_f // 2
        self.f = lax.axis_index("fsdp")
        self.c = lax.axis_index("ctx")
        self.t = lax.axis_index("tp")
        self.p = self.spot(self.f)
        self.side = self.t // (n_t - 1)
        self.right = (self.owner(1), self.c, self.t)
        self.left = (self.owner(-1), self.c, self.t)
        self.sib = (self.f, 1 - self.c, self.t)

    def spot(self, g):
        a = g // self.m
        return (1 - a) * g + a * (self.n_f - 1 + self.m - g)

    def owner(self, k):
        return self.spot(lax.rem(self.p + k + self.n_f, self.n_f))

    def shard(self, k, other=False):
        c = 1 - self.c if other else self.c
        return 2 * self.owner(k) + c

    def tp(self, d):
        return (self.f, self.c, lax.rem(self.t + d + self.n_t, self.n_t))

    def plane(self, k):
        return (lax.rem(self.f + k, self.n_f), self.c, self.t)

    def greet_signal(self):
        bar = pltpu.get_barrier_semaphore()
        others = [self.sib] + [self.plane(k) for k in range(1, self.n_f)]
        others += [self.tp(k) for k in range(1, self.n_t)]
        for other in others:
            pl.semaphore_signal(bar, 1, device_id=other, device_id_type=MESH)

    def greet_wait(self):
        pl.semaphore_wait(pltpu.get_barrier_semaphore(), self.n_f + self.n_t - 1)

    def greet(self):
        self.greet_signal()
        self.greet_wait()


def remote(src, dst, send, recv, to):
    return pltpu.make_async_remote_copy(
        src_ref=src, dst_ref=dst, send_sem=send, recv_sem=recv, device_id=to, device_id_type=MESH
    )


class Gather:
    def __init__(self, here, own, slot, send, recv):
        self.here, self.own, self.slot, self.send, self.recv = here, own, slot, send, recv
        self.m = here.m

    def half(self, way, s):
        return None if s < self.m else way

    def hop(self, way, s):
        here, sign = self.here, (-1, 1)[way]
        part = self.half(way, s)
        idx = here.shard(sign * (s - 1))
        src = self.own(part) if s == 1 else self.slot(idx, part)
        k = way * self.m + s - 1
        to = (here.right, here.left)[way]
        return remote(src, self.slot(idx, part), self.send.at[k], self.recv.at[k], to)

    def landing(self, way, s):
        here, sign = self.here, (-1, 1)[way]
        part = self.half(way, s)
        ref = self.slot(here.shard(sign * s), part)
        k = way * self.m + s - 1
        to = (here.right, here.left)[way]
        return remote(ref, ref, self.send.at[k], self.recv.at[k], to)

    def cross(self, k, offset, other=False):
        here = self.here
        ref = self.slot(here.shard(offset, other), None)
        src = self.own(None) if (offset == 0 and not other) else ref
        n = 2 * self.m + k
        return remote(src, ref, self.send.at[n], self.recv.at[n], here.sib)

    def crossings(self):
        found = [(0, 0)]
        for s in range(1, self.m):
            found += [(2 * s - 1, -s), (2 * s, s)]
        return found + [(2 * self.m - 1, self.m)]

    def start(self):
        self.hop(0, 1).start()
        self.hop(1, 1).start()
        self.cross(0, 0).start()

    def step(self, s):
        self.landing(0, s).wait_recv()
        self.landing(1, s).wait_recv()
        if s < self.m:
            self.hop(0, s + 1).start()
            self.hop(1, s + 1).start()
            self.cross(2 * s - 1, -s).start()
            self.cross(2 * s, s).start()
        else:
            self.cross(2 * self.m - 1, self.m).start()

    def arrive(self):
        for k, offset in self.crossings():
            self.cross(k, offset, True).wait_recv()

    def finish(self):
        for s in range(1, self.m + 1):
            self.hop(0, s).wait_send()
            self.hop(1, s).wait_send()
        for k, offset in self.crossings():
            self.cross(k, offset).wait_send()

    @staticmethod
    def sems(n_f):
        return 2 * n_f


class Line:
    def __init__(self, here, part, rbuf, norm, sems, chunks, lag):
        self.here, self.part, self.rbuf, self.norm = here, part, rbuf, norm
        self.s_send, self.s_recv, self.g_send, self.g_recv = sems
        self.half = part.shape[0] // 2
        self.nc, self.lag = chunks, lag
        self.cr = self.half // chunks

    def rows(self, d, j):
        return pl.ds(al(d * self.half + j * self.cr, self.cr), self.cr)

    def span(self, j):
        return pl.ds(al(j * self.cr, self.cr), self.cr)

    def s_copy(self, d, j):
        return remote(
            self.part.at[self.rows(d, j)],
            self.rbuf.at[d, self.span(j)],
            self.s_send.at[d, j],
            self.s_recv.at[d, j],
            self.here.tp(2 * d - 1),
        )

    def g_copy(self, d, j):
        ref = self.norm.at[self.rows(d, j)]
        to = self.here.tp(1 - 2 * d)
        return remote(ref, ref, self.g_send.at[d, j], self.g_recv.at[d, j], to)

    def depth(self, d):
        t, n = self.here.t, self.here.n_t
        return t if d == 1 else n - 1 - t

    def sum_step(self, d, tau):
        depth, n = self.depth(d), self.here.n_t
        j = tau - self.lag * depth
        valid = (j >= 0) & (j < self.nc)

        @pl.when(valid & (depth > 0))
        def _():
            self.s_copy(d, j).wait_recv()

        @pl.when(valid & (depth > 0) & (depth < n - 1))
        def _():
            own = self.part[self.rows(d, j), :].astype(F32)
            got = self.rbuf[d, self.span(j), :].astype(F32)
            self.part[self.rows(d, j), :] = (own + got).astype(BF)

        @pl.when(valid & (depth < n - 1))
        def _():
            self.s_copy(d, j).start()

    def owner_step(self, tau, final, back=True):
        here, n = self.here, self.here.n_t
        j = tau - self.lag * (n - 1)
        end = (here.t == 0) | (here.t == n - 1)

        @pl.when(end & (j >= 0) & (j < self.nc))
        def _():
            d = here.side
            rows = self.rows(d, j)
            total = self.part[rows, :].astype(F32) + self.rbuf[d, self.span(j), :].astype(F32)
            final(rows, self.span(j), total)
            if back:
                self.back_copy(j).start()

    def back_copy(self, j):
        here = self.here
        d = here.side
        ref = self.norm.at[self.rows(d, j)]
        return remote(
            ref, ref, self.g_send.at[d, j], self.g_recv.at[d, j], here.tp(1 - 2 * d)
        )

    def gather_step(self, d, tau, base):
        t, n = self.here.t, self.here.n_t
        depth = t if d == 0 else n - 1 - t
        j = tau - base - self.lag * depth
        valid = (j >= 0) & (j < self.nc) & (depth > 0)

        @pl.when(valid)
        def _():
            self.g_copy(d, j).wait_recv()

        @pl.when(valid & (depth < n - 1))
        def _():
            self.g_copy(d, j).start()

    def sum_ticks(self):
        return self.nc + self.lag * (self.here.n_t - 1)

    def ticks(self):
        return self.nc + 2 * self.lag * (self.here.n_t - 1)

    def tick(self, tau, final, back=True):
        self.sum_step(1, tau)
        self.sum_step(0, tau)
        self.owner_step(tau, final, back)
        if back:
            base = self.lag * (self.here.n_t - 1)
            self.gather_step(0, tau, base)
            self.gather_step(1, tau, base)

    def finish_sum(self):
        t, n = self.here.t, self.here.n_t

        def body(j, _):
            @pl.when(t > 0)
            def _():
                self.s_copy(0, j).wait_send()

            @pl.when(t < n - 1)
            def _():
                self.s_copy(1, j).wait_send()

            return 0

        lax.fori_loop(0, self.nc, body, 0)

    def finish_back(self):
        t, n = self.here.t, self.here.n_t

        def body(j, _):
            @pl.when(t < n - 1)
            def _():
                self.g_copy(0, j).wait_send()

            @pl.when(t > 0)
            def _():
                self.g_copy(1, j).wait_send()

            return 0

        lax.fori_loop(0, self.nc, body, 0)

    @staticmethod
    def sems(chunks):
        return [pltpu.SemaphoreType.DMA((2, chunks))] * 4


def norm_rows(values):
    mean = jnp.mean(values, axis=-1, keepdims=True)
    center = values - mean
    spread = lax.rsqrt(jnp.mean(center * center, axis=-1, keepdims=True) + epsilon)
    return center * spread, spread


class Outs:
    def __init__(self, sem):
        self.sem, self.made = sem, []

    def put(self, src, dst):
        copy = pltpu.make_async_copy(src, dst, self.sem.at[len(self.made)])
        copy.start()
        self.made.append(copy)

    def wait(self):
        for copy in self.made:
            copy.wait()


def row_slots(ref, size):
    def slot(idx, part):
        if part is None:
            return ref.at[pl.ds(al(idx * size, size), size)]
        return ref.at[pl.ds(al(idx * size + part * (size // 2), size // 2), size // 2)]

    return slot


def column_slots(ref, width):
    size = ref.shape[0]

    def slot(idx, part):
        cols = pl.ds(al(idx * width, width), width)
        if part is None:
            return ref.at[:, cols]
        return ref.at[pl.ds(part * (size // 2), size // 2), cols]

    return slot


def own_part(ref):
    size = ref.shape[0]

    def own(part):
        if part is None:
            return ref
        return ref.at[pl.ds(part * (size // 2), size // 2)]

    return own


def place_ids(ids, col, row, here):
    rows = col.shape[0]
    row[0:1, :] = ids[:, pl.ds(al(here.c * rows, rows), rows)].astype(F32)
    row[1:2, :] = ids[:, pl.ds(al((1 - here.c) * rows, rows), rows)].astype(F32)
    step = 128

    def turn(i, _):
        start = al(i * step, step)
        down = lax.broadcasted_iota(jnp.int32, (step, rows), 0) + start
        along = lax.broadcasted_iota(jnp.int32, (step, rows), 1)
        kept = jnp.where(down == along, row[0:1, :], 0.0)
        col[pl.ds(start, step), :] = jnp.sum(kept, axis=1, keepdims=True)
        return 0

    lax.fori_loop(0, rows // step, turn, 0)


def picker(index, piece, count):
    down = lax.broadcasted_iota(jnp.int32, (piece, piece * count), 0) + index * piece
    return jnp.where(down == lax.broadcasted_iota(jnp.int32, (piece, piece * count), 1), 1.0, 0.0)


def allowed_scores(q, k, col, row, scale):
    return jnp.where(row <= col, dot_nt(q, k) * scale, NEG)


def forward_kernel(
    n_f, n_t, chunks, lag,
    tok, ids, g1, s1, b_o, g2, s2, b_r, b_q, b_v, b_e, wq, wk, wv, wo, we, wr,
    n1_o, q_o, kv_o, ctx_o, probs_o, n2_o, mid_o, par_o, a_o, o_o, e_o, r_o,
    tokv, n1, full_a, full_o, stage_e, stage_r, q, kv, ctx, part, rbuf, norm, mid,
    probs, col, row, small, sib_small, all_small, par,
    ga_s, ga_r, go_s, go_r, ge_s, ge_r, gr_s, gr_r,
    ls_s, ls_r, lg_s, lg_r, sm_s, sm_r, kv_s, kv_r, in_sem, out_sem,
):
    here = Place(n_f, n_t)
    width = wo.shape[0]
    shard = wq.shape[0]
    rows_all, model = n1.shape
    heads = width // HD
    scale = 1.0 / math.sqrt(HD)
    tok_in = pltpu.make_async_copy(tok, tokv, in_sem.at[0])
    tok_in.start()
    me = 2 * here.f + here.c
    a_slot, o_slot = row_slots(full_a, shard), column_slots(full_o, shard)
    e_slot, r_slot = row_slots(e_o, shard), column_slots(r_o, shard)
    wr = wr.at[pl.ds(0, r_o.shape[0])]
    loads = [
        pltpu.make_async_copy(wo, o_slot(me, None), in_sem.at[1]),
        pltpu.make_async_copy(we, stage_e, in_sem.at[2]),
        pltpu.make_async_copy(wr, stage_r, in_sem.at[3]),
    ]
    mine = pl.ds(al(me * shard, shard), shard)
    for k, w in enumerate((wq, wk, wv)):
        spot = full_a.at[mine, pl.ds(k * width, width)]
        loads.append(pltpu.make_async_copy(w, spot, in_sem.at[4 + k]))
    for load in loads[3:] + loads[:3]:
        load.start()
    here.greet_signal()
    small[...] = jnp.zeros_like(small)
    for k, vector in enumerate((g1, s1, b_o, g2, s2, b_r)):
        small[k : k + 1, mine] = vector[...].astype(F32).reshape(1, shard)

    def put_bias(bias, line, base):
        count, piece = bias.shape
        wide = dot(bias[...].astype(F32), picker(me, piece, 2 * n_f))
        size = piece * 2 * n_f
        for h in range(count):
            small[line : line + 1, base + h * size : base + (h + 1) * size] = wide[h : h + 1, :]

    put_bias(b_q, 6, 0)
    put_bias(b_v, 6, width)
    put_bias(b_e, 7, 0)
    here.greet_wait()
    ga = Gather(here, lambda part: a_slot(me, part), a_slot, ga_s, ga_r)
    go = Gather(here, own_part(wo), o_slot, go_s, go_r)
    ge = Gather(here, own_part(we), e_slot, ge_s, ge_r)
    gr = Gather(here, own_part(wr), r_slot, gr_s, gr_r)
    outs = Outs(out_sem)
    to_sib = remote(small, sib_small, sm_s.at[0], sm_r.at[0], here.sib)
    to_sib.start()
    go.start()
    to_sib.wait_recv()
    all_small[here.f] = small[...] + sib_small[...]

    def small_copy(k):
        spot = all_small.at[here.f]
        return remote(spot, spot, sm_s.at[k], sm_r.at[k], here.plane(k))

    def small_landing(k):
        spot = all_small.at[lax.rem(here.f + n_f - k, n_f)]
        return remote(spot, spot, sm_s.at[k], sm_r.at[k], here.plane(k))

    for k in range(1, n_f):
        small_copy(k).start()
    for load in loads[3:]:
        load.wait()
    ga.start()
    for load in loads[1:3]:
        load.wait()
    outs.put(stage_e, e_slot(me, None))
    outs.put(stage_r, r_slot(me, None))
    for s in range(1, here.m):
        go.step(s)
    for k in range(1, n_f):
        small_landing(k).wait_recv()
    total = all_small[0]
    for k in range(1, n_f):
        total = total + all_small[k]
    par[...] = total
    outs.put(par, par_o)
    tok_in.wait()

    def norm_one(i, _):
        rows = pl.ds(al(i * 64, 64), 64)
        scaled, _spread = norm_rows(tokv[rows, :].astype(F32))
        n1[rows, :] = (scaled * par[0:1, :] + par[1:2, :]).astype(BF)
        return 0

    lax.fori_loop(0, rows_all // 64, norm_one, 0)
    outs.put(n1, n1_o)
    place_ids(ids, col, row, here)
    for s in range(1, here.m):
        ga.step(s)
    gr.start()
    ge.start()
    go.step(here.m)
    ga.step(here.m)
    loads[0].wait()
    ga.arrive()
    q[...] = (dot(n1[...], full_a[:, 0:width]) + par[6:7, 0:width]).astype(BF)
    kv[0, :, 0:width] = dot(n1[...], full_a[:, width : 2 * width]).astype(BF)
    kv[0, :, width : 2 * width] = (
        dot(n1[...], full_a[:, 2 * width : 3 * width]) + par[6:7, width : 2 * width]
    ).astype(BF)
    swap = remote(kv.at[0], kv.at[1], kv_s.at[0], kv_r.at[0], here.sib)
    swap.start()
    outs.put(full_a, a_o)
    outs.put(q, q_o)
    go.arrive()
    outs.put(full_o, o_o)
    swap.wait_recv()
    outs.put(kv, kv_o)
    blk = rows_all // 2

    def head(i, _):
        h = i // 2
        rows = pl.ds(al((i - 2 * h) * blk, blk), blk)
        kc = pl.ds(al(h * HD, HD), HD)
        vc = pl.ds(al(width + h * HD, HD), HD)
        ids = col[rows, :]
        qh = q[rows, kc]
        near = allowed_scores(qh, kv[0, :, kc], ids, row[0:1, :], scale)
        far = allowed_scores(qh, kv[1, :, kc], ids, row[1:2, :], scale)
        top = jnp.maximum(
            jnp.max(near, axis=-1, keepdims=True), jnp.max(far, axis=-1, keepdims=True)
        )
        near = jnp.exp(near - top)
        far = jnp.exp(far - top)
        total = jnp.sum(near, axis=-1, keepdims=True) + jnp.sum(far, axis=-1, keepdims=True)
        inv = 1.0 / total
        near = (near * inv).astype(BF)
        far = (far * inv).astype(BF)
        probs[h, rows, 0:rows_all] = near
        probs[h, rows, rows_all:] = far
        ctx[rows, kc] = (dot(near, kv[0, :, vc]) + dot(far, kv[1, :, vc])).astype(BF)
        return 0

    lax.fori_loop(0, 2 * heads, head, 0)
    outs.put(ctx, ctx_o)
    outs.put(probs, probs_o)

    wide = model // 4

    def project(i, _):
        cols = pl.ds(al(i * wide, wide), wide)
        part[:, cols] = dot(ctx[...], full_o[:, cols]).astype(BF)
        return 0

    lax.fori_loop(0, 4, project, 0)
    line = Line(here, part, rbuf, norm, (ls_s, ls_r, lg_s, lg_r), chunks, lag)

    def final(rows, span, total):
        middle = tokv[rows, :].astype(F32) + total + par[2:3, :]
        mid[span, :] = middle
        scaled, _spread = norm_rows(middle)
        norm[rows, :] = (scaled * par[3:4, :] + par[4:5, :]).astype(BF)

    ticks = line.ticks()
    events = []
    for s in range(1, here.m):
        events += [functools.partial(gr.step, s), functools.partial(ge.step, s)]
    when = [1 + (ticks // 2) * i // max(1, len(events) - 1) for i in range(len(events))]
    events.append(functools.partial(gr.step, here.m))
    when.append(ticks - 2)

    def tick(tau, _):
        line.tick(tau, final)
        for at, event in zip(when, events):
            pl.when(tau == at)(event)
        return 0

    lax.fori_loop(0, ticks, tick, 0)
    outs.put(mid, mid_o)
    outs.put(norm, n2_o)
    ge.step(here.m)
    gr.arrive()
    ge.arrive()
    line.finish_sum()
    line.finish_back()
    for gather in (ga, go, gr, ge):
        gather.finish()
    to_sib.wait_send()
    for k in range(1, n_f):
        small_copy(k).wait_send()
    swap.wait_send()
    outs.wait()


def forward(n_f, n_t, tok, ids, vectors, biases, wq, wk, wv, wo, we, wr, chunks=16, lag=2):
    rows, model = tok.shape
    shard, width, ff = wq.shape[0], wo.shape[0], we.shape[1]
    early = ff - LATE * (ff // TILES)
    sds = jax.ShapeDtypeStruct
    dma = pltpu.SemaphoreType.DMA
    outs = (
        sds((rows, model), BF),
        sds((rows, width), BF),
        sds((2, rows, 2 * width), BF),
        sds((rows, width), BF),
        sds((width // HD, rows, 2 * rows), BF),
        sds((rows, model), BF),
        sds((rows // 2, model), F32),
        sds((8, model), F32),
        sds((model, 3 * width), BF),
        sds((width, model), BF),
        sds((model, ff), BF),
        sds((early, model), BF),
    )
    v = pltpu.VMEM
    return pl.pallas_call(
        functools.partial(forward_kernel, n_f, n_t, chunks, lag),
        out_shape=outs,
        in_specs=[ANY] + [VM] * 10 + [ANY] * 6,
        out_specs=(ANY,) * len(outs),
        scratch_shapes=[
            v((rows, model), BF), v((rows, model), BF), v((model, 3 * width), BF),
            v((width, model), BF), v((shard, ff), BF), v((early, shard), BF),
            v((rows, width), BF), v((2, rows, 2 * width), BF), v((rows, width), BF),
            v((rows, model), BF), v((2, rows // 2, model), BF), v((rows, model), BF),
            v((rows // 2, model), F32), v((width // HD, rows, 2 * rows), BF),
            v((rows, 1), F32), v((2, rows), F32), v((8, model), F32),
            v((8, model), F32), v((n_f, 8, model), F32), v((8, model), F32),
        ]
        + [dma((Gather.sems(n_f),))] * 8
        + Line.sems(chunks)
        + [dma((n_f,)), dma((n_f,)), dma((1,)), dma((1,)), dma((7,)), dma((16,))],
        compiler_params=pltpu.CompilerParams(
            collective_id=0, has_side_effects=True, vmem_limit_bytes=60 << 20
        ),
        cost_estimate=pl.CostEstimate(
            flops=8 * 10**9, bytes_accessed=60 * 10**6, transcendentals=10**6
        ),
        name="attention_forward",
    )(tok, ids, *vectors, *biases, wq, wk, wv, wo, we, wr)


class Scatter:
    def __init__(self, here, sums, stage, ring_half, ring_full, send, recv, block):
        self.here, self.sums, self.stage = here, sums, stage
        self.ring_half, self.ring_full = ring_half, ring_full
        self.send, self.recv, self.block = send, recv, block
        self.m, self.size = here.m, sums.shape[1]

    def offset(self, i):
        odd = lax.rem(i, 2)
        return self.m + (1 - 2 * odd) * ((i + 1) // 2)

    def shard(self, i, other):
        return self.here.shard(self.offset(i), other)

    def cross(self, i):
        slot = self.sums.at[self.here.owner(self.offset(i))]
        n = 2 * self.m + i
        return remote(self.stage(i), slot, self.send.at[n], self.recv.at[n], self.here.sib)

    def combine(self, i, own):
        f = self.here.owner(self.offset(i))
        self.sums[f] = (own + self.sums[f].astype(F32)).astype(BF)

    def slot(self, k, half):
        f = self.here.owner(k)
        if half is None:
            return self.sums.at[f]
        return self.sums.at[f, pl.ds(half * (self.size // 2), self.size // 2)]

    def hop(self, way, s):
        here, sign = self.here, (1, -1)[way]
        half = way if s == self.m else None
        dst = self.ring_half.at[way] if s == self.m else self.ring_full.at[way, s - 1]
        n = way * self.m + s - 1
        to = (here.right, here.left)[way]
        return remote(self.slot(sign * s, half), dst, self.send.at[n], self.recv.at[n], to)

    def launch(self, s):
        self.hop(0, s).start()
        self.hop(1, s).start()

    def absorb(self, s):
        for way in (0, 1):
            sign = (1, -1)[way]
            self.hop(way, s).wait_recv()
            f = self.here.owner(sign * (s - 1))
            base = way * (self.size // 2) if s == self.m else 0
            count = (self.size // 2 if s == self.m else self.size) // self.block

            def body(i, _, way=way, f=f, base=base):
                there = pl.ds(al(base + i * self.block, self.block), self.block)
                here_rows = pl.ds(al(i * self.block, self.block), self.block)
                if s == self.m:
                    got = self.ring_half[way, here_rows, :]
                else:
                    got = self.ring_full[way, s - 1, here_rows, :]
                self.sums[f, there, :] = (
                    self.sums[f, there, :].astype(F32) + got.astype(F32)
                ).astype(BF)
                return 0

            lax.fori_loop(0, count, body, 0)

    def last(self):
        self.hop(0, 1).wait_recv()
        self.hop(1, 1).wait_recv()
        f = self.here.owner(0)

        def body(i, _):
            rows = pl.ds(al(i * self.block, self.block), self.block)
            total = self.sums[f, rows, :].astype(F32) + self.ring_full[0, 0, rows, :].astype(F32)
            total = total + self.ring_full[1, 0, rows, :].astype(F32)
            self.sums[f, rows, :] = total.astype(BF)
            return 0

        lax.fori_loop(0, self.size // self.block, body, 0)

    def finish(self, crossed=True):
        for s in range(1, self.m + 1):
            self.hop(0, s).wait_send()
            self.hop(1, s).wait_send()
        if crossed:
            for i in range(2 * self.m):
                self.cross(i).wait_send()

    @staticmethod
    def buffers(n_f, rows, cols):
        v = pltpu.VMEM
        m = n_f // 2
        return [
            v((n_f, rows, cols), BF),
            v((2, rows // 2, cols), BF),
            v((2, max(1, m - 1), rows, cols), BF),
        ]

    @staticmethod
    def sems(n_f):
        return [pltpu.SemaphoreType.DMA((2 * n_f,))] * 2


def norm_back_rows(total, scaled, spread, gain):
    e = total * gain
    inner = (
        e
        - jnp.mean(e, axis=-1, keepdims=True)
        - scaled * jnp.mean(e * scaled, axis=-1, keepdims=True)
    )
    return inner * spread


def span_when(tau, start, stop, task):
    @pl.when((tau >= start) & (tau < stop))
    def _():
        task(tau - start)


def middle_kernel(
    n_f, n_t, chunks, lag,
    live, n2_i, cot, mid_i, par, full_e, full_r, wr,
    gb_o, p2_o, gm_o, eg_o, pr_o, sums_o,
    ev, rv, n2, g, act, gh, part, part2, rbuf, gb, mid, gm, sums,
    e_sum, e_half, e_full, r_sum,
    e_s, e_r, r_s, r_r, gl_s, gl_r,
    ls_s, ls_r, lg_s, lg_r, in_sem, te_sem, tr_sem, out_sem,
):
    here = Place(n_f, n_t)
    rows_all, model = n2.shape
    ff = act.shape[1]
    shard = e_sum.shape[1]
    tiles = TILES
    ft = ff // tiles
    early = full_r.shape[0]
    late = ff - early
    here.greet_signal()
    late_own = wr.at[pl.ds(early, late)]
    late_slot = column_slots(rv.at[pl.ds(early, late)], shard)
    gl = Gather(here, own_part(late_own), late_slot, gl_s, gl_r)

    def e_load(i):
        cols = pl.ds(i * ft, ft)
        return pltpu.make_async_copy(full_e.at[:, cols], ev.at[:, cols], te_sem.at[i])

    def r_load(i):
        rows = pl.ds(i * ft, ft)
        return pltpu.make_async_copy(full_r.at[rows], rv.at[rows], tr_sem.at[i])

    loads = [
        pltpu.make_async_copy(n2_i, n2, in_sem.at[0]),
        pltpu.make_async_copy(cot, g, in_sem.at[1]),
        pltpu.make_async_copy(mid_i, mid, in_sem.at[2]),
        pltpu.make_async_copy(late_own, late_slot(2 * here.f + here.c, None), in_sem.at[3]),
    ]
    loads[0].start()
    e_load(0).start()
    loads[1].start()
    for i in range(1, tiles):
        e_load(i).start()
    for i in range(early // ft):
        r_load(i).start()
    loads[3].start()
    loads[2].start()
    here.greet_wait()
    gl.start()
    alive = live[0].astype(F32)
    loads[0].wait()
    loads[1].wait()
    sums[...] = jnp.zeros_like(sums)

    def mask(i, total):
        rows = pl.ds(al(i * 64, 64), 64)
        value = g[rows, :].astype(F32) * alive
        g[rows, :] = value.astype(BF)
        return total + jnp.sum(value, axis=0, keepdims=True)

    sums[0:1, :] = lax.fori_loop(0, rows_all // 64, mask, jnp.zeros((1, model), F32))

    def hidden_tile(i):
        cols = pl.ds(i * ft, ft)
        e_load(i).wait()
        h = dot(n2[...], ev[:, cols]) + par[7:8, cols]
        bell = 0.5 * (1.0 + lax.erf(h * (1.0 / math.sqrt(2.0))))
        act[:, cols] = (h * bell).astype(BF)
        slope = bell + h * jnp.exp(-0.5 * h * h) * (1.0 / math.sqrt(2.0 * math.pi))
        gh[:, cols] = slope.astype(BF)

    def grad_piece(cols):
        low = (dot_nt(g[...], rv[cols, :]) * gh[:, cols].astype(F32)).astype(BF)
        gh[:, cols] = low
        sums[1:2, cols] = jnp.sum(low.astype(F32), axis=0, keepdims=True)

    for i in range(tiles):
        hidden_tile(i)
    for s in range(1, here.m):
        gl.step(s)
    for i in range(early // ft):
        r_load(i).wait()
        grad_piece(pl.ds(i * ft, ft))
    gl.step(here.m)
    loads[3].wait()
    gl.arrive()
    line = Line(here, part, rbuf, gb, (ls_s, ls_r, lg_s, lg_r), chunks, lag)
    outs = Outs(out_sem)

    def final(rows, span, total):
        scaled, spread = norm_rows(mid[span, :])
        grad = g[rows, :].astype(F32) + norm_back_rows(total, scaled, spread, par[3:4, :])
        gm[span, :] = grad
        gb[rows, :] = grad.astype(BF)
        sums[4:5, :] += jnp.sum(total * scaled, axis=0, keepdims=True)
        sums[5:6, :] += jnp.sum(total, axis=0, keepdims=True)

    def mlp(i):
        cols = pl.ds(al(i * shard, shard), shard)
        part2[:, cols] = dot(act[...], rv[:, cols]).astype(BF)

    loads[2].wait()
    piece = ft // 2
    pieces, backs = late // piece, 8
    wide = model // backs

    def grad_step(i, _):
        grad_piece(pl.ds(al(early + i * piece, piece), piece))
        return 0

    def back_step(i, _):
        cols = pl.ds(al(i * wide, wide), wide)
        part[:, cols] = dot_nt(gh[...], ev[cols, :]).astype(BF)
        return 0

    lax.fori_loop(0, pieces, grad_step, 0)
    lax.fori_loop(0, backs, back_step, 0)
    gl.finish()

    def e_stage(i):
        return ev.at[pl.ds(al(i * shard, shard), shard)]

    def r_stage(i):
        return rv.at[:, pl.ds(al(i * shard, shard), shard)]

    def cols_of(i):
        return pl.ds(al(i * shard, shard), shard)

    es = Scatter(here, e_sum, e_stage, e_half, e_full, e_s, e_r, 64)
    rs = Scatter(here, r_sum, r_stage, None, None, r_s, r_r, 256)

    def e_other(i):
        value = dot_tn(n2[:, cols_of(es.shard(i, True))], gh[...])
        ev[pl.ds(al(i * shard, shard), shard), :] = value.astype(BF)
        es.cross(i).start()

    def e_own(i):
        value = dot_tn(n2[:, cols_of(es.shard(i, False))], gh[...])
        es.cross(i).wait_recv()
        es.combine(i, value)

    def r_other(i):
        value = dot_tn(act[...], g[:, cols_of(rs.shard(i, True))])
        rv[:, cols_of(i)] = value.astype(BF)
        rs.cross(i).start()

    def r_own(i):
        value = dot_tn(act[...], g[:, cols_of(rs.shard(i, False))])
        rs.cross(i).wait_recv()
        rs.combine(i, value)

    a, b = n_f, 2 * n_f
    d = b + 2 * n_f
    ticks = max(line.ticks(), d + 2 * n_f)
    gap = max(1, (ticks - b) // (n_f // 2 + 1))

    def tick(tau, _):
        line.tick(tau, final)
        span_when(tau, 0, a, e_other)
        span_when(tau, a, b, e_own)
        span_when(tau, b, d, mlp)
        span_when(tau, d, d + n_f, r_other)
        span_when(tau, d + n_f, d + 2 * n_f, r_own)

        @pl.when(tau == a)
        def _():
            es.launch(here.m)

        for s in range(here.m, 1, -1):

            @pl.when(tau == b + gap * (here.m - s + 1) - 1)
            def _(s=s):
                es.absorb(s)
                es.launch(s - 1)

        return 0

    lax.fori_loop(0, ticks, tick, 0)
    outs.put(gb, gb_o)
    outs.put(gm, gm_o)
    outs.put(part2, p2_o)
    outs.put(r_sum, pr_o)
    outs.put(sums, sums_o)
    es.last()
    outs.put(e_sum.at[here.f], eg_o)
    line.finish_sum()
    line.finish_back()
    es.finish()
    for i in range(n_f):
        rs.cross(i).wait_send()
    outs.wait()


def middle(n_f, n_t, live, n2, cot, mid, par, full_e, full_r, wr, chunks=16, lag=2):
    rows, model = n2.shape
    ff = full_e.shape[1]
    shard = model // (2 * n_f)
    sds, dma, v = jax.ShapeDtypeStruct, pltpu.SemaphoreType.DMA, pltpu.VMEM
    outs = (
        sds((rows, model), BF),
        sds((rows, model), BF),
        sds((rows // 2, model), F32),
        sds((shard, ff), BF),
        sds((n_f, ff, shard), BF),
        sds((8, model), F32),
    )
    return pl.pallas_call(
        functools.partial(middle_kernel, n_f, n_t, chunks, lag),
        out_shape=outs,
        in_specs=[pl.BlockSpec(memory_space=pltpu.SMEM), ANY, ANY, ANY, VM, ANY, ANY, ANY],
        out_specs=(ANY,) * len(outs),
        scratch_shapes=[
            v((model, ff), BF), v((ff, model), BF), v((rows, model), BF), v((rows, model), BF),
            v((rows, ff), BF), v((rows, ff), BF), v((rows, model), BF), v((rows, model), BF),
            v((2, rows // 2, model), BF), v((rows, model), BF),
            v((rows // 2, model), F32), v((rows // 2, model), F32),
            v((8, model), F32),
        ]
        + Scatter.buffers(n_f, shard, ff)
        + [v((n_f, ff, shard), BF)]
        + Scatter.sems(n_f)
        + Scatter.sems(n_f)
        + [dma((Gather.sems(n_f),))] * 2
        + Line.sems(chunks)
        + [dma((4,)), dma((4,)), dma((4,)), dma((6,))],
        compiler_params=pltpu.CompilerParams(
            collective_id=1, has_side_effects=True, vmem_limit_bytes=63 << 20
        ),
        cost_estimate=pl.CostEstimate(
            flops=26 * 10**9, bytes_accessed=40 * 10**6, transcendentals=4 * 10**6
        ),
        name="feed_forward",
    )(live, n2, cot, mid, par, full_e, full_r, wr)


def backward_kernel(
    n_f, n_t, chunks, lag, chunks2, lag2,
    live, par, sums_i, tok, gm_i, mid_i, p2_i, gb_i, ctx_i, q_i, kv_i, probs_i, n1_i, full_a, full_o, pr_i,
    lo_o, tg_o, rg_o, og_o, ag_o, small_o,
    av, ov, gb, n1, tokh, gm, ctx, q, kv, probs, gc, grads, near_g, far_g, got_g, lof, p2, mid, rbuf2, norm, part, rbuf,
    sm, tp_small, sib_small, all_small,
    r_sum, r_half, r_full, o_sum, o_half, o_full, a_sum, a_half, a_full,
    r_s, r_r, o_s, o_r, a_s, a_r,
    ls_s, ls_r, lg_s, lg_r, ms_s, ms_r, mg_s, mg_r,
    kv_s, kv_r, tp_s, tp_r, sb_s, sb_r, pl_s, pl_r, in_sem, out_sem,
):
    here = Place(n_f, n_t)
    rows_all, model = gb.shape
    width = q.shape[1]
    shard = a_sum.shape[1]
    heads = width // HD
    half = rows_all // 2
    scale = 1.0 / math.sqrt(HD)
    here.greet_signal()
    mine = pl.ds(al(here.side * half, half), half)
    pairs = [
        (gb_i, gb), (full_o, ov), (p2_i, p2), (mid_i, mid), (pr_i, r_sum), (q_i, q), (kv_i, kv), (probs_i, probs), (ctx_i, ctx),
        (full_a, av), (n1_i, n1), (gm_i, gm), (tok.at[mine], tokh),
    ]
    loads = [pltpu.make_async_copy(s, d, in_sem.at[i]) for i, (s, d) in enumerate(pairs)]
    for load in loads:
        load.start()
    end = (here.t == 0) | (here.t == n_t - 1)
    sm[...] = sums_i[...]
    loads[0].wait()
    loads[1].wait()
    gc[...] = dot_nt(gb[...], ov[...]).astype(BF)
    for load in loads[2:5]:
        load.wait()
    here.greet_wait()
    alive = live[0].astype(F32)
    outs = Outs(out_sem)
    line = Line(here, part, rbuf, norm, (ls_s, ls_r, lg_s, lg_r), chunks, lag)
    back = Line(here, p2, rbuf2, lof, (ms_s, ms_r, mg_s, mg_r), chunks2, lag2)

    back_ticks = back.ticks()

    def final2(rows, span, total):
        lof[rows, :] = ((mid[span, :] + total + par[5:6, :]) * alive).astype(BF)

    def back_tick(tau):
        back.tick(tau, final2)

    def cols_of(i):
        return pl.ds(al(i * shard, shard), shard)

    def rows_of(i):
        return pl.ds(al(i * shard, shard), shard)

    rs = Scatter(here, r_sum, None, r_half, r_full, r_s, r_r, 256)
    os = Scatter(here, o_sum, lambda i: ov.at[:, cols_of(i)], o_half, o_full, o_s, o_r, 128)
    sa = Scatter(here, a_sum, lambda i: av.at[rows_of(i)], a_half, a_full, a_s, a_r, 64)
    rs.launch(here.m)
    for load in loads[5:9]:
        load.wait()

    def head(h, _):
        kc = pl.ds(al(h * HD, HD), HD)
        vc = pl.ds(al(width + h * HD, HD), HD)
        qh, gh = q[:, kc], gc[:, kc]
        near_low, far_low = probs[h, :, 0:rows_all], probs[h, :, rows_all:]
        near_gv, far_gv = dot_tn(near_low, gh), dot_tn(far_low, gh)
        near, far = near_low.astype(F32), far_low.astype(F32)
        gp_near = dot_nt(gh, kv[0, :, vc])
        gp_far = dot_nt(gh, kv[1, :, vc])
        inner = jnp.sum(gp_near * near, axis=-1, keepdims=True) + jnp.sum(
            gp_far * far, axis=-1, keepdims=True
        )
        gs_near = (near * (gp_near - inner)).astype(BF)
        gs_far = (far * (gp_far - inner)).astype(BF)
        gq = (dot(gs_near, kv[0, :, kc]) + dot(gs_far, kv[1, :, kc])) * scale
        grads[:, kc] = gq.astype(BF)
        near_g[:, kc] = dot_tn(gs_near, qh) * scale
        far_g[:, kc] = (dot_tn(gs_far, qh) * scale).astype(BF)
        near_g[:, vc] = near_gv
        far_g[:, vc] = far_gv.astype(BF)
        for k in range(3):
            back_tick(3 * h + k)

        @pl.when(h == heads // 2)
        def _():
            rs.absorb(here.m)
            rs.launch(here.m - 1)

        return 0

    lax.fori_loop(0, heads, head, 0)
    swap = remote(far_g, got_g, kv_s.at[0], kv_r.at[0], here.sib)
    swap.start()
    for s in range(here.m - 1, 1, -1):
        rs.absorb(s)
        rs.launch(s - 1)

    def out_other(i):
        value = dot_tn(ctx[...], gb[:, cols_of(os.shard(i, True))])
        ov[:, cols_of(i)] = value.astype(BF)
        os.cross(i).start()

    def out_own(i):
        value = dot_tn(ctx[...], gb[:, cols_of(os.shard(i, False))])
        os.cross(i).wait_recv()
        os.combine(i, value)

    swap.wait_recv()

    def add_rows(i, total):
        rows = pl.ds(al(i * 128, 128), 128)
        low = (near_g[rows, :] + got_g[rows, :].astype(F32)).astype(BF)
        grads[rows, width:] = low
        back_tick(3 * heads + i)
        both = jnp.concatenate([grads[rows, 0:width], low[:, width:]], axis=1).astype(F32)
        return total + jnp.sum(both, axis=0, keepdims=True)

    sm[3:4, 0 : 2 * width] = lax.fori_loop(
        0, rows_all // 128, add_rows, jnp.zeros((1, 2 * width), F32)
    )
    loads[9].wait()
    wide = model // 4

    def back_part(i, _):
        cols = pl.ds(al(i * wide, wide), wide)
        part[:, cols] = dot_nt(grads[...], av[cols, :]).astype(BF)
        back_tick(first + i)
        return 0

    first = 3 * heads + rows_all // 128

    lax.fori_loop(0, 4, back_part, 0)
    for load in loads[10:]:
        load.wait()

    def final(rows, span, total):
        scaled, spread = norm_rows(tokh[span, :].astype(F32))
        grad = gm[span, :] + norm_back_rows(total, scaled, spread, par[0:1, :])
        norm[rows, :] = grad.astype(BF)
        sm[6:7, :] += jnp.sum(total * scaled, axis=0, keepdims=True)
        sm[7:8, :] += jnp.sum(total, axis=0, keepdims=True)

    def a_other(i):
        value = dot_tn(n1[:, cols_of(sa.shard(i, True))], grads[...])
        av[rows_of(i), :] = value.astype(BF)
        sa.cross(i).start()

    def a_own(i):
        value = dot_tn(n1[:, cols_of(sa.shard(i, False))], grads[...])
        sa.cross(i).wait_recv()
        sa.combine(i, value)

    def branch_sum(i):
        rows = pl.ds(al(i * 64, 64), 64)
        sm[2:3, :] += jnp.sum(gb[rows, :].astype(F32), axis=0, keepdims=True)

    sm[2:3, :] = jnp.zeros((1, model), F32)
    blocks = rows_all // 64
    d = 2 * n_f
    full = d + 2 * n_f
    ticks = max(line.ticks(), d + blocks, full + 2 * here.m)
    plan = [(d, rs.last)]
    room, spots = ticks - full, here.m - 1
    for s in range(here.m, 1, -1):
        k = here.m - s
        plan.append((full + 1 + (room * k) // (2 * spots), functools.partial(ring_step, os, s)))
        plan.append((d + 3 + (ticks - d) // 4 + (room * k) // (2 * spots), functools.partial(ring_step, sa, s)))

    def tick(tau, _):
        line.tick(tau, final)
        span_when(tau, 0, n_f, a_other)
        span_when(tau, n_f, d, a_own)
        span_when(tau, d, d + blocks, branch_sum)
        pl.when(tau == n_f)(lambda: sa.launch(here.m))
        span_when(tau, d, d + n_f, out_other)
        span_when(tau, d + n_f, full, out_own)
        pl.when(tau == d + n_f)(lambda: os.launch(here.m))
        back_tick(first + 4 + tau)
        for at, event in plan:
            pl.when(tau == at)(event)
        return 0

    lax.fori_loop(0, ticks, tick, 0)
    outs.put(norm, tg_o)
    outs.put(r_sum.at[here.f], rg_o)

    def rest(tau, _):
        back_tick(tau)
        return 0

    lax.fori_loop(min(first + 4 + ticks, back_ticks), back_ticks, rest, 0)
    outs.put(lof, lo_o)

    def tp_copy(k):
        spot = tp_small.at[here.side]
        return remote(sm, spot, tp_s.at[k - 1], tp_r.at[here.side], here.tp(k))

    @pl.when(end)
    def _():
        for k in range(1, n_t):
            tp_copy(k).start()

    def tp_landing(side):
        spot = tp_small.at[side]
        return remote(sm, spot, tp_s.at[0], tp_r.at[side], here.tp(1))

    @pl.when(here.t != 0)
    def _():
        tp_landing(0).wait_recv()

    @pl.when(here.t != n_t - 1)
    def _():
        tp_landing(1).wait_recv()

    @pl.when(end)
    def _():
        tp_small[here.side] = sm[...]

    top_rows = lax.broadcasted_iota(jnp.int32, (8, model), 0) < 4
    all_small[here.f] = jnp.where(top_rows, sm[...], tp_small[0] + tp_small[1])
    to_sib = remote(all_small.at[here.f], sib_small, sb_s.at[0], sb_r.at[0], here.sib)
    to_sib.start()
    to_sib.wait()
    all_small[here.f] += sib_small[...]

    def plane_copy(k):
        spot = all_small.at[here.f]
        return remote(spot, spot, pl_s.at[k], pl_r.at[k], here.plane(k))

    def plane_landing(k):
        spot = all_small.at[lax.rem(here.f + n_f - k, n_f)]
        return remote(spot, spot, pl_s.at[k], pl_r.at[k], here.plane(k))

    for k in range(1, n_f):
        plane_copy(k).start()
    os.last()
    outs.put(o_sum.at[here.f], og_o)
    sa.last()
    outs.put(a_sum.at[here.f], ag_o)
    for k in range(1, n_f):
        plane_landing(k).wait_recv()
    total = all_small[0]
    for k in range(1, n_f):
        total = total + all_small[k]
    sib_small[...] = total
    outs.put(sib_small, small_o)
    line.finish_sum()
    line.finish_back()
    back.finish_sum()
    back.finish_back()
    rs.finish(False)
    os.finish()
    sa.finish()
    swap.wait_send()

    @pl.when(end)
    def _():
        for k in range(1, n_t):
            tp_copy(k).wait_send()

    for k in range(1, n_f):
        plane_copy(k).wait_send()
    outs.wait()


def ring_step(scatter, s):
    scatter.absorb(s)
    scatter.launch(s - 1)


def backward(
    n_f, n_t, live, par, sums, tok, gm, mid, p2, gb, ctx, q, kv, probs, n1, full_a, full_o, pr,
    chunks=16, lag=2, chunks2=16, lag2=2,
):
    rows, model = gb.shape
    width, ff = q.shape[1], pr.shape[1]
    shard = model // (2 * n_f)
    sds, dma, v = jax.ShapeDtypeStruct, pltpu.SemaphoreType.DMA, pltpu.VMEM
    outs = (
        sds((rows, model), BF),
        sds((rows, model), BF),
        sds((ff, shard), BF),
        sds((width, shard), BF),
        sds((shard, 3 * width), BF),
        sds((8, model), F32),
    )
    return pl.pallas_call(
        functools.partial(backward_kernel, n_f, n_t, chunks, lag, chunks2, lag2),
        out_shape=outs,
        in_specs=[pl.BlockSpec(memory_space=pltpu.SMEM)] + [VM] * 2 + [ANY] * 13,
        out_specs=(ANY,) * len(outs),
        scratch_shapes=[
            v((model, 3 * width), BF), v((width, model), BF), v((rows, model), BF),
            v((rows, model), BF), v((rows // 2, model), BF), v((rows // 2, model), F32),
            v((rows, width), BF), v((rows, width), BF), v((2, rows, 2 * width), BF),
            v((width // HD, rows, 2 * rows), BF),
            v((rows, width), BF), v((rows, 3 * width), BF), v((rows, 2 * width), F32),
            v((rows, 2 * width), BF), v((rows, 2 * width), BF), v((rows, model), BF),
            v((rows, model), BF), v((rows // 2, model), F32), v((2, rows // 2, model), BF),
            v((rows, model), BF), v((rows, model), BF), v((2, rows // 2, model), BF),
            v((8, model), F32), v((2, 8, model), F32), v((8, model), F32),
            v((n_f, 8, model), F32),
        ]
        + Scatter.buffers(n_f, ff, shard)
        + Scatter.buffers(n_f, width, shard)
        + Scatter.buffers(n_f, shard, 3 * width)
        + Scatter.sems(n_f) * 3
        + Line.sems(chunks)
        + Line.sems(chunks2)
        + [dma((1,)), dma((1,)), dma((n_t - 1,)), dma((2,)), dma((1,)), dma((1,))]
        + [dma((n_f,)), dma((n_f,)), dma((13,)), dma((6,))],
        compiler_params=pltpu.CompilerParams(
            collective_id=2, has_side_effects=True, vmem_limit_bytes=63 << 20
        ),
        cost_estimate=pl.CostEstimate(
            flops=14 * 10**9, bytes_accessed=40 * 10**6, transcendentals=4 * 10**6
        ),
        name="attention_backward",
    )(live, par, sums, tok, gm, mid, p2, gb, ctx, q, kv, probs, n1, full_a, full_o, pr)


def finish_kernel(
    n_f, total, lo_i, tg_i, e_i, r_i, a_i, o_i,
    lo_o, tg_o, e_o, r_o, q_o, k_o, v_o, o_o, g1_o, s1_o, bo_o, g2_o, s2_o, br_o, bq_o, bv_o, be_o,
    lo, tg, e, r, a, o, e32, r32, a32, o32, in_sem, out_sem,
):
    me = 2 * lax.axis_index("fsdp") + lax.axis_index("ctx")
    shard, width = q_o.shape
    parts = 4

    def slab(ref, i):
        size = ref.shape[0] // parts
        return ref.at[pl.ds(i * size, size)]

    def load(n, src, dst):
        found = [
            pltpu.make_async_copy(slab(src, i), slab(dst, i), in_sem.at[n, i]) for i in range(parts)
        ]
        for copy in found:
            copy.start()
        return found

    outs = Outs(out_sem)
    loads = [load(n, *pair) for n, pair in enumerate(((e_i, e), (r_i, r), (lo_i, lo), (a_i, a), (o_i, o), (tg_i, tg)))]

    def widen(found, src, dst, out):
        size = src.shape[0] // parts
        for i, copy in enumerate(found):
            copy.wait()
            rows = pl.ds(i * size, size)
            dst[rows, :] = src[rows, :].astype(F32)
            outs.put(slab(dst, i), slab(out, i))

    def pass_on(found, src, out):
        for i, copy in enumerate(found):
            copy.wait()
            outs.put(slab(src, i), slab(out, i))

    widen(loads[0], e, e32, e_o)
    widen(loads[1], r, r32, r_o)
    pass_on(loads[2], lo, lo_o.at[0])
    for copy in loads[3]:
        copy.wait()
    for k, out in enumerate((q_o, k_o, v_o)):
        a32[k] = a[:, k * width : (k + 1) * width].astype(F32)
        outs.put(a32.at[k], out)
    widen(loads[4], o, o32, o_o)
    pass_on(loads[5], tg, tg_o.at[0])
    for k, out in ((0, br_o), (2, bo_o), (4, g2_o), (5, s2_o), (6, g1_o), (7, s1_o)):
        out[...] = total[k : k + 1, pl.ds(al(me * shard, shard), shard)]

    def take_bias(out, line, base):
        count, piece = out.shape
        size = piece * 2 * n_f
        wide = jnp.concatenate(
            [total[line : line + 1, base + h * size : base + (h + 1) * size] for h in range(count)]
        )
        out[...] = lax.dot_general(
            wide, picker(me, piece, 2 * n_f), (((1,), (1,)), ((), ())),
            precision=lax.Precision.HIGHEST, preferred_element_type=F32,
        )

    take_bias(bq_o, 3, 0)
    take_bias(bv_o, 3, width)
    take_bias(be_o, 1, 0)
    outs.wait()


def finish(n_f, total, lo, tg, e, r, a, o, bias, wide_bias):
    (rows, model), (shard, ff), width = lo.shape, e.shape, o.shape[0]
    sds, dma, v = jax.ShapeDtypeStruct, pltpu.SemaphoreType.DMA, pltpu.VMEM
    big = [(1, rows, model)] * 2 + [(shard, ff), (ff, shard)] + [(shard, width)] * 3 + [(width, shard)]
    outs = tuple(sds(shape, BF if i < 2 else F32) for i, shape in enumerate(big))
    outs += (sds((1, shard), F32),) * 6
    outs += (sds(bias.shape, F32),) * 2 + (sds(wide_bias.shape, F32),)
    return pl.pallas_call(
        functools.partial(finish_kernel, n_f),
        out_shape=outs,
        in_specs=[VM] + [HBM] * 6,
        out_specs=(HBM,) * 8 + (VM,) * 9,
        scratch_shapes=[v(x.shape, BF) for x in (lo, tg, e, r, a, o)]
        + [v((shard, ff), F32), v((ff, shard), F32), v((3, shard, width), F32), v((width, shard), F32)]
        + [dma((6, 4)), dma((24,))],
        compiler_params=pltpu.CompilerParams(vmem_limit_bytes=60 << 20),
        cost_estimate=pl.CostEstimate(flops=10**6, bytes_accessed=18 * 10**6, transcendentals=0),
        name="finish",
    )(total, lo, tg, e, r, a, o)


def local(
    tokens, cotangent, block_ids, live_count, first_gain, first_shift, query_weight, query_bias,
    key_weight, value_weight, value_bias, output_weight, output_bias, second_gain, second_shift,
    expand_weight, expand_bias, reduce_weight, reduce_bias,
):
    n_f, n_t = lax.axis_size("fsdp"), lax.axis_size("tp")
    _, rows, model = tokens.shape
    tok = tokens.reshape(rows, model)
    vectors = (first_gain, first_shift, output_bias, second_gain, second_shift, reduce_bias)
    n1, q, kv, ctx, probs, n2, mid, par, full_a, full_o, full_e, full_r = forward(
        n_f, n_t, tok, block_ids, vectors, (query_bias, value_bias, expand_bias),
        query_weight, key_weight, value_weight, output_weight, expand_weight, reduce_weight,
    )
    gb, p2, gm, e_grad, r_part, sums = middle(
        n_f, n_t, live_count, n2, cotangent.reshape(rows, model), mid, par, full_e, full_r, reduce_weight
    )
    lo, tg, r_grad, o_grad, a_grad, total = backward(
        n_f, n_t, live_count, par, sums, tok, gm, mid, p2, gb, ctx, q, kv, probs, n1, full_a, full_o, r_part
    )
    (
        layer_out, tokens_grad, e_grad, r_grad, q_grad, k_grad, v_grad, o_grad,
        g1, s1, b_o, g2, s2, b_r, b_q, b_v, b_e,
    ) = finish(n_f, total, lo, tg, e_grad, r_grad, a_grad, o_grad, query_bias, expand_bias)
    flat = lambda vector: vector.reshape(-1)
    return (
        layer_out, tokens_grad, flat(g1), flat(s1), q_grad, b_q, k_grad, v_grad, b_v, o_grad,
        flat(b_o), flat(g2), flat(s2), e_grad, b_e, r_grad, flat(b_r),
    )


def solution(mesh):
    tokens, vector = P("fsdp", "ctx", None), P(("fsdp", "ctx"))
    down, across = P(("fsdp", "ctx"), "tp"), P("tp", ("fsdp", "ctx"))
    return jax.shard_map(
        local,
        mesh=mesh,
        in_specs=(
            tokens, tokens, P("fsdp", None), P("fsdp"), vector, vector, down, across, down, down,
            across, across, vector, vector, vector, down, across, across, vector,
        ),
        out_specs=(
            tokens, tokens, vector, vector, down, across, down, down, across, across, vector,
            vector, vector, down, across, across, vector,
        ),
        check_vma=False,
    )
```

```python
import functools
import math

import jax
import jax.numpy as jnp
from jax import lax
from jax.experimental import pallas as pl
from jax.experimental.pallas import tpu as pltpu
from jax.sharding import PartitionSpec as P

HD = 128
NEG = -1e30
MESH = pl.DeviceIdType.MESH
ANY = pl.BlockSpec(memory_space=pl.ANY)
HBM = pl.BlockSpec(memory_space=pltpu.HBM)
VM = pl.BlockSpec(memory_space=pltpu.VMEM)
BF = jnp.bfloat16
F32 = jnp.float32
epsilon = 1e-05
TILES = 4
LATE = 1


def dot(left, right):
    return lax.dot_general(left, right, (((1,), (0,)), ((), ())), preferred_element_type=F32)


def dot_nt(left, right):
    return lax.dot_general(left, right, (((1,), (1,)), ((), ())), preferred_element_type=F32)


def dot_tn(left, right):
    return lax.dot_general(left, right, (((0,), (0,)), ((), ())), preferred_element_type=F32)


def al(value, step):
    return pl.multiple_of(value, step)


class Place:
    def __init__(self, n_f, n_t):
        self.n_f, self.n_t, self.m = n_f, n_t, n_f // 2
        self.f = lax.axis_index("fsdp")
        self.c = lax.axis_index("ctx")
        self.t = lax.axis_index("tp")
        self.p = self.spot(self.f)
        self.side = self.t // (n_t - 1)
        self.right = (self.owner(1), self.c, self.t)
        self.left = (self.owner(-1), self.c, self.t)
        self.sib = (self.f, 1 - self.c, self.t)

    def spot(self, g):
        a = g // self.m
        return (1 - a) * g + a * (self.n_f - 1 + self.m - g)

    def owner(self, k):
        return self.spot(lax.rem(self.p + k + self.n_f, self.n_f))

    def shard(self, k, other=False):
        c = 1 - self.c if other else self.c
        return 2 * self.owner(k) + c

    def tp(self, d):
        return (self.f, self.c, lax.rem(self.t + d + self.n_t, self.n_t))

    def plane(self, k):
        return (lax.rem(self.f + k, self.n_f), self.c, self.t)

    def greet_signal(self):
        bar = pltpu.get_barrier_semaphore()
        others = [self.sib] + [self.plane(k) for k in range(1, self.n_f)]
        others += [self.tp(k) for k in range(1, self.n_t)]
        for other in others:
            pl.semaphore_signal(bar, 1, device_id=other, device_id_type=MESH)

    def greet_wait(self):
        pl.semaphore_wait(pltpu.get_barrier_semaphore(), self.n_f + self.n_t - 1)

    def greet(self):
        self.greet_signal()
        self.greet_wait()


def remote(src, dst, send, recv, to):
    return pltpu.make_async_remote_copy(
        src_ref=src, dst_ref=dst, send_sem=send, recv_sem=recv, device_id=to, device_id_type=MESH
    )


class Gather:
    def __init__(self, here, own, slot, send, recv):
        self.here, self.own, self.slot, self.send, self.recv = here, own, slot, send, recv
        self.m = here.m

    def half(self, way, s):
        return None if s < self.m else way

    def hop(self, way, s):
        here, sign = self.here, (-1, 1)[way]
        part = self.half(way, s)
        idx = here.shard(sign * (s - 1))
        src = self.own(part) if s == 1 else self.slot(idx, part)
        k = way * self.m + s - 1
        to = (here.right, here.left)[way]
        return remote(src, self.slot(idx, part), self.send.at[k], self.recv.at[k], to)

    def landing(self, way, s):
        here, sign = self.here, (-1, 1)[way]
        part = self.half(way, s)
        ref = self.slot(here.shard(sign * s), part)
        k = way * self.m + s - 1
        to = (here.right, here.left)[way]
        return remote(ref, ref, self.send.at[k], self.recv.at[k], to)

    def cross(self, k, offset, other=False):
        here = self.here
        ref = self.slot(here.shard(offset, other), None)
        src = self.own(None) if (offset == 0 and not other) else ref
        n = 2 * self.m + k
        return remote(src, ref, self.send.at[n], self.recv.at[n], here.sib)

    def crossings(self):
        found = [(0, 0)]
        for s in range(1, self.m):
            found += [(2 * s - 1, -s), (2 * s, s)]
        return found + [(2 * self.m - 1, self.m)]

    def start(self):
        self.hop(0, 1).start()
        self.hop(1, 1).start()
        self.cross(0, 0).start()

    def step(self, s):
        self.landing(0, s).wait_recv()
        self.landing(1, s).wait_recv()
        if s < self.m:
            self.hop(0, s + 1).start()
            self.hop(1, s + 1).start()
            self.cross(2 * s - 1, -s).start()
            self.cross(2 * s, s).start()
        else:
            self.cross(2 * self.m - 1, self.m).start()

    def arrive(self):
        for k, offset in self.crossings():
            self.cross(k, offset, True).wait_recv()

    def finish(self):
        for s in range(1, self.m + 1):
            self.hop(0, s).wait_send()
            self.hop(1, s).wait_send()
        for k, offset in self.crossings():
            self.cross(k, offset).wait_send()

    @staticmethod
    def sems(n_f):
        return 2 * n_f


class Line:
    def __init__(self, here, part, rbuf, norm, sems, chunks, lag):
        self.here, self.part, self.rbuf, self.norm = here, part, rbuf, norm
        self.s_send, self.s_recv, self.g_send, self.g_recv = sems
        self.half = part.shape[0] // 2
        self.nc, self.lag = chunks, lag
        self.cr = self.half // chunks

    def rows(self, d, j):
        return pl.ds(al(d * self.half + j * self.cr, self.cr), self.cr)

    def span(self, j):
        return pl.ds(al(j * self.cr, self.cr), self.cr)

    def s_copy(self, d, j):
        return remote(
            self.part.at[self.rows(d, j)],
            self.rbuf.at[d, self.span(j)],
            self.s_send.at[d, j],
            self.s_recv.at[d, j],
            self.here.tp(2 * d - 1),
        )

    def g_copy(self, d, j):
        ref = self.norm.at[self.rows(d, j)]
        to = self.here.tp(1 - 2 * d)
        return remote(ref, ref, self.g_send.at[d, j], self.g_recv.at[d, j], to)

    def depth(self, d):
        t, n = self.here.t, self.here.n_t
        return t if d == 1 else n - 1 - t

    def sum_step(self, d, tau):
        depth, n = self.depth(d), self.here.n_t
        j = tau - self.lag * depth
        valid = (j >= 0) & (j < self.nc)

        @pl.when(valid & (depth > 0))
        def _():
            self.s_copy(d, j).wait_recv()

        @pl.when(valid & (depth > 0) & (depth < n - 1))
        def _():
            own = self.part[self.rows(d, j), :].astype(F32)
            got = self.rbuf[d, self.span(j), :].astype(F32)
            self.part[self.rows(d, j), :] = (own + got).astype(BF)

        @pl.when(valid & (depth < n - 1))
        def _():
            self.s_copy(d, j).start()

    def owner_step(self, tau, final, back=True):
        here, n = self.here, self.here.n_t
        j = tau - self.lag * (n - 1)
        end = (here.t == 0) | (here.t == n - 1)

        @pl.when(end & (j >= 0) & (j < self.nc))
        def _():
            d = here.side
            rows = self.rows(d, j)
            total = self.part[rows, :].astype(F32) + self.rbuf[d, self.span(j), :].astype(F32)
            final(rows, self.span(j), total)
            if back:
                self.back_copy(j).start()

    def back_copy(self, j):
        here = self.here
        d = here.side
        ref = self.norm.at[self.rows(d, j)]
        return remote(
            ref, ref, self.g_send.at[d, j], self.g_recv.at[d, j], here.tp(1 - 2 * d)
        )

    def gather_step(self, d, tau, base):
        t, n = self.here.t, self.here.n_t
        depth = t if d == 0 else n - 1 - t
        j = tau - base - self.lag * depth
        valid = (j >= 0) & (j < self.nc) & (depth > 0)

        @pl.when(valid)
        def _():
            self.g_copy(d, j).wait_recv()

        @pl.when(valid & (depth < n - 1))
        def _():
            self.g_copy(d, j).start()

    def sum_ticks(self):
        return self.nc + self.lag * (self.here.n_t - 1)

    def ticks(self):
        return self.nc + 2 * self.lag * (self.here.n_t - 1)

    def tick(self, tau, final, back=True):
        self.sum_step(1, tau)
        self.sum_step(0, tau)
        self.owner_step(tau, final, back)
        if back:
            base = self.lag * (self.here.n_t - 1)
            self.gather_step(0, tau, base)
            self.gather_step(1, tau, base)

    def finish_sum(self):
        t, n = self.here.t, self.here.n_t

        def body(j, _):
            @pl.when(t > 0)
            def _():
                self.s_copy(0, j).wait_send()

            @pl.when(t < n - 1)
            def _():
                self.s_copy(1, j).wait_send()

            return 0

        lax.fori_loop(0, self.nc, body, 0)

    def finish_back(self):
        t, n = self.here.t, self.here.n_t

        def body(j, _):
            @pl.when(t < n - 1)
            def _():
                self.g_copy(0, j).wait_send()

            @pl.when(t > 0)
            def _():
                self.g_copy(1, j).wait_send()

            return 0

        lax.fori_loop(0, self.nc, body, 0)

    @staticmethod
    def sems(chunks):
        return [pltpu.SemaphoreType.DMA((2, chunks))] * 4


def norm_rows(values):
    mean = jnp.mean(values, axis=-1, keepdims=True)
    center = values - mean
    spread = lax.rsqrt(jnp.mean(center * center, axis=-1, keepdims=True) + epsilon)
    return center * spread, spread


class Outs:
    def __init__(self, sem):
        self.sem, self.made = sem, []

    def put(self, src, dst):
        copy = pltpu.make_async_copy(src, dst, self.sem.at[len(self.made)])
        copy.start()
        self.made.append(copy)

    def wait(self):
        for copy in self.made:
            copy.wait()


def row_slots(ref, size):
    def slot(idx, part):
        if part is None:
            return ref.at[pl.ds(al(idx * size, size), size)]
        return ref.at[pl.ds(al(idx * size + part * (size // 2), size // 2), size // 2)]

    return slot


def column_slots(ref, width):
    size = ref.shape[0]

    def slot(idx, part):
        cols = pl.ds(al(idx * width, width), width)
        if part is None:
            return ref.at[:, cols]
        return ref.at[pl.ds(part * (size // 2), size // 2), cols]

    return slot


def own_part(ref):
    size = ref.shape[0]

    def own(part):
        if part is None:
            return ref
        return ref.at[pl.ds(part * (size // 2), size // 2)]

    return own


def place_ids(ids, col, row, here):
    rows = col.shape[0]
    row[0:1, :] = ids[:, pl.ds(al(here.c * rows, rows), rows)].astype(F32)
    row[1:2, :] = ids[:, pl.ds(al((1 - here.c) * rows, rows), rows)].astype(F32)
    step = 128

    def turn(i, _):
        start = al(i * step, step)
        down = lax.broadcasted_iota(jnp.int32, (step, rows), 0) + start
        along = lax.broadcasted_iota(jnp.int32, (step, rows), 1)
        kept = jnp.where(down == along, row[0:1, :], 0.0)
        col[pl.ds(start, step), :] = jnp.sum(kept, axis=1, keepdims=True)
        return 0

    lax.fori_loop(0, rows // step, turn, 0)


def picker(index, piece, count):
    down = lax.broadcasted_iota(jnp.int32, (piece, piece * count), 0) + index * piece
    return jnp.where(down == lax.broadcasted_iota(jnp.int32, (piece, piece * count), 1), 1.0, 0.0)


def allowed_scores(q, k, col, row, scale):
    return jnp.where(row <= col, dot_nt(q, k) * scale, NEG)


def forward_kernel(
    n_f, n_t, chunks, lag,
    tok, ids, g1, s1, b_o, g2, s2, b_r, b_q, b_v, b_e, wq, wk, wv, wo, we, wr,
    n1_o, q_o, kv_o, ctx_o, probs_o, n2_o, mid_o, par_o, a_o, o_o, e_o, r_o,
    tokv, n1, full_a, full_o, stage_e, stage_r, q, kv, ctx, part, rbuf, norm, mid,
    probs, col, row, small, sib_small, all_small, par,
    ga_s, ga_r, go_s, go_r, ge_s, ge_r, gr_s, gr_r,
    ls_s, ls_r, lg_s, lg_r, sm_s, sm_r, kv_s, kv_r, in_sem, out_sem,
):
    here = Place(n_f, n_t)
    width = wo.shape[0]
    shard = wq.shape[0]
    rows_all, model = n1.shape
    heads = width // HD
    scale = 1.0 / math.sqrt(HD)
    tok_in = pltpu.make_async_copy(tok, tokv, in_sem.at[0])
    tok_in.start()
    me = 2 * here.f + here.c
    a_slot, o_slot = row_slots(full_a, shard), column_slots(full_o, shard)
    e_slot, r_slot = row_slots(e_o, shard), column_slots(r_o, shard)
    wr = wr.at[pl.ds(0, r_o.shape[0])]
    loads = [
        pltpu.make_async_copy(wo, o_slot(me, None), in_sem.at[1]),
        pltpu.make_async_copy(we, stage_e, in_sem.at[2]),
        pltpu.make_async_copy(wr, stage_r, in_sem.at[3]),
    ]
    mine = pl.ds(al(me * shard, shard), shard)
    for k, w in enumerate((wq, wk, wv)):
        spot = full_a.at[mine, pl.ds(k * width, width)]
        loads.append(pltpu.make_async_copy(w, spot, in_sem.at[4 + k]))
    for load in loads[3:] + loads[:3]:
        load.start()
    here.greet_signal()
    small[...] = jnp.zeros_like(small)
    for k, vector in enumerate((g1, s1, b_o, g2, s2, b_r)):
        small[k : k + 1, mine] = vector[...].astype(F32).reshape(1, shard)

    def put_bias(bias, line, base):
        count, piece = bias.shape
        wide = dot(bias[...].astype(F32), picker(me, piece, 2 * n_f))
        size = piece * 2 * n_f
        for h in range(count):
            small[line : line + 1, base + h * size : base + (h + 1) * size] = wide[h : h + 1, :]

    put_bias(b_q, 6, 0)
    put_bias(b_v, 6, width)
    put_bias(b_e, 7, 0)
    here.greet_wait()
    ga = Gather(here, lambda part: a_slot(me, part), a_slot, ga_s, ga_r)
    go = Gather(here, own_part(wo), o_slot, go_s, go_r)
    ge = Gather(here, own_part(we), e_slot, ge_s, ge_r)
    gr = Gather(here, own_part(wr), r_slot, gr_s, gr_r)
    outs = Outs(out_sem)
    to_sib = remote(small, sib_small, sm_s.at[0], sm_r.at[0], here.sib)
    to_sib.start()
    go.start()
    to_sib.wait_recv()
    all_small[here.f] = small[...] + sib_small[...]

    def small_copy(k):
        spot = all_small.at[here.f]
        return remote(spot, spot, sm_s.at[k], sm_r.at[k], here.plane(k))

    def small_landing(k):
        spot = all_small.at[lax.rem(here.f + n_f - k, n_f)]
        return remote(spot, spot, sm_s.at[k], sm_r.at[k], here.plane(k))

    for k in range(1, n_f):
        small_copy(k).start()
    for load in loads[3:]:
        load.wait()
    ga.start()
    for load in loads[1:3]:
        load.wait()
    outs.put(stage_e, e_slot(me, None))
    outs.put(stage_r, r_slot(me, None))
    for s in range(1, here.m):
        go.step(s)
    for k in range(1, n_f):
        small_landing(k).wait_recv()
    total = all_small[0]
    for k in range(1, n_f):
        total = total + all_small[k]
    par[...] = total
    outs.put(par, par_o)
    tok_in.wait()

    def norm_one(i, _):
        rows = pl.ds(al(i * 64, 64), 64)
        scaled, _spread = norm_rows(tokv[rows, :].astype(F32))
        n1[rows, :] = (scaled * par[0:1, :] + par[1:2, :]).astype(BF)
        return 0

    lax.fori_loop(0, rows_all // 64, norm_one, 0)
    outs.put(n1, n1_o)
    place_ids(ids, col, row, here)
    for s in range(1, here.m):
        ga.step(s)
    gr.start()
    ge.start()
    go.step(here.m)
    ga.step(here.m)
    loads[0].wait()
    ga.arrive()
    q[...] = (dot(n1[...], full_a[:, 0:width]) + par[6:7, 0:width]).astype(BF)
    kv[0, :, 0:width] = dot(n1[...], full_a[:, width : 2 * width]).astype(BF)
    kv[0, :, width : 2 * width] = (
        dot(n1[...], full_a[:, 2 * width : 3 * width]) + par[6:7, width : 2 * width]
    ).astype(BF)
    swap = remote(kv.at[0], kv.at[1], kv_s.at[0], kv_r.at[0], here.sib)
    swap.start()
    outs.put(full_a, a_o)
    outs.put(q, q_o)
    go.arrive()
    outs.put(full_o, o_o)
    swap.wait_recv()
    outs.put(kv, kv_o)
    blk = rows_all // 2

    def head(i, _):
        h = i // 2
        rows = pl.ds(al((i - 2 * h) * blk, blk), blk)
        kc = pl.ds(al(h * HD, HD), HD)
        vc = pl.ds(al(width + h * HD, HD), HD)
        ids = col[rows, :]
        qh = q[rows, kc]
        near = allowed_scores(qh, kv[0, :, kc], ids, row[0:1, :], scale)
        far = allowed_scores(qh, kv[1, :, kc], ids, row[1:2, :], scale)
        top = jnp.maximum(
            jnp.max(near, axis=-1, keepdims=True), jnp.max(far, axis=-1, keepdims=True)
        )
        near = jnp.exp(near - top)
        far = jnp.exp(far - top)
        total = jnp.sum(near, axis=-1, keepdims=True) + jnp.sum(far, axis=-1, keepdims=True)
        inv = 1.0 / total
        near = (near * inv).astype(BF)
        far = (far * inv).astype(BF)
        probs[h, rows, 0:rows_all] = near
        probs[h, rows, rows_all:] = far
        ctx[rows, kc] = (dot(near, kv[0, :, vc]) + dot(far, kv[1, :, vc])).astype(BF)
        return 0

    lax.fori_loop(0, 2 * heads, head, 0)
    outs.put(ctx, ctx_o)
    outs.put(probs, probs_o)

    wide = model // 4

    def project(i, _):
        cols = pl.ds(al(i * wide, wide), wide)
        part[:, cols] = dot(ctx[...], full_o[:, cols]).astype(BF)
        return 0

    lax.fori_loop(0, 4, project, 0)
    line = Line(here, part, rbuf, norm, (ls_s, ls_r, lg_s, lg_r), chunks, lag)

    def final(rows, span, total):
        middle = tokv[rows, :].astype(F32) + total + par[2:3, :]
        mid[span, :] = middle
        scaled, _spread = norm_rows(middle)
        norm[rows, :] = (scaled * par[3:4, :] + par[4:5, :]).astype(BF)

    ticks = line.ticks()
    events = []
    for s in range(1, here.m):
        events += [functools.partial(gr.step, s), functools.partial(ge.step, s)]
    when = [1 + (ticks // 2) * i // max(1, len(events) - 1) for i in range(len(events))]
    events.append(functools.partial(gr.step, here.m))
    when.append(ticks - 2)

    def tick(tau, _):
        line.tick(tau, final)
        for at, event in zip(when, events):
            pl.when(tau == at)(event)
        return 0

    lax.fori_loop(0, ticks, tick, 0)
    outs.put(mid, mid_o)
    outs.put(norm, n2_o)
    ge.step(here.m)
    gr.arrive()
    ge.arrive()
    line.finish_sum()
    line.finish_back()
    for gather in (ga, go, gr, ge):
        gather.finish()
    to_sib.wait_send()
    for k in range(1, n_f):
        small_copy(k).wait_send()
    swap.wait_send()
    outs.wait()


def forward(n_f, n_t, tok, ids, vectors, biases, wq, wk, wv, wo, we, wr, chunks=16, lag=2):
    rows, model = tok.shape
    shard, width, ff = wq.shape[0], wo.shape[0], we.shape[1]
    early = ff - LATE * (ff // TILES)
    sds = jax.ShapeDtypeStruct
    dma = pltpu.SemaphoreType.DMA
    outs = (
        sds((rows, model), BF),
        sds((rows, width), BF),
        sds((2, rows, 2 * width), BF),
        sds((rows, width), BF),
        sds((width // HD, rows, 2 * rows), BF),
        sds((rows, model), BF),
        sds((rows // 2, model), F32),
        sds((8, model), F32),
        sds((model, 3 * width), BF),
        sds((width, model), BF),
        sds((model, ff), BF),
        sds((early, model), BF),
    )
    v = pltpu.VMEM
    return pl.pallas_call(
        functools.partial(forward_kernel, n_f, n_t, chunks, lag),
        out_shape=outs,
        in_specs=[ANY] + [VM] * 10 + [ANY] * 6,
        out_specs=(ANY,) * len(outs),
        scratch_shapes=[
            v((rows, model), BF), v((rows, model), BF), v((model, 3 * width), BF),
            v((width, model), BF), v((shard, ff), BF), v((early, shard), BF),
            v((rows, width), BF), v((2, rows, 2 * width), BF), v((rows, width), BF),
            v((rows, model), BF), v((2, rows // 2, model), BF), v((rows, model), BF),
            v((rows // 2, model), F32), v((width // HD, rows, 2 * rows), BF),
            v((rows, 1), F32), v((2, rows), F32), v((8, model), F32),
            v((8, model), F32), v((n_f, 8, model), F32), v((8, model), F32),
        ]
        + [dma((Gather.sems(n_f),))] * 8
        + Line.sems(chunks)
        + [dma((n_f,)), dma((n_f,)), dma((1,)), dma((1,)), dma((7,)), dma((16,))],
        compiler_params=pltpu.CompilerParams(
            collective_id=0, has_side_effects=True, vmem_limit_bytes=60 << 20
        ),
        cost_estimate=pl.CostEstimate(
            flops=8 * 10**9, bytes_accessed=60 * 10**6, transcendentals=10**6
        ),
        name="attention_forward",
    )(tok, ids, *vectors, *biases, wq, wk, wv, wo, we, wr)


class Scatter:
    def __init__(self, here, sums, stage, ring_half, ring_full, send, recv, block):
        self.here, self.sums, self.stage = here, sums, stage
        self.ring_half, self.ring_full = ring_half, ring_full
        self.send, self.recv, self.block = send, recv, block
        self.m, self.size = here.m, sums.shape[1]

    def offset(self, i):
        odd = lax.rem(i, 2)
        return self.m + (1 - 2 * odd) * ((i + 1) // 2)

    def shard(self, i, other):
        return self.here.shard(self.offset(i), other)

    def cross(self, i):
        slot = self.sums.at[self.here.owner(self.offset(i))]
        n = 2 * self.m + i
        return remote(self.stage(i), slot, self.send.at[n], self.recv.at[n], self.here.sib)

    def combine(self, i, own):
        f = self.here.owner(self.offset(i))
        self.sums[f] = (own + self.sums[f].astype(F32)).astype(BF)

    def slot(self, k, half):
        f = self.here.owner(k)
        if half is None:
            return self.sums.at[f]
        return self.sums.at[f, pl.ds(half * (self.size // 2), self.size // 2)]

    def hop(self, way, s):
        here, sign = self.here, (1, -1)[way]
        half = way if s == self.m else None
        dst = self.ring_half.at[way] if s == self.m else self.ring_full.at[way, s - 1]
        n = way * self.m + s - 1
        to = (here.right, here.left)[way]
        return remote(self.slot(sign * s, half), dst, self.send.at[n], self.recv.at[n], to)

    def launch(self, s):
        self.hop(0, s).start()
        self.hop(1, s).start()

    def absorb(self, s):
        for way in (0, 1):
            sign = (1, -1)[way]
            self.hop(way, s).wait_recv()
            f = self.here.owner(sign * (s - 1))
            base = way * (self.size // 2) if s == self.m else 0
            count = (self.size // 2 if s == self.m else self.size) // self.block

            def body(i, _, way=way, f=f, base=base):
                there = pl.ds(al(base + i * self.block, self.block), self.block)
                here_rows = pl.ds(al(i * self.block, self.block), self.block)
                if s == self.m:
                    got = self.ring_half[way, here_rows, :]
                else:
                    got = self.ring_full[way, s - 1, here_rows, :]
                self.sums[f, there, :] = (
                    self.sums[f, there, :].astype(F32) + got.astype(F32)
                ).astype(BF)
                return 0

            lax.fori_loop(0, count, body, 0)

    def last(self):
        self.hop(0, 1).wait_recv()
        self.hop(1, 1).wait_recv()
        f = self.here.owner(0)

        def body(i, _):
            rows = pl.ds(al(i * self.block, self.block), self.block)
            total = self.sums[f, rows, :].astype(F32) + self.ring_full[0, 0, rows, :].astype(F32)
            total = total + self.ring_full[1, 0, rows, :].astype(F32)
            self.sums[f, rows, :] = total.astype(BF)
            return 0

        lax.fori_loop(0, self.size // self.block, body, 0)

    def finish(self, crossed=True):
        for s in range(1, self.m + 1):
            self.hop(0, s).wait_send()
            self.hop(1, s).wait_send()
        if crossed:
            for i in range(2 * self.m):
                self.cross(i).wait_send()

    @staticmethod
    def buffers(n_f, rows, cols):
        v = pltpu.VMEM
        m = n_f // 2
        return [
            v((n_f, rows, cols), BF),
            v((2, rows // 2, cols), BF),
            v((2, max(1, m - 1), rows, cols), BF),
        ]

    @staticmethod
    def sems(n_f):
        return [pltpu.SemaphoreType.DMA((2 * n_f,))] * 2


def norm_back_rows(total, scaled, spread, gain):
    e = total * gain
    inner = (
        e
        - jnp.mean(e, axis=-1, keepdims=True)
        - scaled * jnp.mean(e * scaled, axis=-1, keepdims=True)
    )
    return inner * spread


def span_when(tau, start, stop, task):
    @pl.when((tau >= start) & (tau < stop))
    def _():
        task(tau - start)


def middle_kernel(
    n_f, n_t, chunks, lag,
    live, n2_i, cot, mid_i, par, full_e, full_r, wr,
    gb_o, p2_o, gm_o, eg_o, pr_o, sums_o,
    ev, rv, n2, g, act, gh, part, part2, rbuf, gb, mid, gm, sums,
    e_sum, e_half, e_full, r_sum,
    e_s, e_r, r_s, r_r, gl_s, gl_r,
    ls_s, ls_r, lg_s, lg_r, in_sem, te_sem, tr_sem, out_sem,
):
    here = Place(n_f, n_t)
    rows_all, model = n2.shape
    ff = act.shape[1]
    shard = e_sum.shape[1]
    tiles = TILES
    ft = ff // tiles
    early = full_r.shape[0]
    late = ff - early
    here.greet_signal()
    late_own = wr.at[pl.ds(early, late)]
    late_slot = column_slots(rv.at[pl.ds(early, late)], shard)
    gl = Gather(here, own_part(late_own), late_slot, gl_s, gl_r)

    def e_load(i):
        cols = pl.ds(i * ft, ft)
        return pltpu.make_async_copy(full_e.at[:, cols], ev.at[:, cols], te_sem.at[i])

    def r_load(i):
        rows = pl.ds(i * ft, ft)
        return pltpu.make_async_copy(full_r.at[rows], rv.at[rows], tr_sem.at[i])

    loads = [
        pltpu.make_async_copy(n2_i, n2, in_sem.at[0]),
        pltpu.make_async_copy(cot, g, in_sem.at[1]),
        pltpu.make_async_copy(mid_i, mid, in_sem.at[2]),
        pltpu.make_async_copy(late_own, late_slot(2 * here.f + here.c, None), in_sem.at[3]),
    ]
    loads[0].start()
    e_load(0).start()
    loads[1].start()
    for i in range(1, tiles):
        e_load(i).start()
    for i in range(early // ft):
        r_load(i).start()
    loads[3].start()
    loads[2].start()
    here.greet_wait()
    gl.start()
    alive = live[0].astype(F32)
    loads[0].wait()
    loads[1].wait()
    sums[...] = jnp.zeros_like(sums)

    def mask(i, total):
        rows = pl.ds(al(i * 64, 64), 64)
        value = g[rows, :].astype(F32) * alive
        g[rows, :] = value.astype(BF)
        return total + jnp.sum(value, axis=0, keepdims=True)

    sums[0:1, :] = lax.fori_loop(0, rows_all // 64, mask, jnp.zeros((1, model), F32))

    def hidden_tile(i):
        cols = pl.ds(i * ft, ft)
        e_load(i).wait()
        h = dot(n2[...], ev[:, cols]) + par[7:8, cols]
        bell = 0.5 * (1.0 + lax.erf(h * (1.0 / math.sqrt(2.0))))
        act[:, cols] = (h * bell).astype(BF)
        slope = bell + h * jnp.exp(-0.5 * h * h) * (1.0 / math.sqrt(2.0 * math.pi))
        gh[:, cols] = slope.astype(BF)

    def grad_piece(cols):
        low = (dot_nt(g[...], rv[cols, :]) * gh[:, cols].astype(F32)).astype(BF)
        gh[:, cols] = low
        sums[1:2, cols] = jnp.sum(low.astype(F32), axis=0, keepdims=True)

    for i in range(tiles):
        hidden_tile(i)
    for s in range(1, here.m):
        gl.step(s)
    for i in range(early // ft):
        r_load(i).wait()
        grad_piece(pl.ds(i * ft, ft))
    gl.step(here.m)
    loads[3].wait()
    gl.arrive()
    line = Line(here, part, rbuf, gb, (ls_s, ls_r, lg_s, lg_r), chunks, lag)
    outs = Outs(out_sem)

    def final(rows, span, total):
        scaled, spread = norm_rows(mid[span, :])
        grad = g[rows, :].astype(F32) + norm_back_rows(total, scaled, spread, par[3:4, :])
        gm[span, :] = grad
        gb[rows, :] = grad.astype(BF)
        sums[4:5, :] += jnp.sum(total * scaled, axis=0, keepdims=True)
        sums[5:6, :] += jnp.sum(total, axis=0, keepdims=True)

    def mlp(i):
        cols = pl.ds(al(i * shard, shard), shard)
        part2[:, cols] = dot(act[...], rv[:, cols]).astype(BF)

    loads[2].wait()
    piece = ft // 2
    pieces, backs = late // piece, 8
    wide = model // backs

    def grad_step(i, _):
        grad_piece(pl.ds(al(early + i * piece, piece), piece))
        return 0

    def back_step(i, _):
        cols = pl.ds(al(i * wide, wide), wide)
        part[:, cols] = dot_nt(gh[...], ev[cols, :]).astype(BF)
        return 0

    lax.fori_loop(0, pieces, grad_step, 0)
    lax.fori_loop(0, backs, back_step, 0)
    gl.finish()

    def e_stage(i):
        return ev.at[pl.ds(al(i * shard, shard), shard)]

    def r_stage(i):
        return rv.at[:, pl.ds(al(i * shard, shard), shard)]

    def cols_of(i):
        return pl.ds(al(i * shard, shard), shard)

    es = Scatter(here, e_sum, e_stage, e_half, e_full, e_s, e_r, 64)
    rs = Scatter(here, r_sum, r_stage, None, None, r_s, r_r, 256)

    def e_other(i):
        value = dot_tn(n2[:, cols_of(es.shard(i, True))], gh[...])
        ev[pl.ds(al(i * shard, shard), shard), :] = value.astype(BF)
        es.cross(i).start()

    def e_own(i):
        value = dot_tn(n2[:, cols_of(es.shard(i, False))], gh[...])
        es.cross(i).wait_recv()
        es.combine(i, value)

    def r_other(i):
        value = dot_tn(act[...], g[:, cols_of(rs.shard(i, True))])
        rv[:, cols_of(i)] = value.astype(BF)
        rs.cross(i).start()

    def r_own(i):
        value = dot_tn(act[...], g[:, cols_of(rs.shard(i, False))])
        rs.cross(i).wait_recv()
        rs.combine(i, value)

    a, b = n_f, 2 * n_f
    d = b + 2 * n_f
    ticks = max(line.ticks(), d + 2 * n_f)
    gap = max(1, (ticks - b) // (n_f // 2 + 1))

    def tick(tau, _):
        line.tick(tau, final)
        span_when(tau, 0, a, e_other)
        span_when(tau, a, b, e_own)
        span_when(tau, b, d, mlp)
        span_when(tau, d, d + n_f, r_other)
        span_when(tau, d + n_f, d + 2 * n_f, r_own)

        @pl.when(tau == a)
        def _():
            es.launch(here.m)

        for s in range(here.m, 1, -1):

            @pl.when(tau == b + gap * (here.m - s + 1) - 1)
            def _(s=s):
                es.absorb(s)
                es.launch(s - 1)

        return 0

    lax.fori_loop(0, ticks, tick, 0)
    outs.put(gb, gb_o)
    outs.put(gm, gm_o)
    outs.put(part2, p2_o)
    outs.put(r_sum, pr_o)
    outs.put(sums, sums_o)
    es.last()
    outs.put(e_sum.at[here.f], eg_o)
    line.finish_sum()
    line.finish_back()
    es.finish()
    for i in range(n_f):
        rs.cross(i).wait_send()
    outs.wait()


def middle(n_f, n_t, live, n2, cot, mid, par, full_e, full_r, wr, chunks=16, lag=2):
    rows, model = n2.shape
    ff = full_e.shape[1]
    shard = model // (2 * n_f)
    sds, dma, v = jax.ShapeDtypeStruct, pltpu.SemaphoreType.DMA, pltpu.VMEM
    outs = (
        sds((rows, model), BF),
        sds((rows, model), BF),
        sds((rows // 2, model), F32),
        sds((shard, ff), BF),
        sds((n_f, ff, shard), BF),
        sds((8, model), F32),
    )
    return pl.pallas_call(
        functools.partial(middle_kernel, n_f, n_t, chunks, lag),
        out_shape=outs,
        in_specs=[pl.BlockSpec(memory_space=pltpu.SMEM), ANY, ANY, ANY, VM, ANY, ANY, ANY],
        out_specs=(ANY,) * len(outs),
        scratch_shapes=[
            v((model, ff), BF), v((ff, model), BF), v((rows, model), BF), v((rows, model), BF),
            v((rows, ff), BF), v((rows, ff), BF), v((rows, model), BF), v((rows, model), BF),
            v((2, rows // 2, model), BF), v((rows, model), BF),
            v((rows // 2, model), F32), v((rows // 2, model), F32),
            v((8, model), F32),
        ]
        + Scatter.buffers(n_f, shard, ff)
        + [v((n_f, ff, shard), BF)]
        + Scatter.sems(n_f)
        + Scatter.sems(n_f)
        + [dma((Gather.sems(n_f),))] * 2
        + Line.sems(chunks)
        + [dma((4,)), dma((4,)), dma((4,)), dma((6,))],
        compiler_params=pltpu.CompilerParams(
            collective_id=1, has_side_effects=True, vmem_limit_bytes=63 << 20
        ),
        cost_estimate=pl.CostEstimate(
            flops=26 * 10**9, bytes_accessed=40 * 10**6, transcendentals=4 * 10**6
        ),
        name="feed_forward",
    )(live, n2, cot, mid, par, full_e, full_r, wr)


def backward_kernel(
    n_f, n_t, chunks, lag, chunks2, lag2,
    live, par, sums_i, tok, gm_i, mid_i, p2_i, gb_i, ctx_i, q_i, kv_i, probs_i, n1_i, full_a, full_o, pr_i,
    lo_o, tg_o, rg_o, og_o, ag_o, small_o,
    av, ov, gb, n1, tokh, gm, ctx, q, kv, probs, gc, grads, near_g, far_g, got_g, lof, p2, mid, rbuf2, norm, part, rbuf,
    sm, tp_small, sib_small, all_small,
    r_sum, r_half, r_full, o_sum, o_half, o_full, a_sum, a_half, a_full,
    r_s, r_r, o_s, o_r, a_s, a_r,
    ls_s, ls_r, lg_s, lg_r, ms_s, ms_r, mg_s, mg_r,
    kv_s, kv_r, tp_s, tp_r, sb_s, sb_r, pl_s, pl_r, in_sem, out_sem,
):
    here = Place(n_f, n_t)
    rows_all, model = gb.shape
    width = q.shape[1]
    shard = a_sum.shape[1]
    heads = width // HD
    half = rows_all // 2
    scale = 1.0 / math.sqrt(HD)
    here.greet_signal()
    mine = pl.ds(al(here.side * half, half), half)
    pairs = [
        (gb_i, gb), (full_o, ov), (p2_i, p2), (mid_i, mid), (pr_i, r_sum), (q_i, q), (kv_i, kv), (probs_i, probs), (ctx_i, ctx),
        (full_a, av), (n1_i, n1), (gm_i, gm), (tok.at[mine], tokh),
    ]
    loads = [pltpu.make_async_copy(s, d, in_sem.at[i]) for i, (s, d) in enumerate(pairs)]
    for load in loads:
        load.start()
    end = (here.t == 0) | (here.t == n_t - 1)
    sm[...] = sums_i[...]
    loads[0].wait()
    loads[1].wait()
    gc[...] = dot_nt(gb[...], ov[...]).astype(BF)
    for load in loads[2:5]:
        load.wait()
    here.greet_wait()
    alive = live[0].astype(F32)
    outs = Outs(out_sem)
    line = Line(here, part, rbuf, norm, (ls_s, ls_r, lg_s, lg_r), chunks, lag)
    back = Line(here, p2, rbuf2, lof, (ms_s, ms_r, mg_s, mg_r), chunks2, lag2)

    back_ticks = back.ticks()

    def final2(rows, span, total):
        lof[rows, :] = ((mid[span, :] + total + par[5:6, :]) * alive).astype(BF)

    def back_tick(tau):
        back.tick(tau, final2)

    def cols_of(i):
        return pl.ds(al(i * shard, shard), shard)

    def rows_of(i):
        return pl.ds(al(i * shard, shard), shard)

    rs = Scatter(here, r_sum, None, r_half, r_full, r_s, r_r, 256)
    os = Scatter(here, o_sum, lambda i: ov.at[:, cols_of(i)], o_half, o_full, o_s, o_r, 128)
    sa = Scatter(here, a_sum, lambda i: av.at[rows_of(i)], a_half, a_full, a_s, a_r, 64)
    rs.launch(here.m)
    for load in loads[5:9]:
        load.wait()

    def head(h, _):
        kc = pl.ds(al(h * HD, HD), HD)
        vc = pl.ds(al(width + h * HD, HD), HD)
        qh, gh = q[:, kc], gc[:, kc]
        near_low, far_low = probs[h, :, 0:rows_all], probs[h, :, rows_all:]
        near_gv, far_gv = dot_tn(near_low, gh), dot_tn(far_low, gh)
        near, far = near_low.astype(F32), far_low.astype(F32)
        gp_near = dot_nt(gh, kv[0, :, vc])
        gp_far = dot_nt(gh, kv[1, :, vc])
        inner = jnp.sum(gp_near * near, axis=-1, keepdims=True) + jnp.sum(
            gp_far * far, axis=-1, keepdims=True
        )
        gs_near = (near * (gp_near - inner)).astype(BF)
        gs_far = (far * (gp_far - inner)).astype(BF)
        gq = (dot(gs_near, kv[0, :, kc]) + dot(gs_far, kv[1, :, kc])) * scale
        grads[:, kc] = gq.astype(BF)
        near_g[:, kc] = dot_tn(gs_near, qh) * scale
        far_g[:, kc] = (dot_tn(gs_far, qh) * scale).astype(BF)
        near_g[:, vc] = near_gv
        far_g[:, vc] = far_gv.astype(BF)
        for k in range(5):
            back_tick(5 * h + k)

        @pl.when(h == heads // 2)
        def _():
            rs.absorb(here.m)
            rs.launch(here.m - 1)

        return 0

    lax.fori_loop(0, heads, head, 0)
    swap = remote(far_g, got_g, kv_s.at[0], kv_r.at[0], here.sib)
    swap.start()
    for s in range(here.m - 1, 1, -1):
        rs.absorb(s)
        rs.launch(s - 1)

    def out_other(i):
        value = dot_tn(ctx[...], gb[:, cols_of(os.shard(i, True))])
        ov[:, cols_of(i)] = value.astype(BF)
        os.cross(i).start()

    def out_own(i):
        value = dot_tn(ctx[...], gb[:, cols_of(os.shard(i, False))])
        os.cross(i).wait_recv()
        os.combine(i, value)

    swap.wait_recv()

    def add_rows(i, total):
        rows = pl.ds(al(i * 128, 128), 128)
        low = (near_g[rows, :] + got_g[rows, :].astype(F32)).astype(BF)
        grads[rows, width:] = low
        back_tick(5 * heads + i)
        both = jnp.concatenate([grads[rows, 0:width], low[:, width:]], axis=1).astype(F32)
        return total + jnp.sum(both, axis=0, keepdims=True)

    sm[3:4, 0 : 2 * width] = lax.fori_loop(
        0, rows_all // 128, add_rows, jnp.zeros((1, 2 * width), F32)
    )
    loads[9].wait()
    wide = model // 4

    def back_part(i, _):
        cols = pl.ds(al(i * wide, wide), wide)
        part[:, cols] = dot_nt(grads[...], av[cols, :]).astype(BF)
        back_tick(first + i)
        return 0

    first = 5 * heads + rows_all // 128

    lax.fori_loop(0, 4, back_part, 0)
    for load in loads[10:]:
        load.wait()

    def final(rows, span, total):
        scaled, spread = norm_rows(tokh[span, :].astype(F32))
        grad = gm[span, :] + norm_back_rows(total, scaled, spread, par[0:1, :])
        norm[rows, :] = grad.astype(BF)
        sm[6:7, :] += jnp.sum(total * scaled, axis=0, keepdims=True)
        sm[7:8, :] += jnp.sum(total, axis=0, keepdims=True)

    def a_other(i):
        value = dot_tn(n1[:, cols_of(sa.shard(i, True))], grads[...])
        av[rows_of(i), :] = value.astype(BF)
        sa.cross(i).start()

    def a_own(i):
        value = dot_tn(n1[:, cols_of(sa.shard(i, False))], grads[...])
        sa.cross(i).wait_recv()
        sa.combine(i, value)

    def branch_sum(i):
        rows = pl.ds(al(i * 64, 64), 64)
        sm[2:3, :] += jnp.sum(gb[rows, :].astype(F32), axis=0, keepdims=True)

    sm[2:3, :] = jnp.zeros((1, model), F32)
    blocks = rows_all // 64
    d = 2 * n_f
    full = d + 2 * n_f
    ticks = max(line.ticks(), d + blocks, full + 2 * here.m)
    plan = [(d, rs.last)]
    room, spots = ticks - full, here.m - 1
    for s in range(here.m, 1, -1):
        k = here.m - s
        plan.append((full + 1 + (room * k) // (2 * spots), functools.partial(ring_step, os, s)))
        plan.append((d + 3 + (ticks - d) // 4 + (room * k) // (2 * spots), functools.partial(ring_step, sa, s)))

    def tick(tau, _):
        line.tick(tau, final)
        span_when(tau, 0, n_f, a_other)
        span_when(tau, n_f, d, a_own)
        span_when(tau, d, d + blocks, branch_sum)
        pl.when(tau == n_f)(lambda: sa.launch(here.m))
        span_when(tau, d, d + n_f, out_other)
        span_when(tau, d + n_f, full, out_own)
        pl.when(tau == d + n_f)(lambda: os.launch(here.m))
        back_tick(first + 4 + tau)
        for at, event in plan:
            pl.when(tau == at)(event)
        return 0

    lax.fori_loop(0, ticks, tick, 0)
    outs.put(norm, tg_o)
    outs.put(r_sum.at[here.f], rg_o)

    def rest(tau, _):
        back_tick(tau)
        return 0

    lax.fori_loop(min(first + 4 + ticks, back_ticks), back_ticks, rest, 0)
    outs.put(lof, lo_o)

    def tp_copy(k):
        spot = tp_small.at[here.side]
        return remote(sm, spot, tp_s.at[k - 1], tp_r.at[here.side], here.tp(k))

    @pl.when(end)
    def _():
        for k in range(1, n_t):
            tp_copy(k).start()

    def tp_landing(side):
        spot = tp_small.at[side]
        return remote(sm, spot, tp_s.at[0], tp_r.at[side], here.tp(1))

    @pl.when(here.t != 0)
    def _():
        tp_landing(0).wait_recv()

    @pl.when(here.t != n_t - 1)
    def _():
        tp_landing(1).wait_recv()

    @pl.when(end)
    def _():
        tp_small[here.side] = sm[...]

    top_rows = lax.broadcasted_iota(jnp.int32, (8, model), 0) < 4
    all_small[here.f] = jnp.where(top_rows, sm[...], tp_small[0] + tp_small[1])
    to_sib = remote(all_small.at[here.f], sib_small, sb_s.at[0], sb_r.at[0], here.sib)
    to_sib.start()
    to_sib.wait()
    all_small[here.f] += sib_small[...]

    def plane_copy(k):
        spot = all_small.at[here.f]
        return remote(spot, spot, pl_s.at[k], pl_r.at[k], here.plane(k))

    def plane_landing(k):
        spot = all_small.at[lax.rem(here.f + n_f - k, n_f)]
        return remote(spot, spot, pl_s.at[k], pl_r.at[k], here.plane(k))

    for k in range(1, n_f):
        plane_copy(k).start()
    os.last()
    outs.put(o_sum.at[here.f], og_o)
    sa.last()
    outs.put(a_sum.at[here.f], ag_o)
    for k in range(1, n_f):
        plane_landing(k).wait_recv()
    total = all_small[0]
    for k in range(1, n_f):
        total = total + all_small[k]
    sib_small[...] = total
    outs.put(sib_small, small_o)
    line.finish_sum()
    line.finish_back()
    back.finish_sum()
    back.finish_back()
    rs.finish(False)
    os.finish()
    sa.finish()
    swap.wait_send()

    @pl.when(end)
    def _():
        for k in range(1, n_t):
            tp_copy(k).wait_send()

    for k in range(1, n_f):
        plane_copy(k).wait_send()
    outs.wait()


def ring_step(scatter, s):
    scatter.absorb(s)
    scatter.launch(s - 1)


def backward(
    n_f, n_t, live, par, sums, tok, gm, mid, p2, gb, ctx, q, kv, probs, n1, full_a, full_o, pr,
    chunks=16, lag=2, chunks2=16, lag2=2,
):
    rows, model = gb.shape
    width, ff = q.shape[1], pr.shape[1]
    shard = model // (2 * n_f)
    sds, dma, v = jax.ShapeDtypeStruct, pltpu.SemaphoreType.DMA, pltpu.VMEM
    outs = (
        sds((rows, model), BF),
        sds((rows, model), BF),
        sds((ff, shard), BF),
        sds((width, shard), BF),
        sds((shard, 3 * width), BF),
        sds((8, model), F32),
    )
    return pl.pallas_call(
        functools.partial(backward_kernel, n_f, n_t, chunks, lag, chunks2, lag2),
        out_shape=outs,
        in_specs=[pl.BlockSpec(memory_space=pltpu.SMEM)] + [VM] * 2 + [ANY] * 13,
        out_specs=(ANY,) * len(outs),
        scratch_shapes=[
            v((model, 3 * width), BF), v((width, model), BF), v((rows, model), BF),
            v((rows, model), BF), v((rows // 2, model), BF), v((rows // 2, model), F32),
            v((rows, width), BF), v((rows, width), BF), v((2, rows, 2 * width), BF),
            v((width // HD, rows, 2 * rows), BF),
            v((rows, width), BF), v((rows, 3 * width), BF), v((rows, 2 * width), F32),
            v((rows, 2 * width), BF), v((rows, 2 * width), BF), v((rows, model), BF),
            v((rows, model), BF), v((rows // 2, model), F32), v((2, rows // 2, model), BF),
            v((rows, model), BF), v((rows, model), BF), v((2, rows // 2, model), BF),
            v((8, model), F32), v((2, 8, model), F32), v((8, model), F32),
            v((n_f, 8, model), F32),
        ]
        + Scatter.buffers(n_f, ff, shard)
        + Scatter.buffers(n_f, width, shard)
        + Scatter.buffers(n_f, shard, 3 * width)
        + Scatter.sems(n_f) * 3
        + Line.sems(chunks)
        + Line.sems(chunks2)
        + [dma((1,)), dma((1,)), dma((n_t - 1,)), dma((2,)), dma((1,)), dma((1,))]
        + [dma((n_f,)), dma((n_f,)), dma((13,)), dma((6,))],
        compiler_params=pltpu.CompilerParams(
            collective_id=2, has_side_effects=True, vmem_limit_bytes=63 << 20
        ),
        cost_estimate=pl.CostEstimate(
            flops=14 * 10**9, bytes_accessed=40 * 10**6, transcendentals=4 * 10**6
        ),
        name="attention_backward",
    )(live, par, sums, tok, gm, mid, p2, gb, ctx, q, kv, probs, n1, full_a, full_o, pr)


def finish_kernel(
    n_f, total, lo_i, tg_i, e_i, r_i, a_i, o_i,
    lo_o, tg_o, e_o, r_o, q_o, k_o, v_o, o_o, g1_o, s1_o, bo_o, g2_o, s2_o, br_o, bq_o, bv_o, be_o,
    lo, tg, e, r, a, o, e32, r32, a32, o32, in_sem, out_sem,
):
    me = 2 * lax.axis_index("fsdp") + lax.axis_index("ctx")
    shard, width = q_o.shape
    parts = 4

    def slab(ref, i):
        size = ref.shape[0] // parts
        return ref.at[pl.ds(i * size, size)]

    def load(n, src, dst):
        found = [
            pltpu.make_async_copy(slab(src, i), slab(dst, i), in_sem.at[n, i]) for i in range(parts)
        ]
        for copy in found:
            copy.start()
        return found

    outs = Outs(out_sem)
    loads = [load(n, *pair) for n, pair in enumerate(((e_i, e), (r_i, r), (lo_i, lo), (a_i, a), (o_i, o), (tg_i, tg)))]

    def widen(found, src, dst, out):
        size = src.shape[0] // parts
        for i, copy in enumerate(found):
            copy.wait()
            rows = pl.ds(i * size, size)
            dst[rows, :] = src[rows, :].astype(F32)
            outs.put(slab(dst, i), slab(out, i))

    def pass_on(found, src, out):
        for i, copy in enumerate(found):
            copy.wait()
            outs.put(slab(src, i), slab(out, i))

    widen(loads[0], e, e32, e_o)
    widen(loads[1], r, r32, r_o)
    pass_on(loads[2], lo, lo_o.at[0])
    for copy in loads[3]:
        copy.wait()
    for k, out in enumerate((q_o, k_o, v_o)):
        a32[k] = a[:, k * width : (k + 1) * width].astype(F32)
        outs.put(a32.at[k], out)
    widen(loads[4], o, o32, o_o)
    pass_on(loads[5], tg, tg_o.at[0])
    for k, out in ((0, br_o), (2, bo_o), (4, g2_o), (5, s2_o), (6, g1_o), (7, s1_o)):
        out[...] = total[k : k + 1, pl.ds(al(me * shard, shard), shard)]

    def take_bias(out, line, base):
        count, piece = out.shape
        size = piece * 2 * n_f
        wide = jnp.concatenate(
            [total[line : line + 1, base + h * size : base + (h + 1) * size] for h in range(count)]
        )
        out[...] = lax.dot_general(
            wide, picker(me, piece, 2 * n_f), (((1,), (1,)), ((), ())),
            precision=lax.Precision.HIGHEST, preferred_element_type=F32,
        )

    take_bias(bq_o, 3, 0)
    take_bias(bv_o, 3, width)
    take_bias(be_o, 1, 0)
    outs.wait()


def finish(n_f, total, lo, tg, e, r, a, o, bias, wide_bias):
    (rows, model), (shard, ff), width = lo.shape, e.shape, o.shape[0]
    sds, dma, v = jax.ShapeDtypeStruct, pltpu.SemaphoreType.DMA, pltpu.VMEM
    big = [(1, rows, model)] * 2 + [(shard, ff), (ff, shard)] + [(shard, width)] * 3 + [(width, shard)]
    outs = tuple(sds(shape, BF if i < 2 else F32) for i, shape in enumerate(big))
    outs += (sds((1, shard), F32),) * 6
    outs += (sds(bias.shape, F32),) * 2 + (sds(wide_bias.shape, F32),)
    return pl.pallas_call(
        functools.partial(finish_kernel, n_f),
        out_shape=outs,
        in_specs=[VM] + [HBM] * 6,
        out_specs=(HBM,) * 8 + (VM,) * 9,
        scratch_shapes=[v(x.shape, BF) for x in (lo, tg, e, r, a, o)]
        + [v((shard, ff), F32), v((ff, shard), F32), v((3, shard, width), F32), v((width, shard), F32)]
        + [dma((6, 4)), dma((24,))],
        compiler_params=pltpu.CompilerParams(vmem_limit_bytes=60 << 20),
        cost_estimate=pl.CostEstimate(flops=10**6, bytes_accessed=18 * 10**6, transcendentals=0),
        name="finish",
    )(total, lo, tg, e, r, a, o)


def local(
    tokens, cotangent, block_ids, live_count, first_gain, first_shift, query_weight, query_bias,
    key_weight, value_weight, value_bias, output_weight, output_bias, second_gain, second_shift,
    expand_weight, expand_bias, reduce_weight, reduce_bias,
):
    n_f, n_t = lax.axis_size("fsdp"), lax.axis_size("tp")
    _, rows, model = tokens.shape
    tok = tokens.reshape(rows, model)
    vectors = (first_gain, first_shift, output_bias, second_gain, second_shift, reduce_bias)
    n1, q, kv, ctx, probs, n2, mid, par, full_a, full_o, full_e, full_r = forward(
        n_f, n_t, tok, block_ids, vectors, (query_bias, value_bias, expand_bias),
        query_weight, key_weight, value_weight, output_weight, expand_weight, reduce_weight,
    )
    gb, p2, gm, e_grad, r_part, sums = middle(
        n_f, n_t, live_count, n2, cotangent.reshape(rows, model), mid, par, full_e, full_r, reduce_weight
    )
    lo, tg, r_grad, o_grad, a_grad, total = backward(
        n_f, n_t, live_count, par, sums, tok, gm, mid, p2, gb, ctx, q, kv, probs, n1, full_a, full_o, r_part
    )
    (
        layer_out, tokens_grad, e_grad, r_grad, q_grad, k_grad, v_grad, o_grad,
        g1, s1, b_o, g2, s2, b_r, b_q, b_v, b_e,
    ) = finish(n_f, total, lo, tg, e_grad, r_grad, a_grad, o_grad, query_bias, expand_bias)
    flat = lambda vector: vector.reshape(-1)
    return (
        layer_out, tokens_grad, flat(g1), flat(s1), q_grad, b_q, k_grad, v_grad, b_v, o_grad,
        flat(b_o), flat(g2), flat(s2), e_grad, b_e, r_grad, flat(b_r),
    )


def solution(mesh):
    tokens, vector = P("fsdp", "ctx", None), P(("fsdp", "ctx"))
    down, across = P(("fsdp", "ctx"), "tp"), P("tp", ("fsdp", "ctx"))
    return jax.shard_map(
        local,
        mesh=mesh,
        in_specs=(
            tokens, tokens, P("fsdp", None), P("fsdp"), vector, vector, down, across, down, down,
            across, across, vector, vector, vector, down, across, across, vector,
        ),
        out_specs=(
            tokens, tokens, vector, vector, down, across, down, down, across, across, vector,
            vector, vector, down, across, across, vector,
        ),
        check_vma=False,
    )
```
